32 devices in a mesh: dp: 16 (over z, x, core), tensor: 2 (over y).
Axes of the slice: x: 2, y: 2, z: 4, core: 2. Of those that a mesh axis runs over, the one named last changes fastest.
Arguments:
- inputs: bfloat16 [2, 16, 1024, 768], P(None, 'dp', 'tensor'), may hold values from -6 to 6
- seg_ids: int32 [2, 16, 1024], P(None, 'dp'), may hold values from 0 to 7, never falling along the last dimension, each value on 1 to 512 neighbouring positions
- keep_mask: int32 [2, 16, 1024], P(None, 'dp'), may hold values 0 or 1
- w_qkv: bfloat16 [3, 768, 768], P(None, 'dp', 'tensor'), may hold values from -0.21875 to 0.21875
- b_qv: float32 [2, 768], replicated, may hold values from -3 to 3
- w_o: bfloat16 [768, 768], P('tensor', 'dp'), may hold values from -1.75 to 1.75
- b_o: float32 [768], replicated, may hold values from -3 to 3
- gain_one: float32 [768], replicated, may hold values from 0.5 to 1.5
- shift_one: float32 [768], replicated, may hold values from -3 to 3
- w_up: bfloat16 [768, 3072], P('dp', 'tensor'), may hold values from -0.21875 to 0.21875
- b_up: float32 [3072], replicated, may hold values from -3 to 3
- w_down: bfloat16 [3072, 768], P('tensor', 'dp'), may hold values from -0.109375 to 0.109375
- b_down: float32 [768], replicated, may hold values from -3 to 3
- gain_two: float32 [768], replicated, may hold values from 0.5 to 1.5
- shift_two: float32 [768], replicated, may hold values from -3 to 3
- out_grad: bfloat16 [2, 16, 1024, 768], P(None, 'dp', 'tensor'), may hold values from -6 to 6
Outputs:
- out: bfloat16 [2, 16, 1024, 768], P(None, 'dp', 'tensor')
- x_grad: float32 [2, 16, 1024, 768], P(None, 'dp', 'tensor')
- w_qkv_grad: float32 [3, 768, 768], P(None, 'dp', 'tensor')
- b_qv_grad: float32 [2, 768], P(None, 'tensor')
- w_o_grad: float32 [768, 768], P('tensor', 'dp')
- b_o_grad: float32 [768], replicated
- gain_one_grad: float32 [768], replicated
- shift_one_grad: float32 [768], replicated
- w_up_grad: float32 [768, 3072], P('dp', 'tensor')
- b_up_grad: float32 [3072], P('tensor')
- w_down_grad: float32 [3072, 768], P('tensor', 'dp')
- b_down_grad: float32 [768], replicated
- gain_two_grad: float32 [768], replicated
- shift_two_grad: float32 [768], replicated
The draws below stay inside these ranges and needn't reach their ends.
Inputs may be any that keep to these rules, and one draw needn't show every extreme that they name: `seg_ids`: within each sequence of 1024 positions the document numbers never fall; each document holds 1 to 512 positions and one holds exactly 512.
All inputs are finite; a program needn't handle non-finite values. No bound on the sum of `keep_mask` on one device may be relied on, other than what follows from the above.
Results may differ from the reference program's by a relative error of at most 0.015.
Values may be sent and summed in bfloat16 or wider, within the bound.
A program may use at most 192 MiB of HBM per device.

```python
import math
from functools import partial
import jax
import jax.numpy as jnp
import numpy as np
from jax import lax

D = 768
HEADS = 12
HEAD_DIM = 64
FF = 3072
SEQ = 1024
MICRO = 2
DOCS = 8
DOC_MOST = 512
N_DP = 16


def place_ends(values, stream_key, least, high):
    place = [jax.random.randint(jax.random.fold_in(stream_key, axis), (), 0, length) for axis, length in enumerate(values.shape)]
    main_axis = values.shape.index(max(values.shape))
    neighbour = place[:main_axis] + [(place[main_axis] + 1) % values.shape[main_axis]] + place[main_axis + 1:]
    return values.at[tuple(place)].set(least).at[tuple(neighbour)].set(high)


def shard_levels(stream_key, shape, shards, low, top_value):
    level, own = 1.0, jax.random.fold_in(stream_key, 6)
    for position, blocks in shards:
        draws = jnp.exp(jax.random.uniform(jax.random.fold_in(own, position), (blocks,), jnp.float32, low / len(shards), top_value / len(shards)))
        level = level * jnp.repeat(draws, shape[position] // blocks).reshape([-1 if axis == position else 1 for axis in range(len(shape))])
    return level


def profile(number_of, total, limit, slope):
    loads = [(1 << 20) // math.isqrt(standing ** slope) + 1 for standing in range(2, number_of + 1)]
    rest, counts = total - limit - (number_of - 1), [1] * (number_of - 1)
    while rest > 0:
        candidates = [i for i in range(number_of - 1) if counts[i] < limit]
        whole, budget = sum([loads[i] for i in candidates]), rest
        for i in candidates:
            addition = min(limit - counts[i], max(1, budget * loads[i] // whole), rest)
            counts[i] = counts[i] + addition
            rest = rest - addition
    return np.array([limit] + counts)


def uneven(own_key, number_of, total, reach, lean):
    if number_of == 2:
        one = jax.random.randint(own_key, (), max(1, total - reach), min(reach, total - 1) + 1)
        return jnp.stack([one, total - one])
    sizes = jnp.asarray(profile(number_of, total, reach, lean), jnp.int32)
    twos = (number_of - 1) // 2
    donor, taker = sizes[1:1 + 2 * twos:2], sizes[2:2 + 2 * twos:2]
    room = jnp.minimum(donor - 1, reach - taker)
    shifted = jax.random.randint(jax.random.fold_in(own_key, 1), (twos,), 0, 1 << 20) % (room + 1)
    sizes = sizes.at[1:1 + 2 * twos:2].set(donor - shifted).at[2:2 + 2 * twos:2].set(taker + shifted)
    return sizes[jax.random.permutation(jax.random.fold_in(own_key, 2), number_of)]


def noise(stream_key, extent, width, reach, cuts=(), kind=jnp.bfloat16):
    drawn = jax.random.normal(stream_key, extent, jnp.float32) * width
    if len(cuts) > 0:
        drawn = shard_levels(stream_key, extent, cuts, -0.22, 0.18) * drawn
    return jnp.clip(drawn, min=-reach, max=reach).astype(kind)


def setup_inputs(seed: int = 0) -> dict:
    seeds = jax.random.split(jax.random.key(seed), 17)
    inputs = noise(seeds[0], (MICRO, N_DP, SEQ, D), 1.0, 6.0, ((1, 16), (2, 2)))
    seg_ids = jax.vmap(lambda own: jnp.searchsorted(jnp.cumsum(uneven(own, DOCS, SEQ, DOC_MOST, 2)), jnp.arange(SEQ), side="right"))(jax.random.split(seeds[1], MICRO * N_DP)).reshape((MICRO, N_DP, SEQ)).astype(jnp.int32)
    keep_mask = place_ends((jax.random.randint(seeds[2], (MICRO, N_DP, SEQ), 0, 8) < 7).astype(jnp.int32), jax.random.fold_in(seeds[2], 1), 0, 1)
    w_qkv = noise(seeds[3], (3, D, D), D ** -0.5, 0.21875, ((1, 16), (2, 2)))
    b_qv = noise(seeds[4], (2, D), 0.5, 3.0, (), jnp.float32)
    w_o = noise(seeds[5], (D, D), (D // 64) ** -0.5, 1.75, ((0, 2), (1, 16)))
    b_o = noise(seeds[6], (D,), 0.5, 3.0, (), jnp.float32)
    gain_one = jnp.clip(1.0 + 0.1 * jax.random.normal(seeds[7], (D,), jnp.float32), 0.5, 1.5)
    shift_one = noise(seeds[8], (D,), 0.5, 3.0, (), jnp.float32)
    w_up = noise(seeds[9], (D, FF), D ** -0.5, 0.21875, ((0, 16), (1, 2)))
    b_up = noise(seeds[10], (FF,), 0.5, 3.0, (), jnp.float32)
    w_down = noise(seeds[11], (FF, D), FF ** -0.5, 0.109375, ((0, 2), (1, 16)))
    b_down = noise(seeds[12], (D,), 0.5, 3.0, (), jnp.float32)
    gain_two = jnp.clip(1.0 + 0.1 * jax.random.normal(seeds[13], (D,), jnp.float32), 0.5, 1.5)
    shift_two = noise(seeds[14], (D,), 0.5, 3.0, (), jnp.float32)
    out_grad = noise(seeds[15], (MICRO, N_DP, SEQ, D), 1.0, 6.0, ((1, 16), (2, 2)))
    return dict(inputs=inputs, seg_ids=seg_ids, keep_mask=keep_mask, w_qkv=w_qkv, b_qv=b_qv, w_o=w_o, b_o=b_o, gain_one=gain_one, shift_one=shift_one, w_up=w_up, b_up=b_up, w_down=w_down, b_down=b_down, gain_two=gain_two, shift_two=shift_two, out_grad=out_grad)


@jax.custom_vjp
def low(v):
    return lax.optimization_barrier(v.astype(jnp.bfloat16)).astype(jnp.float32)

@jax.custom_vjp
def low_back(v):
    return v

def low_keep(v):
    return (low(v), None)

def low_pass(kept, grad):
    return (grad,)

def back_keep(v):
    return (v, None)

def back_low(kept, grad):
    return (low(grad),)
low.defvjp(low_keep, low_pass)
low_back.defvjp(back_keep, back_low)
EPS = 1e-06
HIGHEST = lax.Precision.HIGHEST

def gelu_exact(v):
    return 0.5 * v * (1.0 + lax.erf(v * 0.7071067811865476))

def norm_rows(v, gain, shift):
    row_mean = lax.optimization_barrier(jnp.mean(v, axis=-1, keepdims=True))
    centered = v - row_mean
    factor = lax.rsqrt(lax.optimization_barrier(jnp.mean(centered * centered, axis=-1, keepdims=True)) + EPS)
    return centered * factor * gain + shift

def attend_rows(q_rows, seg_block, row_start, key_rows, values, seg_row, keep_row):
    row_count = q_rows.shape[0]
    own_pos = row_start + lax.broadcasted_iota(jnp.int32, (row_count, SEQ), 0)
    key_pos = lax.broadcasted_iota(jnp.int32, (row_count, SEQ), 1)
    allowed = (seg_block[:, None] == seg_row[None, :]) & ((keep_row[None, :] == 1) | (own_pos == key_pos))
    raw = jnp.einsum('qhd,khd->hqk', q_rows, key_rows, precision=HIGHEST) * (1.0 / math.sqrt(HEAD_DIM))
    scores = jnp.where(allowed[None], low_back(raw), -1e+30)
    row_max = lax.optimization_barrier(jnp.max(scores, axis=-1, keepdims=True))
    exps_rows = jnp.exp(scores - row_max)
    probs = low(exps_rows / lax.optimization_barrier(jnp.sum(exps_rows, axis=-1, keepdims=True)))
    return jnp.einsum('hqk,khd->qhd', probs, values, precision=HIGHEST)

def layer_seq(params, tokens, seg_row, keep_row):
    w_qkv, b_qv, w_o, b_o, gain_one, shift_one, w_up, b_up, w_down, b_down, gain_two, shift_two = params
    projected = jnp.einsum('ld,cde->cle', tokens, w_qkv, precision=HIGHEST)
    bias_rows = jnp.stack([b_qv[0], jnp.zeros_like(b_qv[0]), b_qv[1]])
    projected = low(low_back(projected + bias_rows[:, None, :]))
    queries = projected[0].reshape(SEQ, HEADS, HEAD_DIM)
    key_rows = projected[1].reshape(SEQ, HEADS, HEAD_DIM)
    values = projected[2].reshape(SEQ, HEADS, HEAD_DIM)
    block_rows = min(512, SEQ)
    block_count = SEQ // block_rows
    per_block = jax.checkpoint(partial(attend_rows, key_rows=key_rows, values=values, seg_row=seg_row, keep_row=keep_row))
    starts = jnp.arange(block_count, dtype=jnp.int32) * block_rows
    context = lax.map(lambda block_item: per_block(block_item[0], block_item[1], block_item[2]), (queries.reshape(block_count, block_rows, HEADS, HEAD_DIM), seg_row.reshape(block_count, block_rows), starts))
    context = low(low_back(context.reshape(SEQ, D)))
    attn_rows = low_back(jnp.dot(context, w_o, precision=HIGHEST))
    hidden = norm_rows(tokens + attn_rows + b_o, gain_one, shift_one)
    upward = low_back(jnp.dot(low(hidden), w_up, precision=HIGHEST) + b_up)
    active = low(gelu_exact(upward))
    ffn_rows = low_back(jnp.dot(active, w_down, precision=HIGHEST))
    return norm_rows(hidden + ffn_rows + b_down, gain_two, shift_two)

def reference(inputs, seg_ids, keep_mask, w_qkv, b_qv, w_o, b_o, gain_one, shift_one, w_up, b_up, w_down, b_down, gain_two, shift_two, out_grad):
    params = tuple((p.astype(jnp.float32) for p in (w_qkv, b_qv, w_o, b_o, gain_one, shift_one, w_up, b_up, w_down, b_down, gain_two, shift_two)))
    tokens_all = inputs.astype(jnp.float32).reshape(-1, SEQ, D)
    seg_all = seg_ids.reshape(-1, SEQ)
    keep_all = keep_mask.reshape(-1, SEQ)

    def forward(params, tokens_all):
        layer_fn = jax.checkpoint(layer_seq)
        return lax.map(lambda seq_item: layer_fn(params, seq_item[0], seq_item[1], seq_item[2]), (tokens_all, seg_all, keep_all))
    result, pull_back = jax.vjp(forward, params, tokens_all)
    param_grads, grad_tokens = pull_back(out_grad.astype(jnp.float32).reshape(result.shape))
    return (result.astype(jnp.bfloat16).reshape(inputs.shape), grad_tokens.reshape(inputs.shape), param_grads[0], param_grads[1], param_grads[2], param_grads[3], param_grads[4], param_grads[5], param_grads[6], param_grads[7], param_grads[8], param_grads[9], param_grads[10], param_grads[11])
```

```python
import math
import functools
import jax
import jax.numpy as jnp
from jax import lax
from jax.sharding import PartitionSpec as P
from jax.experimental import pallas as pl
from jax.experimental.pallas import tpu as pltpu

HEAD_DIM = 64
EPS = 1e-06
F32 = jnp.float32
BF16 = jnp.bfloat16
VMEM_MOST = 60 * 1024 * 1024


def dot_nn(a, b):
    return lax.dot_general(a, b, (((1,), (0,)), ((), ())), preferred_element_type=F32)


def dot_nt(a, b):
    return lax.dot_general(a, b, (((1,), (1,)), ((), ())), preferred_element_type=F32)


def dot_tn(a, b):
    return lax.dot_general(a, b, (((0,), (0,)), ((), ())), preferred_element_type=F32)


def params(**more):
    return pltpu.CompilerParams(vmem_limit_bytes=VMEM_MOST, **more)


def qkv_kernel(x_ref, w_ref, bias_ref, out_ref):
    rows = x_ref.shape[0]
    step = min(256, rows)
    for start in range(0, rows, step):
        part = dot_nn(x_ref[start : start + step, :], w_ref[0, 0]) + bias_ref[0]
        out_ref[0, start : start + step, :] = part.astype(BF16)


def project(x, weights, bias):
    rows, width = x.shape
    parts, _, _, cols = weights.shape
    wide = bias.shape[-1]
    return pl.pallas_call(
        qkv_kernel,
        grid=(parts,),
        in_specs=[
            pl.BlockSpec((rows, width), lambda t: (0, 0)),
            pl.BlockSpec((1, 1, width, wide), lambda t: (t, 0, 0, 0)),
            pl.BlockSpec((1, 1, wide), lambda t: (t, 0, 0)),
        ],
        out_specs=pl.BlockSpec((1, rows, wide), lambda t: (t, 0, 0)),
        out_shape=jax.ShapeDtypeStruct((parts, rows, wide), BF16),
        compiler_params=params(),
        name="project",
    )(x, weights, bias)


TILE = 256


def allowed_tile(code_ref, seg_ref, key0, query0):
    codes = code_ref[pl.ds(key0, TILE), :]
    codes = jnp.concatenate([codes] * (TILE // codes.shape[1]), axis=1)
    same = codes == seg_ref[:, pl.ds(query0, TILE)]
    key_pos = key0 + lax.broadcasted_iota(jnp.int32, (TILE, TILE), 0)
    query_pos = query0 + lax.broadcasted_iota(jnp.int32, (TILE, TILE), 1)
    return same | (key_pos == query_pos)


def head_masks(lanes):
    lane = lax.broadcasted_iota(jnp.int32, (1, lanes), 1)
    return [(lane // HEAD_DIM == h).astype(BF16) for h in range(lanes // HEAD_DIM)]


def attend_kernel(
    low_ref, high_ref, code_ref, seg_ref, q_ref, k_ref, v_ref, ctx_ref, lse_ref, top, den, acc
):
    rows, lanes = q_ref.shape[1], q_ref.shape[2]
    heads = lanes // HEAD_DIM
    masks = head_masks(lanes)

    @pl.loop(0, rows // TILE)
    def _(qi):
        query0 = pl.multiple_of(qi * TILE, TILE)
        queries = q_ref[0, pl.ds(query0, TILE), :] * BF16(0.125)
        each = [queries * masks[h] for h in range(heads)]
        top[...] = jnp.full_like(top, -1e30)
        den[...] = jnp.zeros_like(den)
        acc[...] = jnp.zeros_like(acc)

        @pl.loop(low_ref[qi], high_ref[qi])
        def _(ki):
            key0 = pl.multiple_of(ki * TILE, TILE)
            allowed = allowed_tile(code_ref, seg_ref, key0, query0)
            keys = k_ref[0, pl.ds(key0, TILE), :]
            values_t = v_ref[0, pl.ds(key0, TILE), :].T
            for h in range(heads):
                scores = jnp.where(allowed, dot_nt(keys, each[h]), -1e30)
                old = top[h]
                new = jnp.maximum(old, jnp.max(scores, axis=0, keepdims=True))
                expo = jnp.exp(scores - new)
                shrink = jnp.exp(old - new)
                top[h] = new
                den[h] = den[h] * shrink + jnp.sum(expo, axis=0, keepdims=True)
                part = dot_nn(values_t[h * HEAD_DIM : (h + 1) * HEAD_DIM], expo.astype(BF16))
                acc[h] = acc[h] * shrink + part

        both = jnp.concatenate([acc[h] / den[h] for h in range(heads)], axis=0)
        ctx_ref[0, pl.ds(query0, TILE), :] = both.astype(BF16).T
        for h in range(heads):
            lse_ref[0, h : h + 1, pl.ds(query0, TILE)] = top[h] + jnp.log(den[h])


def attend(projected, low, high, codes, seg_row):
    parts, rows, wide = projected.shape
    lanes = 128
    heads = lanes // HEAD_DIM
    groups = wide // 3 // lanes
    return pl.pallas_call(
        attend_kernel,
        grid_spec=pltpu.PrefetchScalarGridSpec(
            num_scalar_prefetch=2,
            grid=(parts, groups),
            in_specs=[
                pl.BlockSpec((rows, 128), lambda t, j, lo, hi: (0, 0)),
                pl.BlockSpec((1, rows), lambda t, j, lo, hi: (0, 0)),
                pl.BlockSpec((1, rows, lanes), lambda t, j, lo, hi: (t, 0, j)),
                pl.BlockSpec((1, rows, lanes), lambda t, j, lo, hi: (t, 0, groups + j)),
                pl.BlockSpec((1, rows, lanes), lambda t, j, lo, hi: (t, 0, 2 * groups + j)),
            ],
            out_specs=[
                pl.BlockSpec((1, rows, lanes), lambda t, j, lo, hi: (t, 0, j)),
                pl.BlockSpec((1, heads, rows), lambda t, j, lo, hi: (t * groups + j, 0, 0)),
            ],
            scratch_shapes=[
                pltpu.VMEM((heads, 1, TILE), F32),
                pltpu.VMEM((heads, 1, TILE), F32),
                pltpu.VMEM((heads, HEAD_DIM, TILE), F32),
            ],
        ),
        out_shape=[
            jax.ShapeDtypeStruct((parts, rows, wide // 3), BF16),
            jax.ShapeDtypeStruct((parts * groups, heads, rows), F32),
        ],
        compiler_params=params(),
        name="attend",
    )(low, high, codes, seg_row, projected, projected, projected)


def attend_back_kernel(
    low_ref,
    high_ref,
    code_ref,
    seg_ref,
    q_ref,
    k_ref,
    v_ref,
    ctx_ref,
    g_ref,
    lse_ref,
    dq_ref,
    dk_ref,
    dv_ref,
    qsum_ref,
    vsum_ref,
    dq_acc,
    dk_acc,
    dv_acc,
):
    rows, lanes = q_ref.shape[1], q_ref.shape[2]
    heads = lanes // HEAD_DIM
    masks = head_masks(lanes)
    dk_acc[...] = jnp.zeros_like(dk_acc)
    dv_acc[...] = jnp.zeros_like(dv_acc)

    @pl.loop(0, rows // TILE)
    def _(qi):
        query0 = pl.multiple_of(qi * TILE, TILE)
        queries = q_ref[0, pl.ds(query0, TILE), :] * BF16(0.125)
        grads = g_ref[0, pl.ds(query0, TILE), :]
        prod_t = (grads.astype(F32) * ctx_ref[0, pl.ds(query0, TILE), :].astype(F32)).T
        q_each = [queries * masks[h] for h in range(heads)]
        g_each = [grads * masks[h] for h in range(heads)]
        inner = [
            jnp.sum(prod_t[h * HEAD_DIM : (h + 1) * HEAD_DIM], axis=0, keepdims=True)
            for h in range(heads)
        ]
        lse = [lse_ref[0, h : h + 1, pl.ds(query0, TILE)] for h in range(heads)]
        dq_acc[...] = jnp.zeros_like(dq_acc)

        @pl.loop(low_ref[qi], high_ref[qi])
        def _(ki):
            key0 = pl.multiple_of(ki * TILE, TILE)
            allowed = allowed_tile(code_ref, seg_ref, key0, query0)
            keys = k_ref[0, pl.ds(key0, TILE), :]
            values = v_ref[0, pl.ds(key0, TILE), :]
            keys_t = keys.T
            dk = dk_acc[pl.ds(key0, TILE), :]
            dv = dv_acc[pl.ds(key0, TILE), :]
            for h in range(heads):
                scores = jnp.where(allowed, dot_nt(keys, q_each[h]), -1e30)
                probs = jnp.exp(scores - lse[h])
                gprobs = dot_nt(values, g_each[h])
                gscores = (probs * (gprobs - inner[h])).astype(BF16)
                dv = dv + dot_nn(probs.astype(BF16), g_each[h])
                dk = dk + dot_nn(gscores, q_each[h])
                lanes_h = slice(h * HEAD_DIM, (h + 1) * HEAD_DIM)
                dq_acc[h] += dot_nn(keys_t[lanes_h], gscores)
            dk_acc[pl.ds(key0, TILE), :] = dk
            dv_acc[pl.ds(key0, TILE), :] = dv

        both = jnp.concatenate([dq_acc[h] for h in range(heads)], axis=0) * 0.125
        dq_ref[0, pl.ds(query0, TILE), :] = both.astype(BF16).T

    low_k = dk_acc[...].astype(BF16)
    low_v = dv_acc[...].astype(BF16)
    dk_ref[0] = low_k
    dv_ref[0] = low_v
    qsum_ref[0] = jnp.sum(dq_ref[0].astype(F32), axis=0, keepdims=True)
    vsum_ref[0] = jnp.sum(low_v.astype(F32), axis=0, keepdims=True)


def attend_back(projected, context, grad_context, lse, low, high, codes, seg_row):
    parts, rows, wide = projected.shape
    lanes = 128
    heads = lanes // HEAD_DIM
    groups = wide // 3 // lanes
    flat = pl.BlockSpec((1, rows, lanes), lambda t, j, lo, hi: (t, 0, j))
    sums = pl.BlockSpec((1, 1, lanes), lambda t, j, lo, hi: (t, 0, j))
    return pl.pallas_call(
        attend_back_kernel,
        grid_spec=pltpu.PrefetchScalarGridSpec(
            num_scalar_prefetch=2,
            grid=(parts, groups),
            in_specs=[
                pl.BlockSpec((rows, 128), lambda t, j, lo, hi: (0, 0)),
                pl.BlockSpec((1, rows), lambda t, j, lo, hi: (0, 0)),
                pl.BlockSpec((1, rows, lanes), lambda t, j, lo, hi: (t, 0, j)),
                pl.BlockSpec((1, rows, lanes), lambda t, j, lo, hi: (t, 0, groups + j)),
                pl.BlockSpec((1, rows, lanes), lambda t, j, lo, hi: (t, 0, 2 * groups + j)),
                flat,
                flat,
                pl.BlockSpec((1, heads, rows), lambda t, j, lo, hi: (t * groups + j, 0, 0)),
            ],
            out_specs=[flat, flat, flat, sums, sums],
            scratch_shapes=[
                pltpu.VMEM((heads, HEAD_DIM, TILE), F32),
                pltpu.VMEM((rows, lanes), F32),
                pltpu.VMEM((rows, lanes), F32),
            ],
        ),
        out_shape=[jax.ShapeDtypeStruct((parts, rows, wide // 3), BF16)] * 3
        + [jax.ShapeDtypeStruct((parts, 1, wide // 3), F32)] * 2,
        compiler_params=params(),
        name="attend_back",
    )(low, high, codes, seg_row, projected, projected, projected, context, grad_context, lse)


def norm_forward(v):
    mean = jnp.mean(v, axis=-1, keepdims=True)
    centered = v - mean
    factor = lax.rsqrt(jnp.mean(centered * centered, axis=-1, keepdims=True) + EPS)
    return centered * factor, factor


def norm_back(inner, normed, factor):
    return factor * (
        inner
        - jnp.mean(inner, axis=-1, keepdims=True)
        - normed * jnp.mean(inner * normed, axis=-1, keepdims=True)
    )


def col_sum(v):
    return jnp.sum(v, axis=0, keepdims=True)


UNIT_STEP = 512


def rows_kernel(
    x_ref,
    ctx_ref,
    g_ref,
    wo_ref,
    up_ref,
    down_ref,
    vec_ref,
    bup_ref,
    out_ref,
    hid_ref,
    sec_ref,
    first_ref,
    gfirst_ref,
    act_ref,
    gup_ref,
    gctx_ref,
    sums_ref,
    upsum_ref,
    slope,
):
    parts, _, units = act_ref.shape

    @pl.when(pl.program_id(0) == 0)
    def _():
        sums_ref[...] = jnp.zeros_like(sums_ref)
        upsum_ref[...] = jnp.zeros_like(upsum_ref)

    b_o, gain_one, shift_one = vec_ref[0:1], vec_ref[1:2], vec_ref[2:3]
    b_down, gain_two, shift_two = vec_ref[3:4], vec_ref[4:5], vec_ref[5:6]
    first_sum = x_ref[...].astype(F32) + b_o
    for t in range(parts):
        first_sum = first_sum + dot_nt(ctx_ref[t], wo_ref[t, 0])
    normed_one, factor_one = norm_forward(first_sum)
    hidden = normed_one * gain_one + shift_one
    hidden_low = hidden.astype(BF16)
    hid_ref[...] = hidden_low
    second_sum = hidden + b_down
    for t in range(parts):
        for u in range(0, units, UNIT_STEP):
            at = slice(u, u + UNIT_STEP)
            up = dot_nn(hidden_low, up_ref[t, 0, :, at]) + bup_ref[t, :, at]
            half = 0.5 * (1.0 + lax.erf(up * 0.7071067811865476))
            active = (up * half).astype(BF16)
            act_ref[t, :, at] = active
            slope[t, :, at] = half + up * jnp.exp(-0.5 * up * up) * 0.3989422804014327
            second_sum = second_sum + dot_nt(active, down_ref[t, 0, :, at])
    normed_two, factor_two = norm_forward(second_sum)
    out_ref[...] = (normed_two * gain_two + shift_two).astype(BF16)
    grad_out = g_ref[...].astype(F32)
    grad_second = norm_back(grad_out * gain_two, normed_two, factor_two)
    second_low = grad_second.astype(BF16)
    sec_ref[...] = second_low
    grad_hidden = grad_second
    for t in range(parts):
        for u in range(0, units, UNIT_STEP):
            at = slice(u, u + UNIT_STEP)
            grad_up = (dot_nn(second_low, down_ref[t, 0, :, at]) * slope[t, :, at]).astype(BF16)
            gup_ref[t, :, at] = grad_up
            upsum_ref[t, :, at] += col_sum(grad_up.astype(F32))
            grad_hidden = grad_hidden + dot_nt(grad_up, up_ref[t, 0, :, at])
    grad_first = norm_back(grad_hidden * gain_one, normed_one, factor_one)
    gfirst_ref[...] = grad_first
    first_low = grad_first.astype(BF16)
    first_ref[...] = first_low
    for t in range(parts):
        gctx_ref[t] = dot_nn(first_low, wo_ref[t, 0]).astype(BF16)
    sums_ref[0:1] += col_sum(grad_first)
    sums_ref[1:2] += col_sum(grad_hidden * normed_one)
    sums_ref[2:3] += col_sum(grad_hidden)
    sums_ref[3:4] += col_sum(grad_second)
    sums_ref[4:5] += col_sum(grad_out * normed_two)
    sums_ref[5:6] += col_sum(grad_out)


def rows_pass(x, context, grads, weights, vectors, bias_up):
    rows, width = x.shape
    parts, _, _, units = weights.shape
    part_width = context.shape[2]
    step = min(256, rows)
    row = pl.BlockSpec((step, width), lambda i: (i, 0))
    split = pl.BlockSpec((parts, step, part_width), lambda i: (0, i, 0))
    wide = pl.BlockSpec((parts, step, units), lambda i: (0, i, 0))
    once = pl.Buffered(1)
    last = units // part_width - 1
    return pl.pallas_call(
        rows_kernel,
        grid=(rows // step,),
        in_specs=[
            row,
            split,
            row,
            pl.BlockSpec(
                (parts, 1, width, part_width), lambda i: (0, 0, 0, last), pipeline_mode=once
            ),
            pl.BlockSpec((parts, 1, width, units), lambda i: (0, 1, 0, 0), pipeline_mode=once),
            pl.BlockSpec((parts, 1, width, units), lambda i: (0, 2, 0, 0), pipeline_mode=once),
            pl.BlockSpec((8, width), lambda i: (0, 0)),
            pl.BlockSpec((parts, 1, units), lambda i: (0, 0, 0)),
        ],
        out_specs=[
            row,
            row,
            row,
            row,
            row,
            wide,
            wide,
            split,
            pl.BlockSpec((8, width), lambda i: (0, 0)),
            pl.BlockSpec((parts, 1, units), lambda i: (0, 0, 0)),
        ],
        out_shape=[
            jax.ShapeDtypeStruct((rows, width), BF16),
            jax.ShapeDtypeStruct((rows, width), BF16),
            jax.ShapeDtypeStruct((rows, width), BF16),
            jax.ShapeDtypeStruct((rows, width), BF16),
            jax.ShapeDtypeStruct((rows, width), F32),
            jax.ShapeDtypeStruct((parts, rows, units), BF16),
            jax.ShapeDtypeStruct((parts, rows, units), BF16),
            jax.ShapeDtypeStruct((parts, rows, part_width), BF16),
            jax.ShapeDtypeStruct((8, width), F32),
            jax.ShapeDtypeStruct((parts, 1, units), F32),
        ],
        scratch_shapes=[pltpu.VMEM((parts, step, units), F32)],
        compiler_params=params(),
        name="rows_pass",
    )(x, context, grads, weights, weights, weights, vectors, bias_up)


GRAD_STEP = 256


def outer_kernel(rows_ref, cols_ref, out_ref):
    width = rows_ref.shape[1]
    for m in range(0, width, GRAD_STEP):
        at = slice(m, m + GRAD_STEP)
        out_ref[0, at, :] = dot_tn(rows_ref[:, at], cols_ref[0]).astype(BF16)


def outer(left, right):
    rows, width = left.shape
    parts, _, units = right.shape
    return pl.pallas_call(
        outer_kernel,
        grid=(parts,),
        in_specs=[
            pl.BlockSpec((rows, width), lambda t: (0, 0)),
            pl.BlockSpec((1, rows, units), lambda t: (t, 0, 0)),
        ],
        out_specs=pl.BlockSpec((1, width, units), lambda t: (t, 0, 0)),
        out_shape=jax.ShapeDtypeStruct((parts, width, units), BF16),
        compiler_params=params(),
        name="outer",
    )(left, right)


def outer_four_kernel(x_ref, first_ref, q_ref, k_ref, v_ref, ctx_ref, out_ref):
    width = x_ref.shape[1]
    part_width = q_ref.shape[2]
    for m in range(0, width, GRAD_STEP):
        at = slice(m, m + GRAD_STEP)
        for n, cols in enumerate((q_ref, k_ref, v_ref, ctx_ref)):
            left = first_ref if n == 3 else x_ref
            part = dot_tn(left[:, at], cols[0])
            out_ref[0, at, n * part_width : (n + 1) * part_width] = part.astype(BF16)


def outer_four(x, first_low, grad_q, grad_k, grad_v, context):
    rows, width = x.shape
    parts, _, part_width = context.shape
    row = pl.BlockSpec((rows, width), lambda t: (0, 0))
    split = pl.BlockSpec((1, rows, part_width), lambda t: (t, 0, 0))
    return pl.pallas_call(
        outer_four_kernel,
        grid=(parts,),
        in_specs=[row, row, split, split, split, split],
        out_specs=pl.BlockSpec((1, width, 4 * part_width), lambda t: (t, 0, 0)),
        out_shape=jax.ShapeDtypeStruct((parts, width, 4 * part_width), BF16),
        compiler_params=params(),
        name="outer_four",
    )(x, first_low, grad_q, grad_k, grad_v, context)


def input_grad_kernel(base_ref, q_ref, k_ref, v_ref, w_ref, out_ref):
    parts, _, part_width = q_ref.shape
    total = base_ref[...]
    for t in range(parts):
        for c, cols in enumerate((q_ref, k_ref, v_ref)):
            at = slice(c * part_width, (c + 1) * part_width)
            total = total + dot_nt(cols[t], w_ref[t, 0, :, at])
    out_ref[...] = total.astype(out_ref.dtype)


def input_grad(grad_first, grad_q, grad_k, grad_v, weights):
    rows, width = grad_first.shape
    parts, _, part_width = grad_q.shape
    step = min(256, rows)
    row = pl.BlockSpec((step, width), lambda i: (i, 0))
    split = pl.BlockSpec((parts, step, part_width), lambda i: (0, i, 0))
    return pl.pallas_call(
        input_grad_kernel,
        grid=(rows // step,),
        in_specs=[
            row,
            split,
            split,
            split,
            pl.BlockSpec((parts, 1, width, 3 * part_width), lambda i: (0, 0, 0, 0)),
        ],
        out_specs=row,
        out_shape=jax.ShapeDtypeStruct((rows, width), BF16),
        compiler_params=params(),
        name="input_grad",
    )(grad_first, grad_q, grad_k, grad_v, weights)


LINE = 4


class Place:
    def __init__(self):
        dp = lax.axis_index("dp")
        self.y = lax.axis_index("tensor")
        self.core = lax.rem(dp, 2)
        self.x = lax.rem(lax.div(dp, 2), 2)
        self.z = lax.div(dp, 4)
        self.fx = lax.rem(self.x + 1 - self.core, 2)
        self.fy = lax.rem(self.y + self.core, 2)
        self.sx = lax.rem(self.x + self.core, 2)
        self.sy = lax.rem(self.y + 1 - self.core, 2)

    @staticmethod
    def at(z, x, core, y):
        return ((z * 2 + x) * 2 + core, y)

    def up(self):
        return self.at(self.z + 1, self.x, self.core, self.y)

    def down(self):
        return self.at(self.z - 1, self.x, self.core, self.y)

    def first(self):
        return self.at(self.z, self.fx, self.core, self.fy)

    def second(self):
        return self.at(self.z, self.sx, self.core, self.sy)

    def partner(self):
        return self.at(self.z, self.x, 1 - self.core, self.y)

    def across_y(self):
        return self.at(self.z, self.x, self.core, 1 - self.y)

    def greet(self):
        barrier = pltpu.get_barrier_semaphore()

        def signal(device):
            pl.semaphore_signal(
                barrier, inc=1, device_id=device, device_id_type=pl.DeviceIdType.MESH
            )

        signal(self.first())
        signal(self.second())
        signal(self.partner())

        @pl.when(self.z < LINE - 1)
        def _():
            signal(self.up())

        @pl.when(self.z > 0)
        def _():
            signal(self.down())

        inner = ((self.z > 0) & (self.z < LINE - 1)).astype(jnp.int32)
        pl.semaphore_wait(barrier, 4 + inner)


def remote(src, dst, sends, recvs, slot, device):
    return pltpu.make_async_remote_copy(
        src_ref=src,
        dst_ref=dst,
        send_sem=sends.at[slot],
        recv_sem=recvs.at[slot],
        device_id=device,
        device_id_type=pl.DeviceIdType.MESH,
    )


def gather_kernel(
    shard_ref, in_ref, grad_ref, w_ref, x_ref, g_ref, z_send, z_recv, s_send, s_recv, local_sem
):
    place = Place()
    z, x, y, core = place.z, place.x, place.y, place.core
    chunks = shard_ref.shape[0]
    place.greet()

    trades = []
    for n, (src, dst) in enumerate(((in_ref, x_ref), (grad_ref, g_ref))):
        copy = remote(
            src.at[1 - y], dst.at[y], s_send, s_recv, chunks * 8 + n, place.across_y()
        )
        trades.append(copy)
    trades[0].start()
    local = [
        pltpu.make_async_copy(in_ref.at[y], x_ref.at[y], local_sem.at[0]),
        pltpu.make_async_copy(grad_ref.at[y], g_ref.at[y], local_sem.at[1]),
    ]
    for k in range(chunks):
        local.append(
            pltpu.make_async_copy(
                shard_ref.at[k], w_ref.at[y, k, z, x, core], local_sem.at[2 + k]
            )
        )
    for copy in local:
        copy.start()

    def piece(k, zz):
        return w_ref.at[y, k, zz, x, core]

    def upward(k, d):
        zz = jnp.maximum(z - d + 1, 0)
        src = shard_ref.at[k] if d == 1 else piece(k, zz)
        return remote(src, piece(k, zz), z_send, z_recv, (k * 2) * LINE + d, place.up())

    def downward(k, d):
        zz = jnp.minimum(z + d - 1, LINE - 1)
        src = shard_ref.at[k] if d == 1 else piece(k, zz)
        return remote(src, piece(k, zz), z_send, z_recv, (k * 2 + 1) * LINE + d, place.down())

    def from_below(k, d):
        here = piece(k, jnp.maximum(z - d, 0))
        return remote(here, here, z_send, z_recv, (k * 2) * LINE + d, place.up())

    def from_above(k, d):
        here = piece(k, jnp.minimum(z + d, LINE - 1))
        return remote(here, here, z_send, z_recv, (k * 2 + 1) * LINE + d, place.down())

    def line(k, yy, xx, cc):
        return w_ref.at[yy, k, :, xx, cc]

    def square(k, n, yy, xx, device, cc=None):
        ref = line(k, yy, xx, core if cc is None else cc)
        return remote(ref, ref, s_send, s_recv, k * 8 + n, device)

    def out_first(k):
        return square(k, 0, y, x, place.first())

    def in_first(k):
        return square(k, 0, place.fy, place.fx, place.first())

    def out_second(k, n):
        yy, xx = (y, x) if n == 0 else (place.fy, place.fx)
        return square(k, 1 + n, yy, xx, place.second())

    def in_second(k, n):
        yy, xx = (place.sy, place.sx) if n == 0 else (1 - y, 1 - x)
        return square(k, 1 + n, yy, xx, place.second())

    corners = ((y, x), (place.fy, place.fx), (place.sy, place.sx), (1 - y, 1 - x))

    def out_partner(k, n):
        yy, xx = corners[n]
        return square(k, 3 + n, yy, xx, place.partner())

    def in_partner(k, n):
        yy, xx = corners[(0, 2, 1, 3)[n]]
        return square(k, 3 + n, yy, xx, place.partner(), 1 - core)

    for k in range(chunks):
        @pl.when(z < LINE - 1)
        def _():
            upward(k, 1).start()

        @pl.when(z > 0)
        def _():
            downward(k, 1).start()

    for copy in local:
        copy.wait()

    def relay(k):
        for d in range(1, LINE):
            @pl.when(z >= d)
            def _():
                from_below(k, d).wait_recv()

            if d < LINE - 1:
                @pl.when((z >= d) & (z < LINE - 1))
                def _():
                    upward(k, d + 1).start()

            @pl.when(z + d < LINE)
            def _():
                from_above(k, d).wait_recv()

            if d < LINE - 1:
                @pl.when((z + d < LINE) & (z > 0))
                def _():
                    downward(k, d + 1).start()
        out_first(k).start()
        out_second(k, 0).start()
        out_partner(k, 0).start()

    def pass_first(k):
        in_first(k).wait_recv()
        out_second(k, 1).start()
        out_partner(k, 1).start()

    def pass_second(k):
        for n in range(2):
            in_second(k, n).wait_recv()
            out_partner(k, 2 + n).start()

    for k in range(chunks + 2):
        if k < chunks:
            relay(k)
            if k == 0:
                trades[1].start()
        if 0 <= k - 1 < chunks:
            pass_first(k - 1)
        if 0 <= k - 2 < chunks:
            pass_second(k - 2)
    for k in range(chunks):
        for n in range(4):
            in_partner(k, n).wait_recv()
    for k in range(chunks):
        for d in range(1, LINE):
            @pl.when((z >= d - 1) & (z < LINE - 1))
            def _():
                upward(k, d).wait_send()

            @pl.when((z + d - 1 < LINE) & (z > 0))
            def _():
                downward(k, d).wait_send()
        out_first(k).wait_send()
        for n in range(2):
            out_second(k, n).wait_send()
        for n in range(4):
            out_partner(k, n).wait_send()
    for copy in trades:
        copy.wait()


def gather_all(shard, halves, grad_halves):
    chunks, own_rows, units = shard.shape
    parts, rows, width = halves.shape
    anywhere = pl.BlockSpec(memory_space=pl.ANY)
    local = pl.BlockSpec(memory_space=pltpu.VMEM)
    weights, x, grads = pl.pallas_call(
        gather_kernel,
        in_specs=[local] * 3,
        out_specs=[anywhere] * 3,
        out_shape=[
            jax.ShapeDtypeStruct((parts, chunks, LINE, 2, 2, own_rows, units), BF16),
            jax.ShapeDtypeStruct((parts, rows, width), BF16),
            jax.ShapeDtypeStruct((parts, rows, width), BF16),
        ],
        scratch_shapes=[
            pltpu.SemaphoreType.DMA((chunks * 2 * LINE,)),
            pltpu.SemaphoreType.DMA((chunks * 2 * LINE,)),
            pltpu.SemaphoreType.DMA((chunks * 8 + 2,)),
            pltpu.SemaphoreType.DMA((chunks * 8 + 2,)),
            pltpu.SemaphoreType.DMA((chunks + 2,)),
        ],
        compiler_params=params(collective_id=0, has_side_effects=True),
        name="gather_all",
    )(shard, halves, grad_halves)
    return (
        weights.reshape(parts, chunks, -1, units),
        x.reshape(parts * rows, width),
        grads.reshape(parts * rows, width),
    )


def reduce_kernel(
    a_ref,
    b_ref,
    c_ref,
    xg_ref,
    small_ref,
    out_ref,
    xr_ref,
    total_ref,
    p_buf,
    s_buf,
    f_buf,
    u_buf,
    d_buf,
    t_buf,
    z_send,
    z_recv,
    s_send,
    s_recv,
    t_send,
    t_recv,
    local_sem,
):
    place = Place()
    z, x, y, core = place.z, place.x, place.y, place.core
    grads = (a_ref, b_ref, c_ref)
    chunks = len(grads)
    corners = ((y, x), (place.fy, place.fx), (place.sy, place.sx), (1 - y, 1 - x))
    place.greet()

    def swap(k, n, src, dst, device):
        return remote(src, dst, s_send, s_recv, k * 8 + n, device)

    def to_partner(k, n):
        yy, xx = corners[n]
        return swap(
            k, n, grads[k].at[yy, :, xx, 1 - core], p_buf.at[k, yy, :, xx], place.partner()
        )

    def from_partner(k, n):
        yy, xx = corners[n]
        here = p_buf.at[k, yy, :, xx]
        return swap(k, (0, 2, 1, 3)[n], here, here, place.partner())

    def to_second(k, n):
        yy, xx = corners[2 + n]
        return swap(k, 4 + n, p_buf.at[k, yy, :, xx], s_buf.at[k, n], place.second())

    def to_first(k):
        return swap(k, 6, s_buf.at[k, 1], f_buf.at[k], place.first())

    def up_copy(k, tt):
        src = u_buf.at[k, tt]
        return remote(src, src, z_send, z_recv, (k * 2) * LINE + tt, place.up())

    def down_copy(k, tt):
        src = d_buf.at[k, tt]
        return remote(src, src, z_send, z_recv, (k * 2 + 1) * LINE + tt, place.down())

    def small_copy(n, src, dst, device):
        return remote(src, dst, t_send, t_recv, n, device)

    over_x = place.at(z, 1 - x, core, y)
    hops = (
        small_copy(0, small_ref, t_buf.at[0], place.partner()),
        small_copy(1, t_buf.at[1], t_buf.at[2], over_x),
        small_copy(2, t_buf.at[3], t_buf.at[4], place.across_y()),
    )

    def small_up(d):
        piece = t_buf.at[5 + jnp.maximum(z - d + 1, 0)]
        return small_copy(2 + d, piece, piece, place.up())

    def small_down(d):
        piece = t_buf.at[5 + jnp.minimum(z + d - 1, LINE - 1)]
        return small_copy(2 + LINE + d, piece, piece, place.down())

    def small_below(d):
        piece = t_buf.at[5 + jnp.maximum(z - d, 0)]
        return small_copy(2 + d, piece, piece, place.up())

    def small_above(d):
        piece = t_buf.at[5 + jnp.minimum(z + d, LINE - 1)]
        return small_copy(2 + LINE + d, piece, piece, place.down())

    def small_step(step):
        if step == 0:
            hops[0].start()
        elif step == 1:
            hops[0].wait_recv()
            t_buf[1] = small_ref[...] + t_buf[0]
            hops[1].start()
        elif step == 2:
            hops[1].wait_recv()
            t_buf[3] = t_buf[1] + t_buf[2]
            hops[2].start()
        elif step == 3:
            hops[2].wait_recv()
            t_buf[5 + z] = t_buf[3] + t_buf[4]

            @pl.when(z < LINE - 1)
            def _():
                small_up(1).start()

            @pl.when(z > 0)
            def _():
                small_down(1).start()
        elif step == 4:
            for d in range(1, LINE):
                @pl.when(z >= d)
                def _():
                    small_below(d).wait_recv()

                if d < LINE - 1:
                    @pl.when((z >= d) & (z < LINE - 1))
                    def _():
                        small_up(d + 1).start()

                @pl.when(z + d < LINE)
                def _():
                    small_above(d).wait_recv()

                if d < LINE - 1:
                    @pl.when((z + d < LINE) & (z > 0))
                    def _():
                        small_down(d + 1).start()
            total_ref[...] = (t_buf[5] + t_buf[6]) + (t_buf[7] + t_buf[8])

    trade = remote(
        xg_ref.at[1 - y], xr_ref.at[y], t_send, t_recv, 3 + 2 * LINE, place.across_y()
    )
    arrive = remote(
        xg_ref.at[1 - y], xr_ref.at[1 - y], t_send, t_recv, 3 + 2 * LINE, place.across_y()
    )
    keep = pltpu.make_async_copy(xg_ref.at[y], xr_ref.at[y], local_sem.at[0])

    def accumulate(target, other):
        @pl.loop(0, LINE)
        def _(i):
            target[i] = target[i] + other[i]

    def stage_partner(k):
        for n in (3, 2, 1, 0):
            yy, xx = corners[n]
            from_partner(k, n).wait_recv()
            accumulate(p_buf.at[k, yy, :, xx], grads[k].at[yy, :, xx, core])
            if n >= 2:
                to_second(k, n - 2).start()

    def stage_second(k):
        for n in (1, 0):
            yy, xx = corners[n]
            to_second(k, n).wait_recv()
            accumulate(s_buf.at[k, n], p_buf.at[k, yy, :, xx])
            if n == 1:
                to_first(k).start()

    def stage_first(k):
        to_first(k).wait_recv()
        accumulate(f_buf.at[k], s_buf.at[k, 0])

    def stage_line(k):
        for tt_up, tt_down in ((3, 0), (2, 1), (1, 2)):
            @pl.when((z > 0) & (z <= tt_up))
            def _():
                up_copy(k, tt_up).wait_recv()

            @pl.when((z > 0) & (z < tt_up))
            def _():
                u_buf[k, tt_up] = u_buf[k, tt_up] + f_buf[k, tt_up]

            @pl.when(z == 0)
            def _():
                u_buf[k, tt_up] = f_buf[k, tt_up]

            @pl.when(z < tt_up)
            def _():
                up_copy(k, tt_up).start()

            @pl.when((z < LINE - 1) & (z >= tt_down))
            def _():
                down_copy(k, tt_down).wait_recv()

            @pl.when((z < LINE - 1) & (z > tt_down))
            def _():
                d_buf[k, tt_down] = d_buf[k, tt_down] + f_buf[k, tt_down]

            @pl.when(z == LINE - 1)
            def _():
                d_buf[k, tt_down] = f_buf[k, tt_down]

            @pl.when(z > tt_down)
            def _():
                down_copy(k, tt_down).start()

    def finish(k):
        own = f_buf[k, z].astype(F32)

        @pl.when(z == 0)
        def _():
            out_ref[k] = own + d_buf[k, 0].astype(F32)

        @pl.when(z == LINE - 1)
        def _():
            out_ref[k] = own + u_buf[k, LINE - 1].astype(F32)

        @pl.when((z > 0) & (z < LINE - 1))
        def _():
            out_ref[k] = own + u_buf[k, z].astype(F32) + d_buf[k, z].astype(F32)

    small_step(0)
    for k in range(chunks):
        for n in (3, 2, 1, 0):
            to_partner(k, n).start()
    keep.start()
    small_step(1)
    for i in range(chunks + 3):
        if i < chunks:
            stage_partner(i)
            if i == 0:
                trade.start()
        if 0 <= i - 1 < chunks:
            stage_second(i - 1)
        if 0 <= i - 2 < chunks:
            stage_first(i - 2)
        if 0 <= i - 3 < chunks:
            stage_line(i - 3)
        if i < 3:
            small_step(2 + i)
    for k in range(chunks):
        finish(k)

    keep.wait()
    trade.wait_send()
    arrive.wait_recv()
    for copy in hops:
        copy.wait_send()
    for d in range(1, LINE):
        @pl.when((z >= d - 1) & (z < LINE - 1))
        def _():
            small_up(d).wait_send()

        @pl.when((z + d - 1 < LINE) & (z > 0))
        def _():
            small_down(d).wait_send()
    for k in range(chunks):
        for n in range(4):
            to_partner(k, n).wait_send()
        for n in range(2):
            to_second(k, n).wait_send()
        to_first(k).wait_send()
        for tt in range(LINE):
            if tt > 0:
                @pl.when(z < tt)
                def _():
                    up_copy(k, tt).wait_send()

            if tt < LINE - 1:
                @pl.when(z > tt)
                def _():
                    down_copy(k, tt).wait_send()


def reduce_all(grads_a, grads_b, grads_c, halves, small):
    parts, width, units = grads_a.shape
    _, rows, model = halves.shape
    own_rows = width // (4 * LINE)
    chunks = 3
    folded = [g.reshape(parts, LINE, 2, 2, own_rows, units) for g in (grads_a, grads_b, grads_c)]
    small_rows = small.shape[0] // 128
    local = pl.BlockSpec(memory_space=pltpu.VMEM)
    line = (LINE, own_rows, units)
    own, x_rows, total = pl.pallas_call(
        reduce_kernel,
        in_specs=[local] * 5,
        out_specs=[local, pl.BlockSpec(memory_space=pl.ANY), local],
        out_shape=[
            jax.ShapeDtypeStruct((chunks, own_rows, units), F32),
            jax.ShapeDtypeStruct((parts, rows, model), BF16),
            jax.ShapeDtypeStruct((small_rows, 128), F32),
        ],
        scratch_shapes=[
            pltpu.VMEM((chunks, 2, LINE, 2, own_rows, units), BF16),
            pltpu.VMEM((chunks, 2) + line, BF16),
            pltpu.VMEM((chunks,) + line, BF16),
            pltpu.VMEM((chunks,) + line, BF16),
            pltpu.VMEM((chunks,) + line, BF16),
            pltpu.VMEM((5 + LINE, small_rows, 128), F32),
            pltpu.SemaphoreType.DMA((chunks * 2 * LINE,)),
            pltpu.SemaphoreType.DMA((chunks * 2 * LINE,)),
            pltpu.SemaphoreType.DMA((chunks * 8,)),
            pltpu.SemaphoreType.DMA((chunks * 8,)),
            pltpu.SemaphoreType.DMA((4 + 2 * LINE,)),
            pltpu.SemaphoreType.DMA((4 + 2 * LINE,)),
            pltpu.SemaphoreType.DMA((1,)),
        ],
        compiler_params=params(collective_id=1, has_side_effects=True),
        name="reduce_all",
    )(*folded, halves, small.reshape(small_rows, 128))
    return own, x_rows, total.reshape(-1)


def trade_in(halves):
    return lax.all_to_all(halves, "tensor", split_axis=0, concat_axis=1, tiled=True)[0]


def trade_out(whole):
    return lax.all_to_all(whole[None], "tensor", split_axis=1, concat_axis=0, tiled=True)


def gather_weights(shard):
    full = lax.all_gather(shard, "dp", axis=1, tiled=True)
    return lax.all_gather(full, "tensor", axis=0, tiled=False)


def scatter_grads(partial):
    own = lax.psum_scatter(partial, "tensor", scatter_dimension=0, tiled=False)
    return lax.psum_scatter(own, "dp", scatter_dimension=0, tiled=True)


def shards(
    inputs,
    seg_ids,
    keep_mask,
    w_qkv,
    b_qv,
    w_o,
    b_o,
    gain_one,
    shift_one,
    w_up,
    b_up,
    w_down,
    b_down,
    gain_two,
    shift_two,
    out_grad,
):
    parts = lax.axis_size("tensor")
    assert inputs.shape[0] == parts
    own_rows = w_qkv.shape[1]
    part_width = w_qkv.shape[2]
    units = w_up.shape[1]
    rank = lax.axis_index("tensor")

    shard_a = jnp.concatenate([w_qkv[0], w_qkv[1], w_qkv[2], w_o.T], axis=1)
    shard = jnp.stack([shard_a, w_up, w_down.T])
    linked = lax.axis_size("dp") == LINE * 4 and parts == 2
    if linked:
        weights, x, grads = gather_all(shard, inputs[:, 0], out_grad[:, 0])
    else:
        weights = gather_weights(shard)
        x = trade_in(inputs[:, 0])
        grads = trade_in(out_grad[:, 0])

    seg = lax.dynamic_index_in_dim(seg_ids[:, 0], rank, 0, keepdims=False)
    keep = lax.dynamic_index_in_dim(keep_mask[:, 0], rank, 0, keepdims=False)
    length = seg.shape[0]
    firsts, lasts = seg[::TILE], seg[TILE - 1 :: TILE]
    low = (jnp.sum(seg[None, :] < firsts[:, None], axis=1) // TILE).astype(jnp.int32)
    past = jnp.sum(seg[None, :] <= lasts[:, None], axis=1)
    high = ((past + TILE - 1) // TILE).astype(jnp.int32)
    codes = jnp.broadcast_to(jnp.where(keep == 1, seg, -1)[:, None], (length, 128))
    seg_row = seg[None, :]

    b_q = b_qv[0].reshape(parts, part_width)
    b_v = b_qv[1].reshape(parts, part_width)
    bias = jnp.concatenate([b_q, jnp.zeros_like(b_q), b_v], axis=1)[:, None, :]
    projected = project(x, weights, bias)
    context, lse = attend(projected, low, high, codes, seg_row)
    zero = jnp.zeros_like(b_o)
    vectors = jnp.stack([b_o, gain_one, shift_one, b_down, gain_two, shift_two, zero, zero])
    out, hidden_low, second_low, first_low, grad_first, active, grad_up, grad_context, sums, upsum = (
        rows_pass(x, context, grads, weights, vectors, b_up.reshape(parts, 1, units))
    )
    if linked:
        swapped = lax.ppermute(out.reshape(parts, -1, out.shape[1])[1 - rank], "tensor", ((0, 1), (1, 0)))
    partial_up = outer(hidden_low, grad_up)
    partial_down = outer(second_low, active)
    grad_q, grad_k, grad_v, qsum, vsum = attend_back(
        projected, context, grad_context, lse, low, high, codes, seg_row
    )
    partial_a = outer_four(x, first_low, grad_q, grad_k, grad_v, context)
    x_whole = input_grad(grad_first, grad_q, grad_k, grad_v, weights)
    small = jnp.concatenate(
        [sums[:6].reshape(-1), qsum.reshape(-1), vsum.reshape(-1), upsum.reshape(-1)]
    )
    if linked:
        halves = x_whole.reshape(parts, -1, x_whole.shape[1])
        own, x_rows, small = reduce_all(partial_a, partial_up, partial_down, halves, small)
        mine = out.reshape(parts, -1, out.shape[1])[rank]
        out_rows = jnp.where(rank == 0, jnp.stack([mine, swapped]), jnp.stack([swapped, mine]))
    else:
        own = jnp.stack(
            [scatter_grads(g).astype(F32) for g in (partial_a, partial_up, partial_down)]
        )
        x_rows = trade_out(x_whole)
        out_rows = trade_out(out)
        small = lax.psum(small, ("dp", "tensor"))
    width = sums.shape[1]
    vec = small[: 6 * width].reshape(6, width)
    flat = parts * part_width
    start = 6 * width
    q_all = lax.dynamic_slice(small, (start + rank * part_width,), (part_width,))
    v_all = lax.dynamic_slice(small, (start + flat + rank * part_width,), (part_width,))
    up_all = lax.dynamic_slice(small, (start + 2 * flat + rank * units,), (units,))

    own_a = own[0]
    qkv_grad = jnp.stack([own_a[:, c * part_width : (c + 1) * part_width] for c in range(3)])
    return (
        out_rows[:, None],
        x_rows.astype(F32)[:, None],
        qkv_grad,
        jnp.stack([q_all, v_all]),
        own_a[:, 3 * part_width :].T,
        vec[0],
        vec[1],
        vec[2],
        own[1],
        up_all,
        own[2].T,
        vec[3],
        vec[4],
        vec[5],
    )


def solution(mesh):
    placed = (
        P(None, "dp", "tensor", None),
        P(None, "dp", None),
        P(None, "dp", None),
        P(None, "dp", "tensor"),
        P(),
        P("tensor", "dp"),
        P(),
        P(),
        P(),
        P("dp", "tensor"),
        P(),
        P("tensor", "dp"),
        P(),
        P(),
        P(),
        P(None, "dp", "tensor", None),
    )
    return jax.shard_map(
        shards,
        mesh=mesh,
        in_specs=placed,
        out_specs=(
            P(None, "dp", "tensor", None),
            P(None, "dp", "tensor", None),
            P(None, "dp", "tensor"),
            P(None, "tensor"),
            P("tensor", "dp"),
            P(),
            P(),
            P(),
            P("dp", "tensor"),
            P("tensor"),
            P("tensor", "dp"),
            P(),
            P(),
            P(),
        ),
        check_vma=False,
    )
```

```python
import math
import functools
import jax
import jax.numpy as jnp
from jax import lax
from jax.sharding import PartitionSpec as P
from jax.experimental import pallas as pl
from jax.experimental.pallas import tpu as pltpu

HEAD_DIM = 64
EPS = 1e-06
F32 = jnp.float32
BF16 = jnp.bfloat16
VMEM_MOST = 60 * 1024 * 1024


def dot_nn(a, b):
    return lax.dot_general(a, b, (((1,), (0,)), ((), ())), preferred_element_type=F32)


def dot_nt(a, b):
    return lax.dot_general(a, b, (((1,), (1,)), ((), ())), preferred_element_type=F32)


def dot_tn(a, b):
    return lax.dot_general(a, b, (((0,), (0,)), ((), ())), preferred_element_type=F32)


def params(**more):
    return pltpu.CompilerParams(vmem_limit_bytes=VMEM_MOST, **more)


def qkv_kernel(x_ref, w_ref, bias_ref, out_ref):
    rows = x_ref.shape[0]
    step = min(256, rows)
    for start in range(0, rows, step):
        part = dot_nn(x_ref[start : start + step, :], w_ref[0, 0]) + bias_ref[0]
        out_ref[0, start : start + step, :] = part.astype(BF16)


def project(x, weights, bias):
    rows, width = x.shape
    parts, _, _, cols = weights.shape
    wide = bias.shape[-1]
    return pl.pallas_call(
        qkv_kernel,
        grid=(parts,),
        in_specs=[
            pl.BlockSpec((rows, width), lambda t: (0, 0)),
            pl.BlockSpec((1, 1, width, wide), lambda t: (t, 0, 0, 0)),
            pl.BlockSpec((1, 1, wide), lambda t: (t, 0, 0)),
        ],
        out_specs=pl.BlockSpec((1, rows, wide), lambda t: (t, 0, 0)),
        out_shape=jax.ShapeDtypeStruct((parts, rows, wide), BF16),
        compiler_params=params(),
        name="project",
    )(x, weights, bias)


TILE = 256
DOC_MOST = 512
REACH = -(-(DOC_MOST - 1) // TILE)


def allowed_tile(code_ref, seg_ref, key0, query0):
    codes = code_ref[pl.ds(key0, TILE), :]
    codes = jnp.concatenate([codes] * (TILE // codes.shape[1]), axis=1)
    same = codes == seg_ref[:, pl.ds(query0, TILE)]
    key_pos = key0 + lax.broadcasted_iota(jnp.int32, (TILE, TILE), 0)
    query_pos = query0 + lax.broadcasted_iota(jnp.int32, (TILE, TILE), 1)
    return same | (key_pos == query_pos)


def head_masks(lanes):
    lane = lax.broadcasted_iota(jnp.int32, (1, lanes), 1)
    return [(lane // HEAD_DIM == h).astype(BF16) for h in range(lanes // HEAD_DIM)]


def attend_kernel(
    low_ref, high_ref, code_ref, seg_ref, q_ref, k_ref, v_ref, ctx_ref, lse_ref, top, den, acc
):
    rows, lanes = q_ref.shape[1], q_ref.shape[2]
    heads = lanes // HEAD_DIM
    masks = head_masks(lanes)

    @pl.loop(0, rows // TILE)
    def _(qi):
        query0 = pl.multiple_of(qi * TILE, TILE)
        queries = q_ref[0, pl.ds(query0, TILE), :] * BF16(0.125)
        each = [queries * masks[h] for h in range(heads)]
        top[...] = jnp.full_like(top, -1e30)
        den[...] = jnp.zeros_like(den)
        acc[...] = jnp.zeros_like(acc)

        @pl.loop(low_ref[qi], high_ref[qi])
        def _(ki):
            key0 = pl.multiple_of(ki * TILE, TILE)
            allowed = allowed_tile(code_ref, seg_ref, key0, query0)
            keys = k_ref[0, pl.ds(key0, TILE), :]
            values_t = v_ref[0, pl.ds(key0, TILE), :].T
            for h in range(heads):
                scores = jnp.where(allowed, dot_nt(keys, each[h]), -1e30)
                old = top[h]
                new = jnp.maximum(old, jnp.max(scores, axis=0, keepdims=True))
                expo = jnp.exp(scores - new)
                shrink = jnp.exp(old - new)
                top[h] = new
                den[h] = den[h] * shrink + jnp.sum(expo, axis=0, keepdims=True)
                part = dot_nn(values_t[h * HEAD_DIM : (h + 1) * HEAD_DIM], expo.astype(BF16))
                acc[h] = acc[h] * shrink + part

        both = jnp.concatenate([acc[h] / den[h] for h in range(heads)], axis=0)
        ctx_ref[0, pl.ds(query0, TILE), :] = both.astype(BF16).T
        for h in range(heads):
            lse_ref[0, h : h + 1, pl.ds(query0, TILE)] = top[h] + jnp.log(den[h])


def attend(projected, low, high, codes, seg_row):
    parts, rows, wide = projected.shape
    lanes = 128
    heads = lanes // HEAD_DIM
    groups = wide // 3 // lanes
    return pl.pallas_call(
        attend_kernel,
        grid_spec=pltpu.PrefetchScalarGridSpec(
            num_scalar_prefetch=2,
            grid=(parts, groups),
            in_specs=[
                pl.BlockSpec((rows, 128), lambda t, j, lo, hi: (0, 0)),
                pl.BlockSpec((1, rows), lambda t, j, lo, hi: (0, 0)),
                pl.BlockSpec((1, rows, lanes), lambda t, j, lo, hi: (t, 0, j)),
                pl.BlockSpec((1, rows, lanes), lambda t, j, lo, hi: (t, 0, groups + j)),
                pl.BlockSpec((1, rows, lanes), lambda t, j, lo, hi: (t, 0, 2 * groups + j)),
            ],
            out_specs=[
                pl.BlockSpec((1, rows, lanes), lambda t, j, lo, hi: (t, 0, j)),
                pl.BlockSpec((1, heads, rows), lambda t, j, lo, hi: (t * groups + j, 0, 0)),
            ],
            scratch_shapes=[
                pltpu.VMEM((heads, 1, TILE), F32),
                pltpu.VMEM((heads, 1, TILE), F32),
                pltpu.VMEM((heads, HEAD_DIM, TILE), F32),
            ],
        ),
        out_shape=[
            jax.ShapeDtypeStruct((parts, rows, wide // 3), BF16),
            jax.ShapeDtypeStruct((parts * groups, heads, rows), F32),
        ],
        compiler_params=params(),
        name="attend",
    )(low, high, codes, seg_row, projected, projected, projected)


def attend_back_kernel(
    low_ref,
    high_ref,
    code_ref,
    seg_ref,
    q_ref,
    k_ref,
    v_ref,
    ctx_ref,
    g_ref,
    lse_ref,
    dq_ref,
    dk_ref,
    dv_ref,
    qsum_ref,
    vsum_ref,
    dq_acc,
    dk_acc,
    dv_acc,
):
    rows, lanes = q_ref.shape[1], q_ref.shape[2]
    heads = lanes // HEAD_DIM
    masks = head_masks(lanes)
    dk_acc[...] = jnp.zeros_like(dk_acc)
    dv_acc[...] = jnp.zeros_like(dv_acc)

    @pl.loop(0, rows // TILE)
    def _(qi):
        query0 = pl.multiple_of(qi * TILE, TILE)
        queries = q_ref[0, pl.ds(query0, TILE), :] * BF16(0.125)
        grads = g_ref[0, pl.ds(query0, TILE), :]
        prod_t = (grads.astype(F32) * ctx_ref[0, pl.ds(query0, TILE), :].astype(F32)).T
        q_each = [queries * masks[h] for h in range(heads)]
        g_each = [grads * masks[h] for h in range(heads)]
        inner = [
            jnp.sum(prod_t[h * HEAD_DIM : (h + 1) * HEAD_DIM], axis=0, keepdims=True)
            for h in range(heads)
        ]
        lse = [lse_ref[0, h : h + 1, pl.ds(query0, TILE)] for h in range(heads)]
        dq_acc[...] = jnp.zeros_like(dq_acc)

        @pl.loop(low_ref[qi], high_ref[qi])
        def _(ki):
            key0 = pl.multiple_of(ki * TILE, TILE)
            allowed = allowed_tile(code_ref, seg_ref, key0, query0)
            keys = k_ref[0, pl.ds(key0, TILE), :]
            values = v_ref[0, pl.ds(key0, TILE), :]
            keys_t = keys.T
            dk = dk_acc[pl.ds(key0, TILE), :]
            dv = dv_acc[pl.ds(key0, TILE), :]
            for h in range(heads):
                scores = jnp.where(allowed, dot_nt(keys, q_each[h]), -1e30)
                probs = jnp.exp(scores - lse[h])
                gprobs = dot_nt(values, g_each[h])
                gscores = (probs * (gprobs - inner[h])).astype(BF16)
                dv = dv + dot_nn(probs.astype(BF16), g_each[h])
                dk = dk + dot_nn(gscores, q_each[h])
                lanes_h = slice(h * HEAD_DIM, (h + 1) * HEAD_DIM)
                dq_acc[h] += dot_nn(keys_t[lanes_h], gscores)
            dk_acc[pl.ds(key0, TILE), :] = dk
            dv_acc[pl.ds(key0, TILE), :] = dv

        both = jnp.concatenate([dq_acc[h] for h in range(heads)], axis=0) * 0.125
        dq_ref[0, pl.ds(query0, TILE), :] = both.astype(BF16).T

    low_k = dk_acc[...].astype(BF16)
    low_v = dv_acc[...].astype(BF16)
    dk_ref[0] = low_k
    dv_ref[0] = low_v
    qsum_ref[0] = jnp.sum(dq_ref[0].astype(F32), axis=0, keepdims=True)
    vsum_ref[0] = jnp.sum(low_v.astype(F32), axis=0, keepdims=True)


def attend_back(projected, context, grad_context, lse, low, high, codes, seg_row):
    parts, rows, wide = projected.shape
    lanes = 128
    heads = lanes // HEAD_DIM
    groups = wide // 3 // lanes
    flat = pl.BlockSpec((1, rows, lanes), lambda t, j, lo, hi: (t, 0, j))
    sums = pl.BlockSpec((1, 1, lanes), lambda t, j, lo, hi: (t, 0, j))
    return pl.pallas_call(
        attend_back_kernel,
        grid_spec=pltpu.PrefetchScalarGridSpec(
            num_scalar_prefetch=2,
            grid=(parts, groups),
            in_specs=[
                pl.BlockSpec((rows, 128), lambda t, j, lo, hi: (0, 0)),
                pl.BlockSpec((1, rows), lambda t, j, lo, hi: (0, 0)),
                pl.BlockSpec((1, rows, lanes), lambda t, j, lo, hi: (t, 0, j)),
                pl.BlockSpec((1, rows, lanes), lambda t, j, lo, hi: (t, 0, groups + j)),
                pl.BlockSpec((1, rows, lanes), lambda t, j, lo, hi: (t, 0, 2 * groups + j)),
                flat,
                flat,
                pl.BlockSpec((1, heads, rows), lambda t, j, lo, hi: (t * groups + j, 0, 0)),
            ],
            out_specs=[flat, flat, flat, sums, sums],
            scratch_shapes=[
                pltpu.VMEM((heads, HEAD_DIM, TILE), F32),
                pltpu.VMEM((rows, lanes), F32),
                pltpu.VMEM((rows, lanes), F32),
            ],
        ),
        out_shape=[jax.ShapeDtypeStruct((parts, rows, wide // 3), BF16)] * 3
        + [jax.ShapeDtypeStruct((parts, 1, wide // 3), F32)] * 2,
        compiler_params=params(),
        name="attend_back",
    )(low, high, codes, seg_row, projected, projected, projected, context, grad_context, lse)


def norm_forward(v):
    mean = jnp.mean(v, axis=-1, keepdims=True)
    centered = v - mean
    factor = lax.rsqrt(jnp.mean(centered * centered, axis=-1, keepdims=True) + EPS)
    return centered * factor, factor


def norm_back(inner, normed, factor):
    return factor * (
        inner
        - jnp.mean(inner, axis=-1, keepdims=True)
        - normed * jnp.mean(inner * normed, axis=-1, keepdims=True)
    )


def col_sum(v):
    return jnp.sum(v, axis=0, keepdims=True)


UNIT_STEP = 512


def rows_kernel(
    x_ref,
    ctx_ref,
    g_ref,
    wo_ref,
    up_ref,
    down_ref,
    vec_ref,
    bup_ref,
    out_ref,
    hid_ref,
    sec_ref,
    first_ref,
    gfirst_ref,
    act_ref,
    gup_ref,
    gctx_ref,
    sums_ref,
    upsum_ref,
    slope,
):
    parts, _, units = act_ref.shape

    @pl.when(pl.program_id(0) == 0)
    def _():
        sums_ref[...] = jnp.zeros_like(sums_ref)
        upsum_ref[...] = jnp.zeros_like(upsum_ref)

    b_o, gain_one, shift_one = vec_ref[0:1], vec_ref[1:2], vec_ref[2:3]
    b_down, gain_two, shift_two = vec_ref[3:4], vec_ref[4:5], vec_ref[5:6]
    first_sum = x_ref[...].astype(F32) + b_o
    for t in range(parts):
        first_sum = first_sum + dot_nt(ctx_ref[t], wo_ref[t, 0])
    normed_one, factor_one = norm_forward(first_sum)
    hidden = normed_one * gain_one + shift_one
    hidden_low = hidden.astype(BF16)
    hid_ref[...] = hidden_low
    second_sum = hidden + b_down
    for t in range(parts):
        for u in range(0, units, UNIT_STEP):
            at = slice(u, u + UNIT_STEP)
            up = dot_nn(hidden_low, up_ref[t, 0, :, at]) + bup_ref[t, :, at]
            half = 0.5 * (1.0 + lax.erf(up * 0.7071067811865476))
            active = (up * half).astype(BF16)
            act_ref[t, :, at] = active
            slope[t, :, at] = half + up * jnp.exp(-0.5 * up * up) * 0.3989422804014327
            second_sum = second_sum + dot_nt(active, down_ref[t, 0, :, at])
    normed_two, factor_two = norm_forward(second_sum)
    out_ref[...] = (normed_two * gain_two + shift_two).astype(BF16)
    grad_out = g_ref[...].astype(F32)
    grad_second = norm_back(grad_out * gain_two, normed_two, factor_two)
    second_low = grad_second.astype(BF16)
    sec_ref[...] = second_low
    grad_hidden = grad_second
    for t in range(parts):
        for u in range(0, units, UNIT_STEP):
            at = slice(u, u + UNIT_STEP)
            grad_up = (dot_nn(second_low, down_ref[t, 0, :, at]) * slope[t, :, at]).astype(BF16)
            gup_ref[t, :, at] = grad_up
            upsum_ref[t, :, at] += col_sum(grad_up.astype(F32))
            grad_hidden = grad_hidden + dot_nt(grad_up, up_ref[t, 0, :, at])
    grad_first = norm_back(grad_hidden * gain_one, normed_one, factor_one)
    gfirst_ref[...] = grad_first
    first_low = grad_first.astype(BF16)
    first_ref[...] = first_low
    for t in range(parts):
        gctx_ref[t] = dot_nn(first_low, wo_ref[t, 0]).astype(BF16)
    sums_ref[0:1] += col_sum(grad_first)
    sums_ref[1:2] += col_sum(grad_hidden * normed_one)
    sums_ref[2:3] += col_sum(grad_hidden)
    sums_ref[3:4] += col_sum(grad_second)
    sums_ref[4:5] += col_sum(grad_out * normed_two)
    sums_ref[5:6] += col_sum(grad_out)


def rows_pass(x, context, grads, first, rest, vectors, bias_up):
    rows, width = x.shape
    parts, _, _, units = rest.shape
    part_width = context.shape[2]
    step = min(256, rows)
    row = pl.BlockSpec((step, width), lambda i: (i, 0))
    split = pl.BlockSpec((parts, step, part_width), lambda i: (0, i, 0))
    wide = pl.BlockSpec((parts, step, units), lambda i: (0, i, 0))
    once = pl.Buffered(1)
    last = units // part_width - 1
    return pl.pallas_call(
        rows_kernel,
        grid=(rows // step,),
        in_specs=[
            row,
            split,
            row,
            pl.BlockSpec(
                (parts, 1, width, part_width), lambda i: (0, 0, 0, last), pipeline_mode=once
            ),
            pl.BlockSpec((parts, 1, width, units), lambda i: (0, 0, 0, 0), pipeline_mode=once),
            pl.BlockSpec((parts, 1, width, units), lambda i: (0, 1, 0, 0), pipeline_mode=once),
            pl.BlockSpec((8, width), lambda i: (0, 0)),
            pl.BlockSpec((parts, 1, units), lambda i: (0, 0, 0)),
        ],
        out_specs=[
            row,
            row,
            row,
            row,
            row,
            wide,
            wide,
            split,
            pl.BlockSpec((8, width), lambda i: (0, 0)),
            pl.BlockSpec((parts, 1, units), lambda i: (0, 0, 0)),
        ],
        out_shape=[
            jax.ShapeDtypeStruct((rows, width), BF16),
            jax.ShapeDtypeStruct((rows, width), BF16),
            jax.ShapeDtypeStruct((rows, width), BF16),
            jax.ShapeDtypeStruct((rows, width), BF16),
            jax.ShapeDtypeStruct((rows, width), F32),
            jax.ShapeDtypeStruct((parts, rows, units), BF16),
            jax.ShapeDtypeStruct((parts, rows, units), BF16),
            jax.ShapeDtypeStruct((parts, rows, part_width), BF16),
            jax.ShapeDtypeStruct((8, width), F32),
            jax.ShapeDtypeStruct((parts, 1, units), F32),
        ],
        scratch_shapes=[pltpu.VMEM((parts, step, units), F32)],
        compiler_params=params(),
        name="rows_pass",
    )(x, context, grads, first, rest, rest, vectors, bias_up)


GRAD_STEP = 256


def outer_kernel(rows_ref, cols_ref, out_ref):
    width = rows_ref.shape[1]
    for m in range(0, width, GRAD_STEP):
        at = slice(m, m + GRAD_STEP)
        out_ref[0, at, :] = dot_tn(rows_ref[:, at], cols_ref[0]).astype(BF16)


def outer(left, right):
    rows, width = left.shape
    parts, _, units = right.shape
    return pl.pallas_call(
        outer_kernel,
        grid=(parts,),
        in_specs=[
            pl.BlockSpec((rows, width), lambda t: (0, 0)),
            pl.BlockSpec((1, rows, units), lambda t: (t, 0, 0)),
        ],
        out_specs=pl.BlockSpec((1, width, units), lambda t: (t, 0, 0)),
        out_shape=jax.ShapeDtypeStruct((parts, width, units), BF16),
        compiler_params=params(),
        name="outer",
    )(left, right)


def outer_four_kernel(x_ref, first_ref, q_ref, k_ref, v_ref, ctx_ref, out_ref):
    width = x_ref.shape[1]
    part_width = q_ref.shape[2]
    for m in range(0, width, GRAD_STEP):
        at = slice(m, m + GRAD_STEP)
        for n, cols in enumerate((q_ref, k_ref, v_ref, ctx_ref)):
            left = first_ref if n == 3 else x_ref
            part = dot_tn(left[:, at], cols[0])
            out_ref[0, at, n * part_width : (n + 1) * part_width] = part.astype(BF16)


def outer_four(x, first_low, grad_q, grad_k, grad_v, context):
    rows, width = x.shape
    parts, _, part_width = context.shape
    row = pl.BlockSpec((rows, width), lambda t: (0, 0))
    split = pl.BlockSpec((1, rows, part_width), lambda t: (t, 0, 0))
    return pl.pallas_call(
        outer_four_kernel,
        grid=(parts,),
        in_specs=[row, row, split, split, split, split],
        out_specs=pl.BlockSpec((1, width, 4 * part_width), lambda t: (t, 0, 0)),
        out_shape=jax.ShapeDtypeStruct((parts, width, 4 * part_width), BF16),
        compiler_params=params(),
        name="outer_four",
    )(x, first_low, grad_q, grad_k, grad_v, context)


def input_grad_kernel(base_ref, q_ref, k_ref, v_ref, w_ref, out_ref):
    parts, _, part_width = q_ref.shape
    total = base_ref[...]
    for t in range(parts):
        for c, cols in enumerate((q_ref, k_ref, v_ref)):
            at = slice(c * part_width, (c + 1) * part_width)
            total = total + dot_nt(cols[t], w_ref[t, 0, :, at])
    out_ref[...] = total.astype(out_ref.dtype)


def input_grad(grad_first, grad_q, grad_k, grad_v, weights):
    rows, width = grad_first.shape
    parts, _, part_width = grad_q.shape
    step = min(256, rows)
    row = pl.BlockSpec((step, width), lambda i: (i, 0))
    split = pl.BlockSpec((parts, step, part_width), lambda i: (0, i, 0))
    return pl.pallas_call(
        input_grad_kernel,
        grid=(rows // step,),
        in_specs=[
            row,
            split,
            split,
            split,
            pl.BlockSpec((parts, 1, width, 3 * part_width), lambda i: (0, 0, 0, 0)),
        ],
        out_specs=row,
        out_shape=jax.ShapeDtypeStruct((rows, width), BF16),
        compiler_params=params(),
        name="input_grad",
    )(grad_first, grad_q, grad_k, grad_v, weights)


LINE = 4
REDUCE_MIXED = (1, 0, 1)


class Place:
    def __init__(self):
        dp = lax.axis_index("dp")
        self.y = lax.axis_index("tensor")
        self.core = lax.rem(dp, 2)
        self.x = lax.rem(lax.div(dp, 2), 2)
        self.z = lax.div(dp, 4)

    @staticmethod
    def at(z, x, core, y):
        return ((z * 2 + x) * 2 + core, y)

    def corners(self, mixed, core=None):
        core = self.core if core is None else core
        side = 1 - (1 - core) * mixed
        first = (lax.rem(self.y + side, 2), lax.rem(self.x + 1 - side, 2))
        second = (lax.rem(self.y + 1 - side, 2), lax.rem(self.x + side, 2))
        return ((self.y, self.x), first, second, (1 - self.y, 1 - self.x))

    def chip(self, corner):
        return self.at(self.z, corner[1], self.core, corner[0])

    def along(self, o):
        return lax.rem(self.z + o, LINE)

    def back(self, o):
        return lax.rem(self.z + LINE - o, LINE)

    def line(self, o):
        return self.at(self.along(o), self.x, self.core, self.y)

    def partner(self):
        return self.at(self.z, self.x, 1 - self.core, self.y)

    def across_x(self):
        return self.at(self.z, 1 - self.x, self.core, self.y)

    def across_y(self):
        return self.at(self.z, self.x, self.core, 1 - self.y)

    def greet(self):
        barrier = pltpu.get_barrier_semaphore()
        others = [self.across_x(), self.across_y(), self.partner()]
        others += [self.line(o) for o in range(1, LINE)]
        for device in others:
            pl.semaphore_signal(
                barrier, inc=1, device_id=device, device_id_type=pl.DeviceIdType.MESH
            )
        pl.semaphore_wait(barrier, len(others))


def remote(src, dst, sends, recvs, slot, device):
    return pltpu.make_async_remote_copy(
        src_ref=src,
        dst_ref=dst,
        send_sem=sends.at[slot],
        recv_sem=recvs.at[slot],
        device_id=device,
        device_id_type=pl.DeviceIdType.MESH,
    )


PER_PIECE = 8


def gather_kernel(
    shard_ref,
    in_ref,
    bias_ref,
    code_ref,
    seg_ref,
    first_ref,
    rest_ref,
    x_ref,
    proj_ref,
    ctx_ref,
    lse_ref,
    sends,
    recvs,
    local_sem,
    top,
    den,
    acc,
):
    place = Place()
    z, x, y, core = place.z, place.x, place.y, place.core
    chunks = shard_ref.shape[0]
    parts, rows, wide = proj_ref.shape
    last = chunks * LINE * PER_PIECE
    place.greet()

    def copy(k, o, n, src, dst, device):
        return remote(src, dst, sends, recvs, (k * LINE + o) * PER_PIECE + n, device)

    def slot(k, yy, zz, xx, cc):
        if isinstance(k, int) and k == 0:
            return first_ref.at[yy, zz, xx, cc]
        return rest_ref.at[yy, k - 1, zz, xx, cc]

    def where(k, cc=None):
        mixed = (k + 1) % 2 if isinstance(k, int) else lax.rem(k + 1, 2)
        return place.corners(mixed, cc)

    def held(k, o, corner, cc=core):
        return slot(k, corner[0], place.back(o), corner[1], cc)

    def to_line(k, o):
        here = slot(k, y, z, x, core)
        return copy(k, o, 0, shard_ref.at[k], here, place.line(o))

    def from_line(k, o):
        here = held(k, o, (y, x))
        return copy(k, o, 0, here, here, place.line(o))

    def hop(k, o, n, corner, device):
        here = held(k, o, where(k)[corner])
        return copy(k, o, n, here, here, device)

    def to_first(k, o):
        return hop(k, o, 1, 0, place.chip(where(k)[1]))

    def from_first(k, o):
        return hop(k, o, 1, 1, place.chip(where(k)[1]))

    def to_second(k, o, n):
        return hop(k, o, 2 + n, n, place.chip(where(k)[2]))

    def from_second(k, o, n):
        return hop(k, o, 2 + n, 2 + n, place.chip(where(k)[2]))

    def to_partner(k, o, n):
        return hop(k, o, 4 + n, n, place.partner())

    def from_partner(k, o, n):
        here = held(k, o, where(k, 1 - core)[n], 1 - core)
        return copy(k, o, 4 + n, here, here, place.partner())

    trade = remote(in_ref.at[1 - y], x_ref.at[y], sends, recvs, last, place.across_y())
    arrive = remote(in_ref.at[y], x_ref.at[1 - y], sends, recvs, last, place.across_y())
    local = [pltpu.make_async_copy(in_ref.at[y], x_ref.at[y], local_sem.at[chunks])]
    for k in range(chunks):
        own = slot(k, y, z, x, core)
        local.append(pltpu.make_async_copy(shard_ref.at[k], own, local_sem.at[k]))
    for part in local:
        part.start()
    for k in range(chunks):
        for o in (2, 1, 3):
            to_line(k, o).start()
    for part in local:
        part.wait()

    def start_line(k, o):
        to_first(k, o).start()
        to_second(k, o, 0).start()
        to_partner(k, o, 0).start()

    def arrive_first(k, o):
        from_first(k, o).wait_recv()
        to_second(k, o, 1).start()
        to_partner(k, o, 1).start()

    def arrive_second(k, o):
        for n in range(2):
            from_second(k, o, n).wait_recv()
            to_partner(k, o, 2 + n).start()

    order = (0, 1, 3, 2)
    for i in range(LINE + 2):
        if i < LINE:
            if order[i] > 0:
                from_line(0, order[i]).wait_recv()
            start_line(0, order[i])
            if i == 0:
                trade.start()
        if 0 <= i - 1 < LINE:
            arrive_first(0, order[i - 1])
        if 0 <= i - 2 < LINE:
            arrive_second(0, order[i - 2])
    arrive.wait_recv()
    for o in order:
        for n in range(4):
            from_partner(0, o, n).wait_recv()

    step = 256
    for t in range(parts):
        @pl.loop(0, rows // step)
        def _(i):
            half = lax.div(i, 2)
            row0 = pl.multiple_of(lax.rem(i, 2) * step, step)
            left = x_ref[half, pl.ds(row0, step), :]
            right = first_ref[t, :, :, :, :, :wide].reshape(-1, wide)
            value = dot_nn(left, right) + bias_ref[t]
            proj_ref[t, pl.ds(pl.multiple_of(i * step, step), step), :] = value.astype(BF16)

    lanes = 128
    groups = wide // 3 // lanes
    heads = lanes // HEAD_DIM
    tiles = rows // TILE
    masks = head_masks(lanes)

    def attend_slice(i):
        group = lax.div(i, tiles)
        qi = lax.rem(i, tiles)
        t = lax.div(group, groups)
        j = lax.rem(group, groups)
        query0 = pl.multiple_of(qi * TILE, TILE)

        def lane(c):
            return pl.ds(pl.multiple_of((c * groups + j) * lanes, lanes), lanes)

        queries = proj_ref[t, pl.ds(query0, TILE), lane(0)] * BF16(0.125)
        each = [queries * masks[h] for h in range(heads)]
        top[...] = jnp.full_like(top, -1e30)
        den[...] = jnp.zeros_like(den)
        acc[...] = jnp.zeros_like(acc)

        @pl.loop(jnp.maximum(qi - REACH, 0), jnp.minimum(qi + REACH + 1, tiles))
        def _(ki):
            key0 = pl.multiple_of(ki * TILE, TILE)
            allowed = allowed_tile(code_ref, seg_ref, key0, query0)
            keys = proj_ref[t, pl.ds(key0, TILE), lane(1)]
            values_t = proj_ref[t, pl.ds(key0, TILE), lane(2)].T
            for h in range(heads):
                scores = jnp.where(allowed, dot_nt(keys, each[h]), -1e30)
                old = top[h]
                new = jnp.maximum(old, jnp.max(scores, axis=0, keepdims=True))
                expo = jnp.exp(scores - new)
                shrink = jnp.exp(old - new)
                top[h] = new
                den[h] = den[h] * shrink + jnp.sum(expo, axis=0, keepdims=True)
                part = dot_nn(values_t[h * HEAD_DIM : (h + 1) * HEAD_DIM], expo.astype(BF16))
                acc[h] = acc[h] * shrink + part

        both = jnp.concatenate([acc[h] / den[h] for h in range(heads)], axis=0)
        ctx_ref[t, pl.ds(query0, TILE), lane(0)] = both.astype(BF16).T
        for h in range(heads):
            lse_ref[group, h : h + 1, pl.ds(query0, TILE)] = top[h] + jnp.log(den[h])

    count = (chunks - 1) * LINE
    slices = parts * groups * tiles
    share = slices // count

    def split(p):
        k = 1 + lax.div(p, LINE)
        r = lax.rem(p, LINE)
        return k, jnp.where(r < 2, r, 5 - r)

    @pl.loop(0, count + 2)
    def _(p):
        @pl.when(p < count)
        def _():
            k, o = split(p)

            @pl.when(o > 0)
            def _():
                from_line(k, o).wait_recv()

            start_line(k, o)

        @pl.when((p >= 1) & (p <= count))
        def _():
            arrive_first(*split(p - 1))

        @pl.when(p >= 2)
        def _():
            arrive_second(*split(p - 2))

        @pl.when(p < count)
        def _():
            @pl.loop(0, share)
            def _(n):
                attend_slice(p * share + n)

    @pl.loop(0, count)
    def _(p):
        k, o = split(p)
        for n in range(4):
            from_partner(k, o, n).wait_recv()

    @pl.loop(0, count)
    def _(p):
        k, o = split(p)

        @pl.when(o > 0)
        def _():
            to_line(k, o).wait_send()

        to_first(k, o).wait_send()
        for n in range(2):
            to_second(k, o, n).wait_send()
        for n in range(4):
            to_partner(k, o, n).wait_send()

    for o in order:
        if o > 0:
            to_line(0, o).wait_send()
        to_first(0, o).wait_send()
        for n in range(2):
            to_second(0, o, n).wait_send()
        for n in range(4):
            to_partner(0, o, n).wait_send()
    trade.wait_send()


def gather_all(shard, halves, bias, codes, seg_row):
    chunks, own_rows, units = shard.shape
    parts, rows, width = halves.shape
    wide = bias.shape[-1]
    length = parts * rows
    groups = wide // 3 // 128
    anywhere = pl.BlockSpec(memory_space=pl.ANY)
    local = pl.BlockSpec(memory_space=pltpu.VMEM)
    copies = chunks * LINE * PER_PIECE + 1
    places = (LINE, 2, 2, own_rows, units)
    first, rest, x, projected, context, lse = pl.pallas_call(
        gather_kernel,
        in_specs=[local] * 5,
        out_specs=[local, anywhere, local, local, local, local],
        out_shape=[
            jax.ShapeDtypeStruct((parts,) + places, BF16),
            jax.ShapeDtypeStruct((parts, chunks - 1) + places, BF16),
            jax.ShapeDtypeStruct((parts, rows, width), BF16),
            jax.ShapeDtypeStruct((parts, length, wide), BF16),
            jax.ShapeDtypeStruct((parts, length, wide // 3), BF16),
            jax.ShapeDtypeStruct((parts * groups, 2, length), F32),
        ],
        scratch_shapes=[
            pltpu.SemaphoreType.DMA((copies,)),
            pltpu.SemaphoreType.DMA((copies,)),
            pltpu.SemaphoreType.DMA((chunks + 1,)),
            pltpu.VMEM((2, 1, TILE), F32),
            pltpu.VMEM((2, 1, TILE), F32),
            pltpu.VMEM((2, HEAD_DIM, TILE), F32),
        ],
        compiler_params=params(collective_id=0, has_side_effects=True),
        name="gather_all",
    )(shard, halves, bias, codes, seg_row)
    first = first.reshape(parts, 1, -1, units)
    rest = rest.reshape(parts, chunks - 1, -1, units)
    return first, rest, x.reshape(length, width), projected, context, lse


def reduce_kernel(
    a_ref,
    b_ref,
    c_ref,
    xg_ref,
    small_ref,
    out_ref,
    xr_ref,
    total_ref,
    p_buf,
    s_buf,
    f_buf,
    z_buf,
    t_buf,
    sends,
    recvs,
    t_send,
    t_recv,
    local_sem,
):
    place = Place()
    z, x, y, core = place.z, place.x, place.y, place.core
    grads = (a_ref, b_ref, c_ref)
    chunks = len(grads)
    place.greet()

    def where(k):
        return place.corners(REDUCE_MIXED[k])

    def copy(k, o, n, src, dst, device):
        return remote(src, dst, sends, recvs, (k * LINE + o) * PER_PIECE + n, device)

    def to_partner(k, o):
        src = grads[k].at[:, place.along(o), :, 1 - core]
        return copy(k, o, 0, src, p_buf.at[k, o], place.partner())

    def to_second(k, o, n):
        yy, xx = where(k)[2 + n]
        device = place.chip(where(k)[2])
        return copy(k, o, 1 + n, p_buf.at[k, o, yy, xx], s_buf.at[k, o, n], device)

    def to_first(k, o):
        device = place.chip(where(k)[1])
        return copy(k, o, 3, s_buf.at[k, o, 1], f_buf.at[k, o], device)

    def to_line(k, o):
        return copy(k, o, 4, f_buf.at[k, o], z_buf.at[k, o - 1], place.line(o))

    def small_copy(n, src, dst, device):
        return remote(src, dst, t_send, t_recv, n, device)

    hops = (
        small_copy(0, small_ref, t_buf.at[0], place.partner()),
        small_copy(1, t_buf.at[1], t_buf.at[2], place.across_x()),
        small_copy(2, t_buf.at[3], t_buf.at[4], place.across_y()),
    )

    def small_line(o):
        return small_copy(2 + o, t_buf.at[5 + z], t_buf.at[5 + z], place.line(o))

    def small_from(o):
        here = t_buf.at[5 + place.back(o)]
        return small_copy(2 + o, here, here, place.line(o))

    def small_step(step):
        if step == 0:
            hops[0].start()
        elif step == 1:
            hops[0].wait_recv()
            t_buf[1] = small_ref[...] + t_buf[0]
            hops[1].start()
        elif step == 2:
            hops[1].wait_recv()
            t_buf[3] = t_buf[1] + t_buf[2]
            hops[2].start()
        elif step == 3:
            hops[2].wait_recv()
            t_buf[5 + z] = t_buf[3] + t_buf[4]
            for o in range(1, LINE):
                small_line(o).start()
        elif step == 4:
            for o in range(1, LINE):
                small_from(o).wait_recv()
            total_ref[...] = (t_buf[5] + t_buf[6]) + (t_buf[7] + t_buf[8])

    trade = small_copy(2 + LINE, xg_ref.at[1 - y], xr_ref.at[y], place.across_y())
    arrive = small_copy(2 + LINE, xg_ref.at[1 - y], xr_ref.at[1 - y], place.across_y())
    keep = pltpu.make_async_copy(xg_ref.at[y], xr_ref.at[y], local_sem.at[0])

    def stage_partner(k, o):
        to_partner(k, o).wait_recv()
        zz = place.along(o)
        for n in (3, 2, 1, 0):
            yy, xx = where(k)[n]
            p_buf[k, o, yy, xx] = p_buf[k, o, yy, xx] + grads[k][yy, zz, xx, core]
            if n >= 2:
                to_second(k, o, n - 2).start()

    def stage_second(k, o):
        for n in (1, 0):
            yy, xx = where(k)[n]
            to_second(k, o, n).wait_recv()
            s_buf[k, o, n] = s_buf[k, o, n] + p_buf[k, o, yy, xx]
            if n == 1:
                to_first(k, o).start()

    def stage_first(k, o):
        to_first(k, o).wait_recv()
        f_buf[k, o] = f_buf[k, o] + s_buf[k, o, 0]
        if o > 0:
            to_line(k, o).start()

    def finish(k):
        total = f_buf[k, 0].astype(F32)
        for o in range(1, LINE):
            to_line(k, o).wait_recv()
            total = total + z_buf[k, o - 1].astype(F32)
        out_ref[k] = total

    steps = [(k, o) for k in range(chunks) for o in (2, 1, 3, 0)]
    small_step(0)
    for k, o in steps:
        to_partner(k, o).start()
    keep.start()
    small_step(1)
    for i in range(len(steps) + 4):
        if i < len(steps):
            stage_partner(*steps[i])
        if i == 1:
            trade.start()
        if 0 <= i - 2 < len(steps):
            stage_second(*steps[i - 2])
        if 0 <= i - 4 < len(steps):
            stage_first(*steps[i - 4])
        if i in (3, 6, 9):
            small_step(1 + i // 3)
    for k in range(chunks):
        finish(k)

    keep.wait()
    trade.wait_send()
    arrive.wait_recv()
    for part in hops:
        part.wait_send()
    for o in range(1, LINE):
        small_line(o).wait_send()
    for k, o in steps:
        to_partner(k, o).wait_send()
        for n in range(2):
            to_second(k, o, n).wait_send()
        to_first(k, o).wait_send()
        if o > 0:
            to_line(k, o).wait_send()


def reduce_all(grads_a, grads_b, grads_c, halves, small):
    parts, width, units = grads_a.shape
    _, rows, model = halves.shape
    own_rows = width // (4 * LINE)
    chunks = 3
    folded = [g.reshape(parts, LINE, 2, 2, own_rows, units) for g in (grads_a, grads_b, grads_c)]
    small_rows = small.shape[0] // 128
    local = pl.BlockSpec(memory_space=pltpu.VMEM)
    piece = (own_rows, units)
    copies = chunks * LINE * PER_PIECE
    own, x_rows, total = pl.pallas_call(
        reduce_kernel,
        in_specs=[local] * 5,
        out_specs=[local, pl.BlockSpec(memory_space=pl.ANY), local],
        out_shape=[
            jax.ShapeDtypeStruct((chunks, own_rows, units), F32),
            jax.ShapeDtypeStruct((parts, rows, model), BF16),
            jax.ShapeDtypeStruct((small_rows, 128), F32),
        ],
        scratch_shapes=[
            pltpu.VMEM((chunks, LINE, 2, 2) + piece, BF16),
            pltpu.VMEM((chunks, LINE, 2) + piece, BF16),
            pltpu.VMEM((chunks, LINE) + piece, BF16),
            pltpu.VMEM((chunks, LINE - 1) + piece, BF16),
            pltpu.VMEM((5 + LINE, small_rows, 128), F32),
            pltpu.SemaphoreType.DMA((copies,)),
            pltpu.SemaphoreType.DMA((copies,)),
            pltpu.SemaphoreType.DMA((3 + LINE,)),
            pltpu.SemaphoreType.DMA((3 + LINE,)),
            pltpu.SemaphoreType.DMA((1,)),
        ],
        compiler_params=params(collective_id=1, has_side_effects=True),
        name="reduce_all",
    )(*folded, halves, small.reshape(small_rows, 128))
    return own, x_rows, total.reshape(-1)


def trade_in(halves):
    return lax.all_to_all(halves, "tensor", split_axis=0, concat_axis=1, tiled=True)[0]


def trade_out(whole):
    return lax.all_to_all(whole[None], "tensor", split_axis=1, concat_axis=0, tiled=True)


def gather_weights(shard):
    full = lax.all_gather(shard, "dp", axis=1, tiled=True)
    return lax.all_gather(full, "tensor", axis=0, tiled=False)


def scatter_grads(partial):
    own = lax.psum_scatter(partial, "tensor", scatter_dimension=0, tiled=False)
    return lax.psum_scatter(own, "dp", scatter_dimension=0, tiled=True)


def shards(
    inputs,
    seg_ids,
    keep_mask,
    w_qkv,
    b_qv,
    w_o,
    b_o,
    gain_one,
    shift_one,
    w_up,
    b_up,
    w_down,
    b_down,
    gain_two,
    shift_two,
    out_grad,
):
    parts = lax.axis_size("tensor")
    assert inputs.shape[0] == parts
    own_rows = w_qkv.shape[1]
    part_width = w_qkv.shape[2]
    units = w_up.shape[1]
    rank = lax.axis_index("tensor")

    shard_a = jnp.concatenate([w_qkv[0], w_qkv[1], w_qkv[2], w_o.T], axis=1)
    shard = jnp.stack([shard_a, w_up, w_down.T])
    seg = lax.dynamic_index_in_dim(seg_ids[:, 0], rank, 0, keepdims=False)
    keep = lax.dynamic_index_in_dim(keep_mask[:, 0], rank, 0, keepdims=False)
    length = seg.shape[0]
    firsts, lasts = seg[::TILE], seg[TILE - 1 :: TILE]
    low = (jnp.sum(seg[None, :] < firsts[:, None], axis=1) // TILE).astype(jnp.int32)
    past = jnp.sum(seg[None, :] <= lasts[:, None], axis=1)
    high = ((past + TILE - 1) // TILE).astype(jnp.int32)
    codes = jnp.broadcast_to(jnp.where(keep == 1, seg, -1)[:, None], (length, 128))
    seg_row = seg[None, :]

    b_q = b_qv[0].reshape(parts, part_width)
    b_v = b_qv[1].reshape(parts, part_width)
    bias = jnp.concatenate([b_q, jnp.zeros_like(b_q), b_v], axis=1)[:, None, :]
    linked = lax.axis_size("dp") == LINE * 4 and parts == 2
    if linked:
        first, rest, x, projected, context, lse = gather_all(
            shard, inputs[:, 0], bias, codes, seg_row
        )
        theirs = lax.ppermute(out_grad[1 - rank, 0], "tensor", ((0, 1), (1, 0)))
        own_half = out_grad[rank, 0]
        grads = jnp.concatenate([own_half, theirs])
        grads = jnp.where(rank == 0, grads, jnp.concatenate([theirs, own_half]))
    else:
        weights = gather_weights(shard)
        first, rest = weights[:, :1], weights[:, 1:]
        x = trade_in(inputs[:, 0])
        grads = trade_in(out_grad[:, 0])
        projected = project(x, first, bias)
        context, lse = attend(projected, low, high, codes, seg_row)
    zero = jnp.zeros_like(b_o)
    vectors = jnp.stack([b_o, gain_one, shift_one, b_down, gain_two, shift_two, zero, zero])
    out, hidden_low, second_low, first_low, grad_first, active, grad_up, grad_context, sums, upsum = (
        rows_pass(x, context, grads, first, rest, vectors, b_up.reshape(parts, 1, units))
    )
    if linked:
        swapped = lax.ppermute(out.reshape(parts, -1, out.shape[1])[1 - rank], "tensor", ((0, 1), (1, 0)))
    partial_up = outer(hidden_low, grad_up)
    partial_down = outer(second_low, active)
    grad_q, grad_k, grad_v, qsum, vsum = attend_back(
        projected, context, grad_context, lse, low, high, codes, seg_row
    )
    partial_a = outer_four(x, first_low, grad_q, grad_k, grad_v, context)
    x_whole = input_grad(grad_first, grad_q, grad_k, grad_v, first)
    small = jnp.concatenate(
        [sums[:6].reshape(-1), qsum.reshape(-1), vsum.reshape(-1), upsum.reshape(-1)]
    )
    if linked:
        halves = x_whole.reshape(parts, -1, x_whole.shape[1])
        own, x_rows, small = reduce_all(partial_a, partial_up, partial_down, halves, small)
        mine = out.reshape(parts, -1, out.shape[1])[rank]
        out_rows = jnp.where(rank == 0, jnp.stack([mine, swapped]), jnp.stack([swapped, mine]))
    else:
        own = jnp.stack(
            [scatter_grads(g).astype(F32) for g in (partial_a, partial_up, partial_down)]
        )
        x_rows = trade_out(x_whole)
        out_rows = trade_out(out)
        small = lax.psum(small, ("dp", "tensor"))
    width = sums.shape[1]
    vec = small[: 6 * width].reshape(6, width)
    flat = parts * part_width
    start = 6 * width
    q_all = lax.dynamic_slice(small, (start + rank * part_width,), (part_width,))
    v_all = lax.dynamic_slice(small, (start + flat + rank * part_width,), (part_width,))
    up_all = lax.dynamic_slice(small, (start + 2 * flat + rank * units,), (units,))

    own_a = own[0]
    qkv_grad = jnp.stack([own_a[:, c * part_width : (c + 1) * part_width] for c in range(3)])
    return (
        out_rows[:, None],
        x_rows.astype(F32)[:, None],
        qkv_grad,
        jnp.stack([q_all, v_all]),
        own_a[:, 3 * part_width :].T,
        vec[0],
        vec[1],
        vec[2],
        own[1],
        up_all,
        own[2].T,
        vec[3],
        vec[4],
        vec[5],
    )


def solution(mesh):
    placed = (
        P(None, "dp", "tensor", None),
        P(None, "dp", None),
        P(None, "dp", None),
        P(None, "dp", "tensor"),
        P(),
        P("tensor", "dp"),
        P(),
        P(),
        P(),
        P("dp", "tensor"),
        P(),
        P("tensor", "dp"),
        P(),
        P(),
        P(),
        P(None, "dp", "tensor", None),
    )
    return jax.shard_map(
        shards,
        mesh=mesh,
        in_specs=placed,
        out_specs=(
            P(None, "dp", "tensor", None),
            P(None, "dp", "tensor", None),
            P(None, "dp", "tensor"),
            P(None, "tensor"),
            P("tensor", "dp"),
            P(),
            P(),
            P(),
            P("dp", "tensor"),
            P("tensor"),
            P("tensor", "dp"),
            P(),
            P(),
            P(),
        ),
        check_vma=False,
    )
```

```python
import math
import functools
import jax
import jax.numpy as jnp
from jax import lax
from jax.sharding import PartitionSpec as P
from jax.experimental import pallas as pl
from jax.experimental.pallas import tpu as pltpu

HEAD_DIM = 64
EPS = 1e-06
F32 = jnp.float32
BF16 = jnp.bfloat16
VMEM_MOST = 60 * 1024 * 1024


def dot_nn(a, b):
    return lax.dot_general(a, b, (((1,), (0,)), ((), ())), preferred_element_type=F32)


def dot_nt(a, b):
    return lax.dot_general(a, b, (((1,), (1,)), ((), ())), preferred_element_type=F32)


def dot_tn(a, b):
    return lax.dot_general(a, b, (((0,), (0,)), ((), ())), preferred_element_type=F32)


def params(**more):
    return pltpu.CompilerParams(vmem_limit_bytes=VMEM_MOST, **more)


def qkv_kernel(x_ref, w_ref, bias_ref, out_ref):
    rows = x_ref.shape[0]
    step = min(256, rows)
    for start in range(0, rows, step):
        part = dot_nn(x_ref[start : start + step, :], w_ref[0, 0]) + bias_ref[0]
        out_ref[0, start : start + step, :] = part.astype(BF16)


def project(x, weights, bias):
    rows, width = x.shape
    parts, _, _, cols = weights.shape
    wide = bias.shape[-1]
    return pl.pallas_call(
        qkv_kernel,
        grid=(parts,),
        in_specs=[
            pl.BlockSpec((rows, width), lambda t: (0, 0)),
            pl.BlockSpec((1, 1, width, wide), lambda t: (t, 0, 0, 0)),
            pl.BlockSpec((1, 1, wide), lambda t: (t, 0, 0)),
        ],
        out_specs=pl.BlockSpec((1, rows, wide), lambda t: (t, 0, 0)),
        out_shape=jax.ShapeDtypeStruct((parts, rows, wide), BF16),
        compiler_params=params(),
        name="project",
    )(x, weights, bias)


TILE = 256
DOC_MOST = 512
REACH = -(-(DOC_MOST - 1) // TILE)


def allowed_tile(code_ref, seg_ref, key0, query0):
    codes = code_ref[pl.ds(key0, TILE), :]
    codes = jnp.concatenate([codes] * (TILE // codes.shape[1]), axis=1)
    same = codes == seg_ref[:, pl.ds(query0, TILE)]
    key_pos = key0 + lax.broadcasted_iota(jnp.int32, (TILE, TILE), 0)
    query_pos = query0 + lax.broadcasted_iota(jnp.int32, (TILE, TILE), 1)
    return same | (key_pos == query_pos)


def head_masks(lanes):
    lane = lax.broadcasted_iota(jnp.int32, (1, lanes), 1)
    return [(lane // HEAD_DIM == h).astype(BF16) for h in range(lanes // HEAD_DIM)]


def attend_kernel(
    low_ref, high_ref, code_ref, seg_ref, q_ref, k_ref, v_ref, ctx_ref, lse_ref, top, den, acc
):
    rows, lanes = q_ref.shape[1], q_ref.shape[2]
    heads = lanes // HEAD_DIM
    masks = head_masks(lanes)

    @pl.loop(0, rows // TILE)
    def _(qi):
        query0 = pl.multiple_of(qi * TILE, TILE)
        queries = q_ref[0, pl.ds(query0, TILE), :] * BF16(0.125)
        each = [queries * masks[h] for h in range(heads)]
        top[...] = jnp.full_like(top, -1e30)
        den[...] = jnp.zeros_like(den)
        acc[...] = jnp.zeros_like(acc)

        @pl.loop(low_ref[qi], high_ref[qi])
        def _(ki):
            key0 = pl.multiple_of(ki * TILE, TILE)
            allowed = allowed_tile(code_ref, seg_ref, key0, query0)
            keys = k_ref[0, pl.ds(key0, TILE), :]
            values_t = v_ref[0, pl.ds(key0, TILE), :].T
            for h in range(heads):
                scores = jnp.where(allowed, dot_nt(keys, each[h]), -1e30)
                old = top[h]
                new = jnp.maximum(old, jnp.max(scores, axis=0, keepdims=True))
                expo = jnp.exp(scores - new)
                shrink = jnp.exp(old - new)
                top[h] = new
                den[h] = den[h] * shrink + jnp.sum(expo, axis=0, keepdims=True)
                part = dot_nn(values_t[h * HEAD_DIM : (h + 1) * HEAD_DIM], expo.astype(BF16))
                acc[h] = acc[h] * shrink + part

        both = jnp.concatenate([acc[h] / den[h] for h in range(heads)], axis=0)
        ctx_ref[0, pl.ds(query0, TILE), :] = both.astype(BF16).T
        for h in range(heads):
            lse_ref[0, h : h + 1, pl.ds(query0, TILE)] = top[h] + jnp.log(den[h])


def attend(projected, low, high, codes, seg_row):
    parts, rows, wide = projected.shape
    lanes = 128
    heads = lanes // HEAD_DIM
    groups = wide // 3 // lanes
    return pl.pallas_call(
        attend_kernel,
        grid_spec=pltpu.PrefetchScalarGridSpec(
            num_scalar_prefetch=2,
            grid=(parts, groups),
            in_specs=[
                pl.BlockSpec((rows, 128), lambda t, j, lo, hi: (0, 0)),
                pl.BlockSpec((1, rows), lambda t, j, lo, hi: (0, 0)),
                pl.BlockSpec((1, rows, lanes), lambda t, j, lo, hi: (t, 0, j)),
                pl.BlockSpec((1, rows, lanes), lambda t, j, lo, hi: (t, 0, groups + j)),
                pl.BlockSpec((1, rows, lanes), lambda t, j, lo, hi: (t, 0, 2 * groups + j)),
            ],
            out_specs=[
                pl.BlockSpec((1, rows, lanes), lambda t, j, lo, hi: (t, 0, j)),
                pl.BlockSpec((1, heads, rows), lambda t, j, lo, hi: (t * groups + j, 0, 0)),
            ],
            scratch_shapes=[
                pltpu.VMEM((heads, 1, TILE), F32),
                pltpu.VMEM((heads, 1, TILE), F32),
                pltpu.VMEM((heads, HEAD_DIM, TILE), F32),
            ],
        ),
        out_shape=[
            jax.ShapeDtypeStruct((parts, rows, wide // 3), BF16),
            jax.ShapeDtypeStruct((parts * groups, heads, rows), F32),
        ],
        compiler_params=params(),
        name="attend",
    )(low, high, codes, seg_row, projected, projected, projected)


def attend_back_kernel(
    low_ref,
    high_ref,
    code_ref,
    seg_ref,
    q_ref,
    k_ref,
    v_ref,
    ctx_ref,
    g_ref,
    lse_ref,
    dq_ref,
    dk_ref,
    dv_ref,
    qsum_ref,
    vsum_ref,
    dq_acc,
    dk_acc,
    dv_acc,
):
    rows, lanes = q_ref.shape[1], q_ref.shape[2]
    heads = lanes // HEAD_DIM
    masks = head_masks(lanes)
    dk_acc[...] = jnp.zeros_like(dk_acc)
    dv_acc[...] = jnp.zeros_like(dv_acc)

    @pl.loop(0, rows // TILE)
    def _(qi):
        query0 = pl.multiple_of(qi * TILE, TILE)
        queries = q_ref[0, pl.ds(query0, TILE), :] * BF16(0.125)
        grads = g_ref[0, pl.ds(query0, TILE), :]
        prod_t = (grads.astype(F32) * ctx_ref[0, pl.ds(query0, TILE), :].astype(F32)).T
        q_each = [queries * masks[h] for h in range(heads)]
        g_each = [grads * masks[h] for h in range(heads)]
        inner = [
            jnp.sum(prod_t[h * HEAD_DIM : (h + 1) * HEAD_DIM], axis=0, keepdims=True)
            for h in range(heads)
        ]
        lse = [lse_ref[0, h : h + 1, pl.ds(query0, TILE)] for h in range(heads)]
        dq_acc[...] = jnp.zeros_like(dq_acc)

        @pl.loop(low_ref[qi], high_ref[qi])
        def _(ki):
            key0 = pl.multiple_of(ki * TILE, TILE)
            allowed = allowed_tile(code_ref, seg_ref, key0, query0)
            keys = k_ref[0, pl.ds(key0, TILE), :]
            values = v_ref[0, pl.ds(key0, TILE), :]
            keys_t = keys.T
            dk = dk_acc[pl.ds(key0, TILE), :]
            dv = dv_acc[pl.ds(key0, TILE), :]
            for h in range(heads):
                scores = jnp.where(allowed, dot_nt(keys, q_each[h]), -1e30)
                probs = jnp.exp(scores - lse[h])
                gprobs = dot_nt(values, g_each[h])
                gscores = (probs * (gprobs - inner[h])).astype(BF16)
                dv = dv + dot_nn(probs.astype(BF16), g_each[h])
                dk = dk + dot_nn(gscores, q_each[h])
                lanes_h = slice(h * HEAD_DIM, (h + 1) * HEAD_DIM)
                dq_acc[h] += dot_nn(keys_t[lanes_h], gscores)
            dk_acc[pl.ds(key0, TILE), :] = dk
            dv_acc[pl.ds(key0, TILE), :] = dv

        both = jnp.concatenate([dq_acc[h] for h in range(heads)], axis=0) * 0.125
        dq_ref[0, pl.ds(query0, TILE), :] = both.astype(BF16).T

    low_k = dk_acc[...].astype(BF16)
    low_v = dv_acc[...].astype(BF16)
    dk_ref[0] = low_k
    dv_ref[0] = low_v
    qsum_ref[0] = jnp.sum(dq_ref[0].astype(F32), axis=0, keepdims=True)
    vsum_ref[0] = jnp.sum(low_v.astype(F32), axis=0, keepdims=True)


def attend_back(projected, context, grad_context, lse, low, high, codes, seg_row):
    parts, rows, wide = projected.shape
    lanes = 128
    heads = lanes // HEAD_DIM
    groups = wide // 3 // lanes
    flat = pl.BlockSpec((1, rows, lanes), lambda t, j, lo, hi: (t, 0, j))
    sums = pl.BlockSpec((1, 1, lanes), lambda t, j, lo, hi: (t, 0, j))
    return pl.pallas_call(
        attend_back_kernel,
        grid_spec=pltpu.PrefetchScalarGridSpec(
            num_scalar_prefetch=2,
            grid=(parts, groups),
            in_specs=[
                pl.BlockSpec((rows, 128), lambda t, j, lo, hi: (0, 0)),
                pl.BlockSpec((1, rows), lambda t, j, lo, hi: (0, 0)),
                pl.BlockSpec((1, rows, lanes), lambda t, j, lo, hi: (t, 0, j)),
                pl.BlockSpec((1, rows, lanes), lambda t, j, lo, hi: (t, 0, groups + j)),
                pl.BlockSpec((1, rows, lanes), lambda t, j, lo, hi: (t, 0, 2 * groups + j)),
                flat,
                flat,
                pl.BlockSpec((1, heads, rows), lambda t, j, lo, hi: (t * groups + j, 0, 0)),
            ],
            out_specs=[flat, flat, flat, sums, sums],
            scratch_shapes=[
                pltpu.VMEM((heads, HEAD_DIM, TILE), F32),
                pltpu.VMEM((rows, lanes), F32),
                pltpu.VMEM((rows, lanes), F32),
            ],
        ),
        out_shape=[jax.ShapeDtypeStruct((parts, rows, wide // 3), BF16)] * 3
        + [jax.ShapeDtypeStruct((parts, 1, wide // 3), F32)] * 2,
        compiler_params=params(),
        name="attend_back",
    )(low, high, codes, seg_row, projected, projected, projected, context, grad_context, lse)


def norm_forward(v):
    mean = jnp.mean(v, axis=-1, keepdims=True)
    centered = v - mean
    factor = lax.rsqrt(jnp.mean(centered * centered, axis=-1, keepdims=True) + EPS)
    return centered * factor, factor


def norm_back(inner, normed, factor):
    return factor * (
        inner
        - jnp.mean(inner, axis=-1, keepdims=True)
        - normed * jnp.mean(inner * normed, axis=-1, keepdims=True)
    )


def col_sum(v):
    return jnp.sum(v, axis=0, keepdims=True)


UNIT_STEP = 512


def forward_block(x, context, out_weight, up_weight, vec_ref, bup_ref, rows_at, refs):
    normed_ref, factor_ref, act_ref, slope_ref = refs
    parts, _, units = act_ref.shape
    first_sum = x.astype(F32) + vec_ref[0:1]
    for t in range(parts):
        first_sum = first_sum + dot_nt(context(t), out_weight(t))
    normed, factor = norm_forward(first_sum)
    normed_ref[rows_at, :] = normed
    factor_ref[rows_at, :] = jnp.broadcast_to(factor, (factor.shape[0], 128))
    hidden_low = (normed * vec_ref[1:2] + vec_ref[2:3]).astype(BF16)
    for t in range(parts):
        for u in range(0, units, UNIT_STEP):
            at = slice(u, u + UNIT_STEP)
            up = dot_nn(hidden_low, up_weight(t, at)) + bup_ref[t, :, at]
            half = 0.5 * (1.0 + lax.erf(up * 0.7071067811865476))
            act_ref[t, rows_at, at] = (up * half).astype(BF16)
            slope = half + up * jnp.exp(-0.5 * up * up) * 0.3989422804014327
            slope_ref[t, rows_at, at] = slope


def forward_kernel(x_ref, ctx_ref, wo_ref, up_ref, vec_ref, bup_ref, *refs):
    forward_block(
        x_ref[...],
        lambda t: ctx_ref[t],
        lambda t: wo_ref[t, 0],
        lambda t, at: up_ref[t, 0, :, at],
        vec_ref,
        bup_ref,
        slice(None),
        refs,
    )


def forward_shapes(parts, rows, width, units):
    return [
        jax.ShapeDtypeStruct((rows, width), F32),
        jax.ShapeDtypeStruct((rows, 128), F32),
        jax.ShapeDtypeStruct((parts, rows, units), BF16),
        jax.ShapeDtypeStruct((parts, rows, units), F32),
    ]


def rows_forward(x, context, first, rest, vectors, bias_up):
    rows, width = x.shape
    parts, _, _, units = rest.shape
    part_width = context.shape[2]
    step = min(256, rows)
    last = units // part_width - 1
    row = pl.BlockSpec((step, width), lambda i: (i, 0))
    wide = pl.BlockSpec((parts, step, units), lambda i: (0, i, 0))
    return pl.pallas_call(
        forward_kernel,
        grid=(rows // step,),
        in_specs=[
            row,
            pl.BlockSpec((parts, step, part_width), lambda i: (0, i, 0)),
            pl.BlockSpec((parts, 1, width, part_width), lambda i: (0, 0, 0, last)),
            pl.BlockSpec((parts, 1, width, units), lambda i: (0, 0, 0, 0)),
            pl.BlockSpec((8, width), lambda i: (0, 0)),
            pl.BlockSpec((parts, 1, units), lambda i: (0, 0, 0)),
        ],
        out_specs=[row, pl.BlockSpec((step, 128), lambda i: (i, 0)), wide, wide],
        out_shape=forward_shapes(parts, rows, width, units),
        compiler_params=params(),
        name="rows_forward",
    )(x, context, first, rest, vectors, bias_up)


def rows_kernel(
    normed_ref,
    factor_ref,
    act_ref,
    slope_ref,
    g_ref,
    wo_ref,
    up_ref,
    down_ref,
    vec_ref,
    out_ref,
    hid_ref,
    sec_ref,
    first_ref,
    gfirst_ref,
    gup_ref,
    gctx_ref,
    sums_ref,
    upsum_ref,
):
    parts, _, units = act_ref.shape

    @pl.when(pl.program_id(0) == 0)
    def _():
        sums_ref[...] = jnp.zeros_like(sums_ref)
        upsum_ref[...] = jnp.zeros_like(upsum_ref)

    gain_one, shift_one = vec_ref[1:2], vec_ref[2:3]
    b_down, gain_two, shift_two = vec_ref[3:4], vec_ref[4:5], vec_ref[5:6]
    hidden = normed_ref[...] * gain_one + shift_one
    hid_ref[...] = hidden.astype(BF16)
    second_sum = hidden + b_down
    for t in range(parts):
        second_sum = second_sum + dot_nt(act_ref[t], down_ref[t, 0])
    normed_two, factor_two = norm_forward(second_sum)
    out_ref[...] = (normed_two * gain_two + shift_two).astype(BF16)
    grad_out = g_ref[...].astype(F32)
    grad_second = norm_back(grad_out * gain_two, normed_two, factor_two)
    second_low = grad_second.astype(BF16)
    sec_ref[...] = second_low
    grad_hidden = grad_second
    for t in range(parts):
        for u in range(0, units, UNIT_STEP):
            at = slice(u, u + UNIT_STEP)
            grad_up = (dot_nn(second_low, down_ref[t, 0, :, at]) * slope_ref[t, :, at]).astype(BF16)
            gup_ref[t, :, at] = grad_up
            upsum_ref[t, :, at] += col_sum(grad_up.astype(F32))
            grad_hidden = grad_hidden + dot_nt(grad_up, up_ref[t, 0, :, at])
    normed_one = normed_ref[...]
    grad_first = norm_back(grad_hidden * gain_one, normed_one, factor_ref[:, 0:1])
    gfirst_ref[...] = grad_first
    first_low = grad_first.astype(BF16)
    first_ref[...] = first_low
    for t in range(parts):
        gctx_ref[t] = dot_nn(first_low, wo_ref[t, 0]).astype(BF16)
    sums_ref[0:1] += col_sum(grad_first)
    sums_ref[1:2] += col_sum(grad_hidden * normed_one)
    sums_ref[2:3] += col_sum(grad_hidden)
    sums_ref[3:4] += col_sum(grad_second)
    sums_ref[4:5] += col_sum(grad_out * normed_two)
    sums_ref[5:6] += col_sum(grad_out)


def rows_pass(normed, factor, active, slope, grads, first, rest, vectors):
    rows, width = normed.shape
    parts, _, units = active.shape
    part_width = first.shape[3] // 4
    step = min(256, rows)
    row = pl.BlockSpec((step, width), lambda i: (i, 0))
    split = pl.BlockSpec((parts, step, part_width), lambda i: (0, i, 0))
    wide = pl.BlockSpec((parts, step, units), lambda i: (0, i, 0))
    once = pl.Buffered(1)
    last = units // part_width - 1
    return pl.pallas_call(
        rows_kernel,
        grid=(rows // step,),
        in_specs=[
            row,
            pl.BlockSpec((step, 128), lambda i: (i, 0)),
            wide,
            wide,
            row,
            pl.BlockSpec(
                (parts, 1, width, part_width), lambda i: (0, 0, 0, last), pipeline_mode=once
            ),
            pl.BlockSpec((parts, 1, width, units), lambda i: (0, 0, 0, 0), pipeline_mode=once),
            pl.BlockSpec((parts, 1, width, units), lambda i: (0, 1, 0, 0), pipeline_mode=once),
            pl.BlockSpec((8, width), lambda i: (0, 0)),
        ],
        out_specs=[
            row,
            row,
            row,
            row,
            row,
            wide,
            split,
            pl.BlockSpec((8, width), lambda i: (0, 0)),
            pl.BlockSpec((parts, 1, units), lambda i: (0, 0, 0)),
        ],
        out_shape=[
            jax.ShapeDtypeStruct((rows, width), BF16),
            jax.ShapeDtypeStruct((rows, width), BF16),
            jax.ShapeDtypeStruct((rows, width), BF16),
            jax.ShapeDtypeStruct((rows, width), BF16),
            jax.ShapeDtypeStruct((rows, width), F32),
            jax.ShapeDtypeStruct((parts, rows, units), BF16),
            jax.ShapeDtypeStruct((parts, rows, part_width), BF16),
            jax.ShapeDtypeStruct((8, width), F32),
            jax.ShapeDtypeStruct((parts, 1, units), F32),
        ],
        compiler_params=params(),
        name="rows_pass",
    )(normed, factor, active, slope, grads, first, rest, rest, vectors)


GRAD_STEP = 256


def outer_kernel(rows_ref, cols_ref, out_ref):
    width = rows_ref.shape[1]
    for m in range(0, width, GRAD_STEP):
        at = slice(m, m + GRAD_STEP)
        out_ref[0, at, :] = dot_tn(rows_ref[:, at], cols_ref[0]).astype(BF16)


def outer(left, right):
    rows, width = left.shape
    parts, _, units = right.shape
    return pl.pallas_call(
        outer_kernel,
        grid=(parts,),
        in_specs=[
            pl.BlockSpec((rows, width), lambda t: (0, 0)),
            pl.BlockSpec((1, rows, units), lambda t: (t, 0, 0)),
        ],
        out_specs=pl.BlockSpec((1, width, units), lambda t: (t, 0, 0)),
        out_shape=jax.ShapeDtypeStruct((parts, width, units), BF16),
        compiler_params=params(),
        name="outer",
    )(left, right)


def outer_four_kernel(x_ref, first_ref, q_ref, k_ref, v_ref, ctx_ref, out_ref):
    width = x_ref.shape[1]
    part_width = q_ref.shape[2]
    for m in range(0, width, GRAD_STEP):
        at = slice(m, m + GRAD_STEP)
        for n, cols in enumerate((q_ref, k_ref, v_ref, ctx_ref)):
            left = first_ref if n == 3 else x_ref
            part = dot_tn(left[:, at], cols[0])
            out_ref[0, at, n * part_width : (n + 1) * part_width] = part.astype(BF16)


def outer_four(x, first_low, grad_q, grad_k, grad_v, context):
    rows, width = x.shape
    parts, _, part_width = context.shape
    row = pl.BlockSpec((rows, width), lambda t: (0, 0))
    split = pl.BlockSpec((1, rows, part_width), lambda t: (t, 0, 0))
    return pl.pallas_call(
        outer_four_kernel,
        grid=(parts,),
        in_specs=[row, row, split, split, split, split],
        out_specs=pl.BlockSpec((1, width, 4 * part_width), lambda t: (t, 0, 0)),
        out_shape=jax.ShapeDtypeStruct((parts, width, 4 * part_width), BF16),
        compiler_params=params(),
        name="outer_four",
    )(x, first_low, grad_q, grad_k, grad_v, context)


def input_grad_kernel(base_ref, q_ref, k_ref, v_ref, w_ref, out_ref):
    parts, _, part_width = q_ref.shape
    total = base_ref[...]
    for t in range(parts):
        for c, cols in enumerate((q_ref, k_ref, v_ref)):
            at = slice(c * part_width, (c + 1) * part_width)
            total = total + dot_nt(cols[t], w_ref[t, 0, :, at])
    out_ref[...] = total.astype(out_ref.dtype)


def input_grad(grad_first, grad_q, grad_k, grad_v, weights):
    rows, width = grad_first.shape
    parts, _, part_width = grad_q.shape
    step = min(256, rows)
    row = pl.BlockSpec((step, width), lambda i: (i, 0))
    split = pl.BlockSpec((parts, step, part_width), lambda i: (0, i, 0))
    return pl.pallas_call(
        input_grad_kernel,
        grid=(rows // step,),
        in_specs=[
            row,
            split,
            split,
            split,
            pl.BlockSpec((parts, 1, width, 3 * part_width), lambda i: (0, 0, 0, 0)),
        ],
        out_specs=row,
        out_shape=jax.ShapeDtypeStruct((rows, width), BF16),
        compiler_params=params(),
        name="input_grad",
    )(grad_first, grad_q, grad_k, grad_v, weights)


LINE = 4
CHUNK = 64


class Place:
    def __init__(self):
        dp = lax.axis_index("dp")
        self.y = lax.axis_index("tensor")
        self.core = lax.rem(dp, 2)
        self.x = lax.rem(lax.div(dp, 2), 2)
        self.z = lax.div(dp, 4)

    @staticmethod
    def at(z, x, core, y):
        return ((z * 2 + x) * 2 + core, y)

    def corners(self, mixed, core=None):
        core = self.core if core is None else core
        side = 1 - (1 - core) * mixed
        first = (lax.rem(self.y + side, 2), lax.rem(self.x + 1 - side, 2))
        second = (lax.rem(self.y + 1 - side, 2), lax.rem(self.x + side, 2))
        return ((self.y, self.x), first, second, (1 - self.y, 1 - self.x))

    def chip(self, corner):
        return self.at(self.z, corner[1], self.core, corner[0])

    def along(self, o):
        return lax.rem(self.z + o, LINE)

    def back(self, o):
        return lax.rem(self.z + LINE - o, LINE)

    def line(self, o):
        return self.at(self.along(o), self.x, self.core, self.y)

    def partner(self):
        return self.at(self.z, self.x, 1 - self.core, self.y)

    def across_x(self):
        return self.at(self.z, 1 - self.x, self.core, self.y)

    def across_y(self):
        return self.at(self.z, self.x, self.core, 1 - self.y)

    def greet(self):
        barrier = pltpu.get_barrier_semaphore()
        others = [self.across_x(), self.across_y(), self.partner()]
        others += [self.line(o) for o in range(1, LINE)]
        for device in others:
            pl.semaphore_signal(
                barrier, inc=1, device_id=device, device_id_type=pl.DeviceIdType.MESH
            )
        pl.semaphore_wait(barrier, len(others))


def remote(src, dst, sends, recvs, slot, device):
    return pltpu.make_async_remote_copy(
        src_ref=src,
        dst_ref=dst,
        send_sem=sends.at[slot],
        recv_sem=recvs.at[slot],
        device_id=device,
        device_id_type=pl.DeviceIdType.MESH,
    )


PER_PIECE = 8


def gather_kernel(
    shard_ref,
    in_ref,
    bias_ref,
    code_ref,
    seg_ref,
    docs_ref,
    bars_ref,
    vec_ref,
    bup_ref,
    grad_ref,
    first_ref,
    rest_out,
    x_ref,
    g_ref,
    proj_ref,
    ctx_ref,
    lse_ref,
    normed_out,
    factor_out,
    act_out,
    slope_out,
    rest_ref,
    normed_buf,
    factor_buf,
    act_buf,
    slope_buf,
    sends,
    recvs,
    local_sem,
    rows_sem,
    turned,
    score_buf,
    expo_buf,
):
    place = Place()
    z, x, y, core = place.z, place.x, place.y, place.core
    chunks = shard_ref.shape[0]
    parts, rows, wide = proj_ref.shape
    last = chunks * LINE * PER_PIECE
    place.greet()

    def copy(k, o, n, src, dst, device):
        return remote(src, dst, sends, recvs, (k * LINE + o) * PER_PIECE + n, device)

    def slot(k, yy, zz, xx, cc):
        if isinstance(k, int) and k == 0:
            return first_ref.at[yy, zz, xx, cc]
        return rest_ref.at[yy, k - 1, zz, xx, cc]

    def where(k, cc=None):
        mixed = k // 2 if isinstance(k, int) else lax.div(k, 2)
        return place.corners(mixed, cc)

    def held(k, o, corner, cc=core):
        return slot(k, corner[0], place.back(o), corner[1], cc)

    def to_line(k, o):
        here = slot(k, y, z, x, core)
        return copy(k, o, 0, shard_ref.at[k], here, place.line(o))

    def from_line(k, o):
        here = held(k, o, (y, x))
        return copy(k, o, 0, here, here, place.line(o))

    def hop(k, o, n, corner, device):
        here = held(k, o, where(k)[corner])
        return copy(k, o, n, here, here, device)

    def to_first(k, o):
        return hop(k, o, 1, 0, place.chip(where(k)[1]))

    def from_first(k, o):
        return hop(k, o, 1, 1, place.chip(where(k)[1]))

    def to_second(k, o, n):
        return hop(k, o, 2 + n, n, place.chip(where(k)[2]))

    def from_second(k, o, n):
        return hop(k, o, 2 + n, 2 + n, place.chip(where(k)[2]))

    def to_partner(k, o, n):
        return hop(k, o, 4 + n, n, place.partner())

    def from_partner(k, o, n):
        here = held(k, o, where(k, 1 - core)[n], 1 - core)
        return copy(k, o, 4 + n, here, here, place.partner())

    trade = remote(in_ref.at[1 - y], x_ref.at[y], sends, recvs, last, place.across_y())
    arrive = remote(in_ref.at[y], x_ref.at[1 - y], sends, recvs, last, place.across_y())
    trade_g = remote(grad_ref.at[1 - y], g_ref.at[y], sends, recvs, last + 1, place.across_y())
    arrive_g = remote(
        grad_ref.at[y], g_ref.at[1 - y], sends, recvs, last + 1, place.across_y()
    )
    keep_g = pltpu.make_async_copy(grad_ref.at[y], g_ref.at[y], local_sem.at[chunks + 1])
    keep_g.start()
    local = [pltpu.make_async_copy(in_ref.at[y], x_ref.at[y], local_sem.at[chunks])]
    for k in range(chunks):
        own = slot(k, y, z, x, core)
        local.append(pltpu.make_async_copy(shard_ref.at[k], own, local_sem.at[k]))
    for part in local:
        part.start()
    for k in range(chunks):
        for o in (2, 1, 3):
            to_line(k, o).start()
    for part in local:
        part.wait()

    def start_line(k, o):
        to_first(k, o).start()
        to_second(k, o, 0).start()
        to_partner(k, o, 0).start()

    def arrive_first(k, o):
        from_first(k, o).wait_recv()
        to_second(k, o, 1).start()
        to_partner(k, o, 1).start()

    def arrive_second(k, o):
        for n in range(2):
            from_second(k, o, n).wait_recv()
            to_partner(k, o, 2 + n).start()

    order = (0, 1, 3, 2)
    lead = 2
    for i in range(LINE + lead):
        k, o = i // LINE, order[i % LINE]
        if o > 0:
            from_line(k, o).wait_recv()
        start_line(k, o)
        if i == 0:
            trade.start()
        if i >= 1:
            arrive_first((i - 1) // LINE, order[(i - 1) % LINE])
        if i >= 2:
            arrive_second((i - 2) // LINE, order[(i - 2) % LINE])
    arrive.wait_recv()
    for o in order:
        for n in range(4):
            from_partner(0, o, n).wait_recv()

    step = 256

    def project_slice(i):
        t = lax.div(i, rows // step)
        row = lax.rem(i, rows // step)
        half = lax.div(row * step, x_ref.shape[1])
        row0 = pl.multiple_of(lax.rem(row * step, x_ref.shape[1]), step)
        left = x_ref[half, pl.ds(row0, step), :]
        right = first_ref[t, :, :, :, :, :wide].reshape(-1, wide)
        value = dot_nn(left, right) + bias_ref[t]
        proj_ref[t, pl.ds(pl.multiple_of(row * step, step), step), :] = value.astype(BF16)

    lanes = 128
    groups = wide // 3 // lanes
    heads = lanes // HEAD_DIM
    tiles = rows // TILE
    masks = head_masks(lanes)

    def attend_slice(i):
        group = lax.div(i, tiles)
        qi = lax.rem(i, tiles)
        t = lax.div(group, groups)
        j = lax.rem(group, groups)

        def lane(c):
            return pl.ds(pl.multiple_of((c * groups + j) * lanes, lanes), lanes)

        def at(ki):
            return pl.ds(pl.multiple_of(ki * TILE, TILE), TILE)

        @pl.when(qi == 0)
        def _():
            for ki in range(tiles):
                turned[ki] = proj_ref[t, ki * TILE : (ki + 1) * TILE, lane(2)].T

        here = at(qi)
        queries = proj_ref[t, here, lane(0)] * BF16(0.125)
        own_docs = docs_ref[here, :]
        allowed = allowed_tile(code_ref, seg_ref, qi * TILE, qi * TILE)
        others = [lax.rem(qi + r, tiles) for r in range(tiles)]
        keys = [proj_ref[t, at(ki), lane(1)] for ki in others]
        values_t = jnp.concatenate([turned[ki] for ki in others], axis=1)
        for r in range(1, tiles):
            keys[r] = jnp.concatenate([keys[r], bars_ref[at(others[r]), :]], axis=1)
        most = []
        for h in range(heads):
            plain = queries * masks[h]
            marked = jnp.concatenate([plain, own_docs], axis=1)
            peak = None
            for r in range(tiles):
                if r == 0:
                    scores = jnp.where(allowed, dot_nt(keys[0], plain), -1e30)
                else:
                    scores = dot_nt(keys[r], marked)
                score_buf[h, r * TILE : (r + 1) * TILE, :] = scores
                part = jnp.max(scores.reshape(-1, 8, TILE), axis=0)
                peak = part if peak is None else jnp.maximum(peak, part)
            most.append(jnp.max(peak, axis=0, keepdims=True))
        done = []
        for h in range(heads):
            total = None
            for c in range(0, tiles * TILE, CHUNK):
                expo = jnp.exp(score_buf[h, c : c + CHUNK, :] - most[h])
                expo_buf[h, c : c + CHUNK, :] = expo.astype(BF16)
                part = jnp.sum(expo.reshape(-1, 8, TILE), axis=0)
                total = part if total is None else total + part
            total = jnp.sum(total, axis=0, keepdims=True)
            part = dot_nn(values_t[h * HEAD_DIM : (h + 1) * HEAD_DIM], expo_buf[h])
            done.append(part / total)
            lse_ref[group, h : h + 1, here] = most[h] + jnp.log(total)
        ctx_ref[t, here, lane(0)] = jnp.concatenate(done, axis=0).astype(BF16).T

    def rows_copies(i):
        at = pl.ds(pl.multiple_of(i * step, step), step)
        pairs = (
            (normed_buf.at[at, :], normed_out.at[at, :]),
            (factor_buf.at[at, :], factor_out.at[at, :]),
            (act_buf.at[:, at, :], act_out.at[:, at, :]),
            (slope_buf.at[:, at, :], slope_out.at[:, at, :]),
        )
        return [
            pltpu.make_async_copy(src, dst, rows_sem.at[i * 4 + n])
            for n, (src, dst) in enumerate(pairs)
        ]

    def rows_slice(i):
        at = pl.ds(pl.multiple_of(i * step, step), step)
        half = lax.div(i * step, x_ref.shape[1])
        row0 = pl.multiple_of(lax.rem(i * step, x_ref.shape[1]), step)
        forward_block(
            x_ref[half, pl.ds(row0, step), :],
            lambda t: ctx_ref[t, at, :],
            lambda t: first_ref[t, :, :, :, :, wide:].reshape(-1, wide // 3),
            lambda t, cols: rest_ref[t, 0, :, :, :, :, cols].reshape(-1, UNIT_STEP),
            vec_ref,
            bup_ref,
            at,
            (normed_buf, factor_buf, act_buf, slope_buf),
        )
        for part in rows_copies(i):
            part.start()

    keep_rest = [
        pltpu.make_async_copy(
            rest_ref.at[t, k], rest_out.at[t, k], local_sem.at[chunks + 2 + parts * k + t]
        )
        for k in range(chunks - 1)
        for t in range(parts)
    ]
    count = (chunks - 1) * LINE
    heavy = 2
    calm = 3
    project_share = parts * (rows // step) // heavy
    attend_share = parts * groups * tiles // calm
    row_slices = rows // step
    rows_from = heavy + calm

    def split(p):
        k = 1 + lax.div(p, LINE)
        r = lax.rem(p, LINE)
        return k, jnp.where(r < 2, r, 5 - r)

    @pl.loop(0, count)
    def _(p):
        @pl.when(p + lead < count)
        def _():
            k, o = split(p + lead)

            @pl.when(o > 0)
            def _():
                from_line(k, o).wait_recv()

            start_line(k, o)

        @pl.when(p + lead - 1 < count)
        def _():
            arrive_first(*split(p + lead - 1))

        arrive_second(*split(p + lead - 2))

        @pl.when(p == LINE - lead)
        def _():
            trade_g.start()

        @pl.when(p < heavy)
        def _():
            @pl.loop(0, project_share)
            def _(n):
                project_slice(p * project_share + n)

        @pl.when((p >= heavy) & (p < rows_from))
        def _():
            @pl.loop(0, attend_share)
            def _(n):
                attend_slice((p - heavy) * attend_share + n)

        @pl.when(p == rows_from)
        def _():
            for o in order:
                for n in range(4):
                    from_partner(1, o, n).wait_recv()

        @pl.when(p >= rows_from)
        def _():
            rows_slice(p - rows_from)

    for i in range(count - rows_from, row_slices):
        rows_slice(i)
    for part in keep_rest[:parts]:
        part.start()
    for o in order:
        for n in range(4):
            from_partner(2, o, n).wait_recv()
    for part in keep_rest[parts:]:
        part.start()

    @pl.loop(0, count)
    def _(p):
        k, o = split(p)

        @pl.when(o > 0)
        def _():
            to_line(k, o).wait_send()

        to_first(k, o).wait_send()
        for n in range(2):
            to_second(k, o, n).wait_send()
        for n in range(4):
            to_partner(k, o, n).wait_send()

    for o in order:
        if o > 0:
            to_line(0, o).wait_send()
        to_first(0, o).wait_send()
        for n in range(2):
            to_second(0, o, n).wait_send()
        for n in range(4):
            to_partner(0, o, n).wait_send()
    trade.wait_send()
    trade_g.wait_send()
    arrive_g.wait_recv()
    keep_g.wait()
    for part in keep_rest:
        part.wait()
    for i in range(row_slices):
        for part in rows_copies(i):
            part.wait()


def gather_all(shard, halves, bias, codes, seg_row, docs, bars, vectors, bias_up, grad_halves):
    chunks, own_rows, units = shard.shape
    parts, rows, width = halves.shape
    wide = bias.shape[-1]
    length = parts * rows
    groups = wide // 3 // 128
    anywhere = pl.BlockSpec(memory_space=pl.ANY)
    local = pl.BlockSpec(memory_space=pltpu.VMEM)
    copies = chunks * LINE * PER_PIECE + 2
    places = (LINE, 2, 2, own_rows, units)
    forward = forward_shapes(parts, length, width, units)
    first, rest, x, grads, projected, context, lse, *state = pl.pallas_call(
        gather_kernel,
        in_specs=[local] * 9 + [anywhere],
        out_specs=[local, anywhere, local, anywhere, local, local, local] + [anywhere] * 4,
        out_shape=[
            jax.ShapeDtypeStruct((parts,) + places, BF16),
            jax.ShapeDtypeStruct((parts, chunks - 1) + places, BF16),
            jax.ShapeDtypeStruct((parts, rows, width), BF16),
            jax.ShapeDtypeStruct((parts, rows, width), BF16),
            jax.ShapeDtypeStruct((parts, length, wide), BF16),
            jax.ShapeDtypeStruct((parts, length, wide // 3), BF16),
            jax.ShapeDtypeStruct((parts * groups, 2, length), F32),
        ]
        + forward,
        scratch_shapes=[
            pltpu.VMEM((parts, chunks - 1) + places, BF16),
        ]
        + [pltpu.VMEM(s.shape, s.dtype) for s in forward]
        + [
            pltpu.SemaphoreType.DMA((copies,)),
            pltpu.SemaphoreType.DMA((copies,)),
            pltpu.SemaphoreType.DMA((chunks + 2 + parts * (chunks - 1),)),
            pltpu.SemaphoreType.DMA((length // 256 * 4,)),
            pltpu.VMEM((length // TILE, 128, TILE), BF16),
            pltpu.VMEM((2, length, TILE), F32),
            pltpu.VMEM((2, length, TILE), BF16),
        ],
        compiler_params=params(collective_id=0, has_side_effects=True),
        name="gather_all",
    )(shard, halves, bias, codes, seg_row, docs, bars, vectors, bias_up, grad_halves)
    first = first.reshape(parts, 1, -1, units)
    rest = rest.reshape(parts, chunks - 1, -1, units)
    x, grads = x.reshape(length, width), grads.reshape(length, width)
    return first, rest, x, grads, projected, context, lse, state


def back_kernel(
    b_ref,
    c_ref,
    x_ref,
    first_ref,
    base_ref,
    proj_ref,
    ctx_ref,
    g_ref,
    lse_ref,
    code_ref,
    seg_ref,
    docs_ref,
    bars_ref,
    w_ref,
    small_ref,
    res_ref,
    out_ref,
    xr_ref,
    rr_ref,
    total_ref,
    a_buf,
    dp_buf,
    xg_buf,
    p_buf,
    s_buf,
    f_buf,
    z_buf,
    t_buf,
    turned,
    score_buf,
    gprob_buf,
    prob_buf,
    gscore_buf,
    dk_acc,
    dv_acc,
    sends,
    recvs,
    t_send,
    t_recv,
    local_sem,
):
    place = Place()
    z, x, y, core = place.z, place.x, place.y, place.core
    chunks = out_ref.shape[0]
    own_rows = out_ref.shape[1]
    parts, rows, wide = proj_ref.shape
    part_width = wide // 3
    width = x_ref.shape[1]
    place.greet()

    def where(k):
        return place.corners(int(k > 0) if isinstance(k, int) else 1)

    def copy(k, o, n, src, dst, device):
        return remote(src, dst, sends, recvs, (k * LINE + o) * PER_PIECE + n, device)

    def a_rows(zz, xx, cc):
        start = pl.multiple_of(((zz * 2 + xx) * 2 + cc) * own_rows, own_rows)
        return pl.ds(start, own_rows)

    def to_partner_a(o, n):
        yy, xx = n // 2, n % 2
        src = a_buf.at[yy, a_rows(place.along(o), xx, 1 - core)]
        slot = (0, 5, 6, 7)[n]
        return copy(0, o, slot, src, p_buf.at[0, o, yy, xx], place.partner())

    def to_partner(source, k, o):
        src = source.at[:, place.along(o), :, 1 - core]
        return copy(k, o, 0, src, p_buf.at[k, o], place.partner())

    def to_second(k, o, n):
        yy, xx = where(k)[2 + n]
        device = place.chip(where(k)[2])
        return copy(k, o, 1 + n, p_buf.at[k, o, yy, xx], s_buf.at[k, o, n], device)

    def to_first(k, o):
        device = place.chip(where(k)[1])
        return copy(k, o, 3, s_buf.at[k, o, 1], f_buf.at[k, o], device)

    def to_line(k, o):
        return copy(k, o, 4, f_buf.at[k, o], z_buf.at[k, o - 1], place.line(o))

    def small_copy(n, src, dst, device):
        return remote(src, dst, t_send, t_recv, n, device)

    hops = (
        small_copy(0, t_buf.at[9], t_buf.at[0], place.partner()),
        small_copy(1, t_buf.at[1], t_buf.at[2], place.across_x()),
        small_copy(2, t_buf.at[3], t_buf.at[4], place.across_y()),
    )

    def small_line(o):
        return small_copy(2 + o, t_buf.at[5 + z], t_buf.at[5 + z], place.line(o))

    def small_from(o):
        here = t_buf.at[5 + place.back(o)]
        return small_copy(2 + o, here, here, place.line(o))

    def small_step(step):
        if step == 0:
            hops[0].start()
        elif step == 1:
            hops[0].wait_recv()
            t_buf[1] = t_buf[9] + t_buf[0]
            hops[1].start()
        elif step == 2:
            hops[1].wait_recv()
            t_buf[3] = t_buf[1] + t_buf[2]
            hops[2].start()
        elif step == 3:
            hops[2].wait_recv()
            t_buf[5 + z] = t_buf[3] + t_buf[4]
            for o in range(1, LINE):
                small_line(o).start()
        elif step == 4:
            for o in range(1, LINE):
                small_from(o).wait_recv()
            total_ref[...] = (t_buf[5] + t_buf[6]) + (t_buf[7] + t_buf[8])

    trade = small_copy(2 + LINE, xg_buf.at[1 - y], xr_ref.at[y], place.across_y())
    arrive = small_copy(2 + LINE, xg_buf.at[1 - y], xr_ref.at[1 - y], place.across_y())
    keep = pltpu.make_async_copy(xg_buf.at[y], xr_ref.at[y], local_sem.at[0])
    trade_r = small_copy(3 + LINE, res_ref.at[1 - y], rr_ref.at[y], place.across_y())
    arrive_r = small_copy(3 + LINE, res_ref.at[1 - y], rr_ref.at[1 - y], place.across_y())
    keep_r = pltpu.make_async_copy(res_ref.at[y], rr_ref.at[y], local_sem.at[1])

    def add_partner(k, o, own):
        for n in (3, 2, 1, 0):
            yy, xx = where(k)[n]
            p_buf[k, o, yy, xx] = p_buf[k, o, yy, xx] + own(yy, xx)
            if n >= 2:
                to_second(k, o, n - 2).start()

    def stage_partner(source, k, o):
        to_partner(source, k, o).wait_recv()
        zz = place.along(o)
        add_partner(k, o, lambda yy, xx: source[yy, zz, xx, core])

    def stage_second(k, o):
        for n in (1, 0):
            yy, xx = where(k)[n]
            to_second(k, o, n).wait_recv()
            s_buf[k, o, n] = s_buf[k, o, n] + p_buf[k, o, yy, xx]
            if n == 1:
                to_first(k, o).start()

    def stage_first(k, o):
        to_first(k, o).wait_recv()
        f_buf[k, o] = f_buf[k, o] + s_buf[k, o, 0]

    def finish(k):
        total = f_buf[k, 0].astype(F32)
        for o in range(1, LINE):
            to_line(k, o).wait_recv()
            total = total + z_buf[k, o - 1].astype(F32)
        out_ref[k] = total

    lanes = 128
    groups = part_width // lanes
    heads = lanes // HEAD_DIM
    tiles = rows // TILE
    masks = head_masks(lanes)
    q_row = small_ref.shape[0] - (2 * parts * groups + parts * w_ref.shape[3] // lanes)

    def lane(c, j):
        return pl.ds(pl.multiple_of((c * groups + j) * lanes, lanes), lanes)

    def at(ki):
        return pl.ds(pl.multiple_of(ki * TILE, TILE), TILE)

    def attend_slice(i):
        group = lax.div(i, tiles)
        qi = lax.rem(i, tiles)
        t = lax.div(group, groups)
        j = lax.rem(group, groups)

        @pl.when(qi == 0)
        def _():
            dk_acc[...] = jnp.zeros_like(dk_acc)
            dv_acc[...] = jnp.zeros_like(dv_acc)
            for ki in range(tiles):
                turned[ki] = proj_ref[t, ki * TILE : (ki + 1) * TILE, lane(1, j)].T

        here = at(qi)
        queries = proj_ref[t, here, lane(0, j)] * BF16(0.125)
        grads = g_ref[t, here, lane(0, j)]
        own_docs = docs_ref[here, :]
        prod_t = (grads.astype(F32) * ctx_ref[t, here, lane(0, j)].astype(F32)).T
        plain = [queries * masks[h] for h in range(heads)]
        g_each = [grads * masks[h] for h in range(heads)]
        marked = [jnp.concatenate([plain[h], own_docs], axis=1) for h in range(heads)]
        q_tall = jnp.concatenate(plain, axis=0)
        g_tall = jnp.concatenate(g_each, axis=0)
        inner = [
            jnp.sum(prod_t[h * HEAD_DIM : (h + 1) * HEAD_DIM], axis=0, keepdims=True)
            for h in range(heads)
        ]
        lse = [lse_ref[group, h : h + 1, here] for h in range(heads)]
        allowed = allowed_tile(code_ref, seg_ref, qi * TILE, qi * TILE)
        dq = [None] * heads

        for r in range(tiles):
            there = at(lax.rem(qi + r, tiles))
            keys = proj_ref[t, there, lane(1, j)]
            values = proj_ref[t, there, lane(2, j)]
            if r > 0:
                keys = jnp.concatenate([keys, bars_ref[there, :]], axis=1)
            for h in range(heads):
                scores = dot_nt(keys, marked[h] if r > 0 else plain[h])
                if r == 0:
                    scores = jnp.where(allowed, scores, -1e30)
                score_buf[r % 2, h] = scores
                gprob_buf[r % 2, h] = dot_nt(values, g_each[h])
            for h in range(heads):
                cols = slice(h * TILE, (h + 1) * TILE)
                for c in range(0, TILE, CHUNK):
                    rows_c = slice(c, c + CHUNK)
                    probs = jnp.exp(score_buf[r % 2, h, rows_c, :] - lse[h])
                    gscores = probs * (gprob_buf[r % 2, h, rows_c, :] - inner[h])
                    prob_buf[r, rows_c, cols] = probs.astype(BF16)
                    gscore_buf[r, rows_c, cols] = gscores.astype(BF16)
            dv_acc[there, :] += dot_nn(prob_buf[r], g_tall)
            dk_acc[there, :] += dot_nn(gscore_buf[r], q_tall)
        keys_t = jnp.concatenate([turned[lax.rem(qi + r, tiles)] for r in range(tiles)], axis=1)
        dq = []
        for h in range(heads):
            tall = gscore_buf[:, :, h * TILE : (h + 1) * TILE].reshape(tiles * TILE, TILE)
            dq.append(dot_nn(keys_t[h * HEAD_DIM : (h + 1) * HEAD_DIM], tall))
        both = jnp.concatenate(dq, axis=0) * 0.125
        dp_buf[t, here, lane(0, j)] = both.astype(BF16).T

        @pl.when(qi == tiles - 1)
        def _():
            low_k = dk_acc[...].astype(BF16)
            low_v = dv_acc[...].astype(BF16)
            low_q = dp_buf[t, :, lane(0, j)]
            dp_buf[t, :, lane(1, j)] = low_k
            dp_buf[t, :, lane(2, j)] = low_v
            t_buf[9, pl.ds(q_row + group, 1), :] = col_sum(low_q.astype(F32))
            v_row = q_row + parts * groups + group
            t_buf[9, pl.ds(v_row, 1), :] = col_sum(low_v.astype(F32))

    order = (2, 1, 3, 0)

    def split(p):
        r = lax.rem(p, LINE)
        o = jnp.where(r == 0, 2, jnp.where(r == 1, 1, jnp.where(r == 2, 3, 0)))
        return 1 + lax.div(p, LINE), o

    for source, k in ((b_ref, 1), (c_ref, 2)):
        for o in order:
            to_partner(source, k, o).start()
    trade_r.start()
    keep_r.start()
    t_buf[9] = small_ref[...]
    count = (chunks - 1) * LINE
    share = parts * groups * tiles // count

    def pass_second(p):
        stage_second(*split(p))

    def pass_first(p):
        k, o = split(p)
        stage_first(k, o)

        @pl.when(o > 0)
        def _():
            to_line(k, o).start()

    @pl.loop(0, count)
    def _(p):
        k, o = split(p)

        @pl.when(p < LINE)
        def _():
            stage_partner(b_ref, k, o)

        @pl.when(p >= LINE)
        def _():
            stage_partner(c_ref, k, o)

        @pl.when(p >= 1)
        def _():
            pass_second(p - 1)

        @pl.when(p >= 2)
        def _():
            pass_first(p - 2)

        @pl.loop(0, share)
        def _(n):
            attend_slice(p * share + n)

    small_step(0)
    pass_second(count - 1)
    pass_first(count - 2)
    for t in range(parts):
        for m in range(0, width, GRAD_STEP):
            at = slice(m, m + GRAD_STEP)
            left = x_ref[:, at]
            part = dot_tn(left, dp_buf[t])
            a_buf[t, at, :wide] = part.astype(BF16)
            part = dot_tn(first_ref[:, at], ctx_ref[t])
            a_buf[t, at, wide:] = part.astype(BF16)
        small_step(1 + t)
        if t == 0:
            pass_first(count - 1)
    for o in order:
        for n in range(4):
            to_partner_a(o, n).start()
    small_step(3)

    step = 256
    half_rows = rows // parts

    def input_slice(i):
        at = slice(i * step, (i + 1) * step)
        value = base_ref[at, :]
        for t in range(parts):
            value = value + dot_nt(dp_buf[t, at, :], w_ref[t, 0, :, :wide])
        half, row0 = i * step // half_rows, i * step % half_rows
        xg_buf[half, row0 : row0 + step, :] = value.astype(BF16)

    for i in range(LINE + 2):
        if i < LINE:
            o = order[i]
            for n in range(4):
                to_partner_a(o, n).wait_recv()
            zz = place.along(o)
            add_partner(0, o, lambda yy, xx: a_buf[yy, a_rows(zz, xx, core), :])
        if 0 <= i - 1 < LINE:
            stage_second(0, order[i - 1])
        if 0 <= i - 2 < LINE:
            stage_first(0, order[i - 2])
            if order[i - 2] > 0:
                to_line(0, order[i - 2]).start()
        if i < rows // step:
            input_slice(i)
        if i == rows // step - 1:
            trade.start()
            keep.start()
            small_step(4)
    for k in (1, 2, 0):
        finish(k)

    for part in (keep, keep_r):
        part.wait()
    for part in (trade, trade_r):
        part.wait_send()
    for part in (arrive, arrive_r):
        part.wait_recv()
    for part in hops:
        part.wait_send()
    for o in range(1, LINE):
        small_line(o).wait_send()
    for k in range(chunks):
        for o in order:
            if k == 0:
                for n in range(4):
                    to_partner_a(o, n).wait_send()
            else:
                to_partner((b_ref, c_ref)[k - 1], k, o).wait_send()
            for n in range(2):
                to_second(k, o, n).wait_send()
            to_first(k, o).wait_send()
            if o > 0:
                to_line(k, o).wait_send()


def back_all(
    grads_b,
    grads_c,
    x,
    first_low,
    grad_first,
    projected,
    context,
    grad_context,
    lse,
    codes,
    seg_row,
    docs,
    bars,
    first,
    small,
    result,
):
    parts, width, units = grads_b.shape
    rows, model = x.shape
    wide = projected.shape[2]
    own_rows = width // (4 * LINE)
    chunks = 3
    folded = [g.reshape(parts, LINE, 2, 2, own_rows, units) for g in (grads_b, grads_c)]
    small_rows = small.shape[0] // 128
    local = pl.BlockSpec(memory_space=pltpu.VMEM)
    anywhere = pl.BlockSpec(memory_space=pl.ANY)
    piece = (own_rows, units)
    copies = chunks * LINE * PER_PIECE
    own, x_rows, out_rows, total = pl.pallas_call(
        back_kernel,
        in_specs=[local] * 15 + [anywhere],
        out_specs=[local, anywhere, anywhere, local],
        out_shape=[
            jax.ShapeDtypeStruct((chunks, own_rows, units), F32),
            jax.ShapeDtypeStruct((parts, rows // parts, model), BF16),
            jax.ShapeDtypeStruct((parts, rows // parts, model), BF16),
            jax.ShapeDtypeStruct((small_rows, 128), F32),
        ],
        scratch_shapes=[
            pltpu.VMEM((parts, width, units), BF16),
            pltpu.VMEM((parts, rows, wide), BF16),
            pltpu.VMEM((parts, rows // parts, model), BF16),
            pltpu.VMEM((chunks, LINE, 2, 2) + piece, BF16),
            pltpu.VMEM((chunks, LINE, 2) + piece, BF16),
            pltpu.VMEM((chunks, LINE) + piece, BF16),
            pltpu.VMEM((chunks, LINE - 1) + piece, BF16),
            pltpu.VMEM((6 + LINE, small_rows, 128), F32),
            pltpu.VMEM((rows // TILE, 128, TILE), BF16),
            pltpu.VMEM((2, 2, TILE, TILE), F32),
            pltpu.VMEM((2, 2, TILE, TILE), F32),
            pltpu.VMEM((rows // TILE, TILE, 2 * TILE), BF16),
            pltpu.VMEM((rows // TILE, TILE, 2 * TILE), BF16),
            pltpu.VMEM((rows, 128), F32),
            pltpu.VMEM((rows, 128), F32),
            pltpu.SemaphoreType.DMA((copies,)),
            pltpu.SemaphoreType.DMA((copies,)),
            pltpu.SemaphoreType.DMA((4 + LINE,)),
            pltpu.SemaphoreType.DMA((4 + LINE,)),
            pltpu.SemaphoreType.DMA((2,)),
        ],
        compiler_params=params(collective_id=1, has_side_effects=True),
        name="back_all",
    )(
        *folded,
        x,
        first_low,
        grad_first,
        projected,
        context,
        grad_context,
        lse,
        codes,
        seg_row,
        docs,
        bars,
        first,
        small.reshape(small_rows, 128),
        result.reshape(parts, rows // parts, model),
    )
    return own, x_rows, out_rows, total.reshape(-1)


def trade_in(halves):
    return lax.all_to_all(halves, "tensor", split_axis=0, concat_axis=1, tiled=True)[0]


def trade_out(whole):
    return lax.all_to_all(whole[None], "tensor", split_axis=1, concat_axis=0, tiled=True)


def gather_weights(shard):
    full = lax.all_gather(shard, "dp", axis=1, tiled=True)
    return lax.all_gather(full, "tensor", axis=0, tiled=False)


def scatter_grads(partial):
    own = lax.psum_scatter(partial, "tensor", scatter_dimension=0, tiled=False)
    return lax.psum_scatter(own, "dp", scatter_dimension=0, tiled=True)


def shards(
    inputs,
    seg_ids,
    keep_mask,
    w_qkv,
    b_qv,
    w_o,
    b_o,
    gain_one,
    shift_one,
    w_up,
    b_up,
    w_down,
    b_down,
    gain_two,
    shift_two,
    out_grad,
):
    parts = lax.axis_size("tensor")
    assert inputs.shape[0] == parts
    own_rows = w_qkv.shape[1]
    part_width = w_qkv.shape[2]
    units = w_up.shape[1]
    rank = lax.axis_index("tensor")

    shard_a = jnp.concatenate([w_qkv[0], w_qkv[1], w_qkv[2], w_o.T], axis=1)
    shard = jnp.stack([shard_a, w_up, w_down.T])
    seg = lax.dynamic_index_in_dim(seg_ids[:, 0], rank, 0, keepdims=False)
    keep = lax.dynamic_index_in_dim(keep_mask[:, 0], rank, 0, keepdims=False)
    length = seg.shape[0]
    firsts, lasts = seg[::TILE], seg[TILE - 1 :: TILE]
    low = (jnp.sum(seg[None, :] < firsts[:, None], axis=1) // TILE).astype(jnp.int32)
    past = jnp.sum(seg[None, :] <= lasts[:, None], axis=1)
    high = ((past + TILE - 1) // TILE).astype(jnp.int32)
    codes = jnp.broadcast_to(jnp.where(keep == 1, seg, -1)[:, None], (length, 128))
    seg_row = seg[None, :]

    b_q = b_qv[0].reshape(parts, part_width)
    b_v = b_qv[1].reshape(parts, part_width)
    bias = jnp.concatenate([b_q, jnp.zeros_like(b_q), b_v], axis=1)[:, None, :]
    zero = jnp.zeros_like(b_o)
    vectors = jnp.stack([b_o, gain_one, shift_one, b_down, gain_two, shift_two, zero, zero])
    bias_up = b_up.reshape(parts, 1, units)
    linked = lax.axis_size("dp") == LINE * 4 and parts == 2
    if linked:
        number = lax.broadcasted_iota(jnp.int32, (1, 128), 1)
        docs = (seg[:, None] == number).astype(BF16)
        bars = jnp.where(codes == number, 0.0, -1e30).astype(BF16)
        first, rest, x, grads, projected, context, lse, state = gather_all(
            shard,
            inputs[:, 0],
            bias,
            codes,
            seg_row,
            docs,
            bars,
            vectors,
            bias_up,
            out_grad[:, 0],
        )
    else:
        weights = gather_weights(shard)
        first, rest = weights[:, :1], weights[:, 1:]
        x = trade_in(inputs[:, 0])
        grads = trade_in(out_grad[:, 0])
        projected = project(x, first, bias)
        context, lse = attend(projected, low, high, codes, seg_row)
        state = rows_forward(x, context, first, rest, vectors, bias_up)
    normed, factor, active, slope = state
    out, hidden_low, second_low, first_low, grad_first, grad_up, grad_context, sums, upsum = (
        rows_pass(normed, factor, active, slope, grads, first, rest, vectors)
    )
    partial_up = outer(hidden_low, grad_up)
    partial_down = outer(second_low, active)
    if linked:
        zeros = jnp.zeros((4 * part_width,), F32)
        small = jnp.concatenate([sums[:6].reshape(-1), zeros, upsum.reshape(-1)])
        own, x_rows, out_rows, small = back_all(
            partial_up,
            partial_down,
            x,
            first_low,
            grad_first,
            projected,
            context,
            grad_context,
            lse,
            codes,
            seg_row,
            docs,
            bars,
            first,
            small,
            out,
        )
    else:
        grad_q, grad_k, grad_v, qsum, vsum = attend_back(
            projected, context, grad_context, lse, low, high, codes, seg_row
        )
        partial_a = outer_four(x, first_low, grad_q, grad_k, grad_v, context)
        own = jnp.stack(
            [scatter_grads(g).astype(F32) for g in (partial_a, partial_up, partial_down)]
        )
        x_rows = trade_out(input_grad(grad_first, grad_q, grad_k, grad_v, first))
        out_rows = trade_out(out)
        small = jnp.concatenate(
            [sums[:6].reshape(-1), qsum.reshape(-1), vsum.reshape(-1), upsum.reshape(-1)]
        )
        small = lax.psum(small, ("dp", "tensor"))
    width = sums.shape[1]
    vec = small[: 6 * width].reshape(6, width)
    flat = parts * part_width
    start = 6 * width
    q_all = lax.dynamic_slice(small, (start + rank * part_width,), (part_width,))
    v_all = lax.dynamic_slice(small, (start + flat + rank * part_width,), (part_width,))
    up_all = lax.dynamic_slice(small, (start + 2 * flat + rank * units,), (units,))

    own_a = own[0]
    qkv_grad = jnp.stack([own_a[:, c * part_width : (c + 1) * part_width] for c in range(3)])
    return (
        out_rows[:, None],
        x_rows.astype(F32)[:, None],
        qkv_grad,
        jnp.stack([q_all, v_all]),
        own_a[:, 3 * part_width :].T,
        vec[0],
        vec[1],
        vec[2],
        own[1],
        up_all,
        own[2].T,
        vec[3],
        vec[4],
        vec[5],
    )


def solution(mesh):
    placed = (
        P(None, "dp", "tensor", None),
        P(None, "dp", None),
        P(None, "dp", None),
        P(None, "dp", "tensor"),
        P(),
        P("tensor", "dp"),
        P(),
        P(),
        P(),
        P("dp", "tensor"),
        P(),
        P("tensor", "dp"),
        P(),
        P(),
        P(),
        P(None, "dp", "tensor", None),
    )
    return jax.shard_map(
        shards,
        mesh=mesh,
        in_specs=placed,
        out_specs=(
            P(None, "dp", "tensor", None),
            P(None, "dp", "tensor", None),
            P(None, "dp", "tensor"),
            P(None, "tensor"),
            P("tensor", "dp"),
            P(),
            P(),
            P(),
            P("dp", "tensor"),
            P("tensor"),
            P("tensor", "dp"),
            P(),
            P(),
            P(),
        ),
        check_vma=False,
    )
```

```python
import math
import functools
import jax
import jax.numpy as jnp
from jax import lax
from jax.sharding import PartitionSpec as P
from jax.experimental import pallas as pl
from jax.experimental.pallas import tpu as pltpu

HEAD_DIM = 64
EPS = 1e-06
F32 = jnp.float32
BF16 = jnp.bfloat16
VMEM_MOST = 60 * 1024 * 1024


def dot_nn(a, b):
    return lax.dot_general(a, b, (((1,), (0,)), ((), ())), preferred_element_type=F32)


def dot_nt(a, b):
    return lax.dot_general(a, b, (((1,), (1,)), ((), ())), preferred_element_type=F32)


def dot_tn(a, b):
    return lax.dot_general(a, b, (((0,), (0,)), ((), ())), preferred_element_type=F32)


def params(**more):
    return pltpu.CompilerParams(vmem_limit_bytes=VMEM_MOST, **more)


def qkv_kernel(x_ref, w_ref, bias_ref, out_ref):
    rows = x_ref.shape[0]
    step = min(256, rows)
    for start in range(0, rows, step):
        part = dot_nn(x_ref[start : start + step, :], w_ref[0, 0]) + bias_ref[0]
        out_ref[0, start : start + step, :] = part.astype(BF16)


def project(x, weights, bias):
    rows, width = x.shape
    parts, _, _, cols = weights.shape
    wide = bias.shape[-1]
    return pl.pallas_call(
        qkv_kernel,
        grid=(parts,),
        in_specs=[
            pl.BlockSpec((rows, width), lambda t: (0, 0)),
            pl.BlockSpec((1, 1, width, wide), lambda t: (t, 0, 0, 0)),
            pl.BlockSpec((1, 1, wide), lambda t: (t, 0, 0)),
        ],
        out_specs=pl.BlockSpec((1, rows, wide), lambda t: (t, 0, 0)),
        out_shape=jax.ShapeDtypeStruct((parts, rows, wide), BF16),
        compiler_params=params(),
        name="project",
    )(x, weights, bias)


TILE = 256
DOC_MOST = 512
REACH = -(-(DOC_MOST - 1) // TILE)


def allowed_tile(code_ref, seg_ref, key0, query0):
    codes = code_ref[pl.ds(key0, TILE), :]
    codes = jnp.concatenate([codes] * (TILE // codes.shape[1]), axis=1)
    same = codes == seg_ref[:, pl.ds(query0, TILE)]
    key_pos = key0 + lax.broadcasted_iota(jnp.int32, (TILE, TILE), 0)
    query_pos = query0 + lax.broadcasted_iota(jnp.int32, (TILE, TILE), 1)
    return same | (key_pos == query_pos)


def head_masks(lanes):
    lane = lax.broadcasted_iota(jnp.int32, (1, lanes), 1)
    return [(lane // HEAD_DIM == h).astype(BF16) for h in range(lanes // HEAD_DIM)]


def attend_kernel(
    low_ref, high_ref, code_ref, seg_ref, q_ref, k_ref, v_ref, ctx_ref, lse_ref, top, den, acc
):
    rows, lanes = q_ref.shape[1], q_ref.shape[2]
    heads = lanes // HEAD_DIM
    masks = head_masks(lanes)

    @pl.loop(0, rows // TILE)
    def _(qi):
        query0 = pl.multiple_of(qi * TILE, TILE)
        queries = q_ref[0, pl.ds(query0, TILE), :] * BF16(0.125)
        each = [queries * masks[h] for h in range(heads)]
        top[...] = jnp.full_like(top, -1e30)
        den[...] = jnp.zeros_like(den)
        acc[...] = jnp.zeros_like(acc)

        @pl.loop(low_ref[qi], high_ref[qi])
        def _(ki):
            key0 = pl.multiple_of(ki * TILE, TILE)
            allowed = allowed_tile(code_ref, seg_ref, key0, query0)
            keys = k_ref[0, pl.ds(key0, TILE), :]
            values_t = v_ref[0, pl.ds(key0, TILE), :].T
            for h in range(heads):
                scores = jnp.where(allowed, dot_nt(keys, each[h]), -1e30)
                old = top[h]
                new = jnp.maximum(old, jnp.max(scores, axis=0, keepdims=True))
                expo = jnp.exp(scores - new)
                shrink = jnp.exp(old - new)
                top[h] = new
                den[h] = den[h] * shrink + jnp.sum(expo, axis=0, keepdims=True)
                part = dot_nn(values_t[h * HEAD_DIM : (h + 1) * HEAD_DIM], expo.astype(BF16))
                acc[h] = acc[h] * shrink + part

        both = jnp.concatenate([acc[h] / den[h] for h in range(heads)], axis=0)
        ctx_ref[0, pl.ds(query0, TILE), :] = both.astype(BF16).T
        for h in range(heads):
            lse_ref[0, h : h + 1, pl.ds(query0, TILE)] = top[h] + jnp.log(den[h])


def attend(projected, low, high, codes, seg_row):
    parts, rows, wide = projected.shape
    lanes = 128
    heads = lanes // HEAD_DIM
    groups = wide // 3 // lanes
    return pl.pallas_call(
        attend_kernel,
        grid_spec=pltpu.PrefetchScalarGridSpec(
            num_scalar_prefetch=2,
            grid=(parts, groups),
            in_specs=[
                pl.BlockSpec((rows, 128), lambda t, j, lo, hi: (0, 0)),
                pl.BlockSpec((1, rows), lambda t, j, lo, hi: (0, 0)),
                pl.BlockSpec((1, rows, lanes), lambda t, j, lo, hi: (t, 0, j)),
                pl.BlockSpec((1, rows, lanes), lambda t, j, lo, hi: (t, 0, groups + j)),
                pl.BlockSpec((1, rows, lanes), lambda t, j, lo, hi: (t, 0, 2 * groups + j)),
            ],
            out_specs=[
                pl.BlockSpec((1, rows, lanes), lambda t, j, lo, hi: (t, 0, j)),
                pl.BlockSpec((1, heads, rows), lambda t, j, lo, hi: (t * groups + j, 0, 0)),
            ],
            scratch_shapes=[
                pltpu.VMEM((heads, 1, TILE), F32),
                pltpu.VMEM((heads, 1, TILE), F32),
                pltpu.VMEM((heads, HEAD_DIM, TILE), F32),
            ],
        ),
        out_shape=[
            jax.ShapeDtypeStruct((parts, rows, wide // 3), BF16),
            jax.ShapeDtypeStruct((parts * groups, heads, rows), F32),
        ],
        compiler_params=params(),
        name="attend",
    )(low, high, codes, seg_row, projected, projected, projected)


def attend_back_kernel(
    low_ref,
    high_ref,
    code_ref,
    seg_ref,
    q_ref,
    k_ref,
    v_ref,
    ctx_ref,
    g_ref,
    lse_ref,
    dq_ref,
    dk_ref,
    dv_ref,
    qsum_ref,
    vsum_ref,
    dq_acc,
    dk_acc,
    dv_acc,
):
    rows, lanes = q_ref.shape[1], q_ref.shape[2]
    heads = lanes // HEAD_DIM
    masks = head_masks(lanes)
    dk_acc[...] = jnp.zeros_like(dk_acc)
    dv_acc[...] = jnp.zeros_like(dv_acc)

    @pl.loop(0, rows // TILE)
    def _(qi):
        query0 = pl.multiple_of(qi * TILE, TILE)
        queries = q_ref[0, pl.ds(query0, TILE), :] * BF16(0.125)
        grads = g_ref[0, pl.ds(query0, TILE), :]
        prod_t = (grads.astype(F32) * ctx_ref[0, pl.ds(query0, TILE), :].astype(F32)).T
        q_each = [queries * masks[h] for h in range(heads)]
        g_each = [grads * masks[h] for h in range(heads)]
        inner = [
            jnp.sum(prod_t[h * HEAD_DIM : (h + 1) * HEAD_DIM], axis=0, keepdims=True)
            for h in range(heads)
        ]
        lse = [lse_ref[0, h : h + 1, pl.ds(query0, TILE)] for h in range(heads)]
        dq_acc[...] = jnp.zeros_like(dq_acc)

        @pl.loop(low_ref[qi], high_ref[qi])
        def _(ki):
            key0 = pl.multiple_of(ki * TILE, TILE)
            allowed = allowed_tile(code_ref, seg_ref, key0, query0)
            keys = k_ref[0, pl.ds(key0, TILE), :]
            values = v_ref[0, pl.ds(key0, TILE), :]
            keys_t = keys.T
            dk = dk_acc[pl.ds(key0, TILE), :]
            dv = dv_acc[pl.ds(key0, TILE), :]
            for h in range(heads):
                scores = jnp.where(allowed, dot_nt(keys, q_each[h]), -1e30)
                probs = jnp.exp(scores - lse[h])
                gprobs = dot_nt(values, g_each[h])
                gscores = (probs * (gprobs - inner[h])).astype(BF16)
                dv = dv + dot_nn(probs.astype(BF16), g_each[h])
                dk = dk + dot_nn(gscores, q_each[h])
                lanes_h = slice(h * HEAD_DIM, (h + 1) * HEAD_DIM)
                dq_acc[h] += dot_nn(keys_t[lanes_h], gscores)
            dk_acc[pl.ds(key0, TILE), :] = dk
            dv_acc[pl.ds(key0, TILE), :] = dv

        both = jnp.concatenate([dq_acc[h] for h in range(heads)], axis=0) * 0.125
        dq_ref[0, pl.ds(query0, TILE), :] = both.astype(BF16).T

    low_k = dk_acc[...].astype(BF16)
    low_v = dv_acc[...].astype(BF16)
    dk_ref[0] = low_k
    dv_ref[0] = low_v
    qsum_ref[0] = jnp.sum(dq_ref[0].astype(F32), axis=0, keepdims=True)
    vsum_ref[0] = jnp.sum(low_v.astype(F32), axis=0, keepdims=True)


def attend_back(projected, context, grad_context, lse, low, high, codes, seg_row):
    parts, rows, wide = projected.shape
    lanes = 128
    heads = lanes // HEAD_DIM
    groups = wide // 3 // lanes
    flat = pl.BlockSpec((1, rows, lanes), lambda t, j, lo, hi: (t, 0, j))
    sums = pl.BlockSpec((1, 1, lanes), lambda t, j, lo, hi: (t, 0, j))
    return pl.pallas_call(
        attend_back_kernel,
        grid_spec=pltpu.PrefetchScalarGridSpec(
            num_scalar_prefetch=2,
            grid=(parts, groups),
            in_specs=[
                pl.BlockSpec((rows, 128), lambda t, j, lo, hi: (0, 0)),
                pl.BlockSpec((1, rows), lambda t, j, lo, hi: (0, 0)),
                pl.BlockSpec((1, rows, lanes), lambda t, j, lo, hi: (t, 0, j)),
                pl.BlockSpec((1, rows, lanes), lambda t, j, lo, hi: (t, 0, groups + j)),
                pl.BlockSpec((1, rows, lanes), lambda t, j, lo, hi: (t, 0, 2 * groups + j)),
                flat,
                flat,
                pl.BlockSpec((1, heads, rows), lambda t, j, lo, hi: (t * groups + j, 0, 0)),
            ],
            out_specs=[flat, flat, flat, sums, sums],
            scratch_shapes=[
                pltpu.VMEM((heads, HEAD_DIM, TILE), F32),
                pltpu.VMEM((rows, lanes), F32),
                pltpu.VMEM((rows, lanes), F32),
            ],
        ),
        out_shape=[jax.ShapeDtypeStruct((parts, rows, wide // 3), BF16)] * 3
        + [jax.ShapeDtypeStruct((parts, 1, wide // 3), F32)] * 2,
        compiler_params=params(),
        name="attend_back",
    )(low, high, codes, seg_row, projected, projected, projected, context, grad_context, lse)


def norm_forward(v):
    mean = jnp.mean(v, axis=-1, keepdims=True)
    centered = v - mean
    factor = lax.rsqrt(jnp.mean(centered * centered, axis=-1, keepdims=True) + EPS)
    return centered * factor, factor


def norm_back(inner, normed, factor):
    return factor * (
        inner
        - jnp.mean(inner, axis=-1, keepdims=True)
        - normed * jnp.mean(inner * normed, axis=-1, keepdims=True)
    )


def col_sum(v):
    return jnp.sum(v, axis=0, keepdims=True)


UNIT_STEP = 512


def forward_block(x, context, out_weight, up_weight, vec_ref, bup_ref, rows_at, refs):
    normed_ref, factor_ref, act_ref, slope_ref = refs
    parts, _, units = act_ref.shape
    first_sum = x.astype(F32) + vec_ref[0:1]
    for t in range(parts):
        first_sum = first_sum + dot_nt(context(t), out_weight(t))
    normed, factor = norm_forward(first_sum)
    normed_ref[rows_at, :] = normed
    factor_ref[rows_at, :] = jnp.broadcast_to(factor, (factor.shape[0], 128))
    hidden_low = (normed * vec_ref[1:2] + vec_ref[2:3]).astype(BF16)
    for t in range(parts):
        for u in range(0, units, UNIT_STEP):
            at = slice(u, u + UNIT_STEP)
            up = dot_nn(hidden_low, up_weight(t, at)) + bup_ref[t, :, at]
            half = 0.5 * (1.0 + lax.erf(up * 0.7071067811865476))
            act_ref[t, rows_at, at] = (up * half).astype(BF16)
            slope = half + up * jnp.exp(-0.5 * up * up) * 0.3989422804014327
            slope_ref[t, rows_at, at] = slope


def forward_kernel(x_ref, ctx_ref, wo_ref, up_ref, vec_ref, bup_ref, *refs):
    forward_block(
        x_ref[...],
        lambda t: ctx_ref[t],
        lambda t: wo_ref[t, 0],
        lambda t, at: up_ref[t, 0, :, at],
        vec_ref,
        bup_ref,
        slice(None),
        refs,
    )


def forward_shapes(parts, rows, width, units):
    return [
        jax.ShapeDtypeStruct((rows, width), F32),
        jax.ShapeDtypeStruct((rows, 128), F32),
        jax.ShapeDtypeStruct((parts, rows, units), BF16),
        jax.ShapeDtypeStruct((parts, rows, units), F32),
    ]


def rows_forward(x, context, first, rest, vectors, bias_up):
    rows, width = x.shape
    parts, _, _, units = rest.shape
    part_width = context.shape[2]
    step = min(256, rows)
    last = units // part_width - 1
    row = pl.BlockSpec((step, width), lambda i: (i, 0))
    wide = pl.BlockSpec((parts, step, units), lambda i: (0, i, 0))
    return pl.pallas_call(
        forward_kernel,
        grid=(rows // step,),
        in_specs=[
            row,
            pl.BlockSpec((parts, step, part_width), lambda i: (0, i, 0)),
            pl.BlockSpec((parts, 1, width, part_width), lambda i: (0, 0, 0, last)),
            pl.BlockSpec((parts, 1, width, units), lambda i: (0, 0, 0, 0)),
            pl.BlockSpec((8, width), lambda i: (0, 0)),
            pl.BlockSpec((parts, 1, units), lambda i: (0, 0, 0)),
        ],
        out_specs=[row, pl.BlockSpec((step, 128), lambda i: (i, 0)), wide, wide],
        out_shape=forward_shapes(parts, rows, width, units),
        compiler_params=params(),
        name="rows_forward",
    )(x, context, first, rest, vectors, bias_up)


def rows_kernel(
    normed_ref,
    factor_ref,
    act_ref,
    slope_ref,
    g_ref,
    wo_ref,
    up_ref,
    down_ref,
    vec_ref,
    out_ref,
    hid_ref,
    sec_ref,
    first_ref,
    gfirst_ref,
    gup_ref,
    gctx_ref,
    sums_ref,
    upsum_ref,
):
    parts, _, units = act_ref.shape

    @pl.when(pl.program_id(0) == 0)
    def _():
        sums_ref[...] = jnp.zeros_like(sums_ref)
        upsum_ref[...] = jnp.zeros_like(upsum_ref)

    gain_one, shift_one = vec_ref[1:2], vec_ref[2:3]
    b_down, gain_two, shift_two = vec_ref[3:4], vec_ref[4:5], vec_ref[5:6]
    hidden = normed_ref[...] * gain_one + shift_one
    hid_ref[...] = hidden.astype(BF16)
    second_sum = hidden + b_down
    for t in range(parts):
        second_sum = second_sum + dot_nt(act_ref[t], down_ref[t, 0])
    normed_two, factor_two = norm_forward(second_sum)
    out_ref[...] = (normed_two * gain_two + shift_two).astype(BF16)
    grad_out = g_ref[...].astype(F32)
    grad_second = norm_back(grad_out * gain_two, normed_two, factor_two)
    second_low = grad_second.astype(BF16)
    sec_ref[...] = second_low
    grad_hidden = grad_second
    for t in range(parts):
        for u in range(0, units, UNIT_STEP):
            at = slice(u, u + UNIT_STEP)
            grad_up = (dot_nn(second_low, down_ref[t, 0, :, at]) * slope_ref[t, :, at]).astype(BF16)
            gup_ref[t, :, at] = grad_up
            upsum_ref[t, :, at] += col_sum(grad_up.astype(F32))
            grad_hidden = grad_hidden + dot_nt(grad_up, up_ref[t, 0, :, at])
    normed_one = normed_ref[...]
    grad_first = norm_back(grad_hidden * gain_one, normed_one, factor_ref[:, 0:1])
    gfirst_ref[...] = grad_first
    first_low = grad_first.astype(BF16)
    first_ref[...] = first_low
    for t in range(parts):
        gctx_ref[t] = dot_nn(first_low, wo_ref[t, 0]).astype(BF16)
    sums_ref[0:1] += col_sum(grad_first)
    sums_ref[1:2] += col_sum(grad_hidden * normed_one)
    sums_ref[2:3] += col_sum(grad_hidden)
    sums_ref[3:4] += col_sum(grad_second)
    sums_ref[4:5] += col_sum(grad_out * normed_two)
    sums_ref[5:6] += col_sum(grad_out)


def rows_pass(normed, factor, active, slope, grads, first, rest, vectors):
    rows, width = normed.shape
    parts, _, units = active.shape
    part_width = first.shape[3] // 4
    step = min(256, rows)
    row = pl.BlockSpec((step, width), lambda i: (i, 0))
    split = pl.BlockSpec((parts, step, part_width), lambda i: (0, i, 0))
    wide = pl.BlockSpec((parts, step, units), lambda i: (0, i, 0))
    once = pl.Buffered(1)
    last = units // part_width - 1
    return pl.pallas_call(
        rows_kernel,
        grid=(rows // step,),
        in_specs=[
            row,
            pl.BlockSpec((step, 128), lambda i: (i, 0)),
            wide,
            wide,
            row,
            pl.BlockSpec(
                (parts, 1, width, part_width), lambda i: (0, 0, 0, last), pipeline_mode=once
            ),
            pl.BlockSpec((parts, 1, width, units), lambda i: (0, 0, 0, 0), pipeline_mode=once),
            pl.BlockSpec((parts, 1, width, units), lambda i: (0, 1, 0, 0), pipeline_mode=once),
            pl.BlockSpec((8, width), lambda i: (0, 0)),
        ],
        out_specs=[
            row,
            row,
            row,
            row,
            row,
            wide,
            split,
            pl.BlockSpec((8, width), lambda i: (0, 0)),
            pl.BlockSpec((parts, 1, units), lambda i: (0, 0, 0)),
        ],
        out_shape=[
            jax.ShapeDtypeStruct((rows, width), BF16),
            jax.ShapeDtypeStruct((rows, width), BF16),
            jax.ShapeDtypeStruct((rows, width), BF16),
            jax.ShapeDtypeStruct((rows, width), BF16),
            jax.ShapeDtypeStruct((rows, width), F32),
            jax.ShapeDtypeStruct((parts, rows, units), BF16),
            jax.ShapeDtypeStruct((parts, rows, part_width), BF16),
            jax.ShapeDtypeStruct((8, width), F32),
            jax.ShapeDtypeStruct((parts, 1, units), F32),
        ],
        compiler_params=params(),
        name="rows_pass",
    )(normed, factor, active, slope, grads, first, rest, rest, vectors)


GRAD_STEP = 256


def outer_kernel(rows_ref, cols_ref, out_ref):
    width = rows_ref.shape[1]
    for m in range(0, width, GRAD_STEP):
        at = slice(m, m + GRAD_STEP)
        out_ref[0, at, :] = dot_tn(rows_ref[:, at], cols_ref[0]).astype(BF16)


def outer(left, right):
    rows, width = left.shape
    parts, _, units = right.shape
    return pl.pallas_call(
        outer_kernel,
        grid=(parts,),
        in_specs=[
            pl.BlockSpec((rows, width), lambda t: (0, 0)),
            pl.BlockSpec((1, rows, units), lambda t: (t, 0, 0)),
        ],
        out_specs=pl.BlockSpec((1, width, units), lambda t: (t, 0, 0)),
        out_shape=jax.ShapeDtypeStruct((parts, width, units), BF16),
        compiler_params=params(),
        name="outer",
    )(left, right)


def outer_four_kernel(x_ref, first_ref, q_ref, k_ref, v_ref, ctx_ref, out_ref):
    width = x_ref.shape[1]
    part_width = q_ref.shape[2]
    for m in range(0, width, GRAD_STEP):
        at = slice(m, m + GRAD_STEP)
        for n, cols in enumerate((q_ref, k_ref, v_ref, ctx_ref)):
            left = first_ref if n == 3 else x_ref
            part = dot_tn(left[:, at], cols[0])
            out_ref[0, at, n * part_width : (n + 1) * part_width] = part.astype(BF16)


def outer_four(x, first_low, grad_q, grad_k, grad_v, context):
    rows, width = x.shape
    parts, _, part_width = context.shape
    row = pl.BlockSpec((rows, width), lambda t: (0, 0))
    split = pl.BlockSpec((1, rows, part_width), lambda t: (t, 0, 0))
    return pl.pallas_call(
        outer_four_kernel,
        grid=(parts,),
        in_specs=[row, row, split, split, split, split],
        out_specs=pl.BlockSpec((1, width, 4 * part_width), lambda t: (t, 0, 0)),
        out_shape=jax.ShapeDtypeStruct((parts, width, 4 * part_width), BF16),
        compiler_params=params(),
        name="outer_four",
    )(x, first_low, grad_q, grad_k, grad_v, context)


def input_grad_kernel(base_ref, q_ref, k_ref, v_ref, w_ref, out_ref):
    parts, _, part_width = q_ref.shape
    total = base_ref[...]
    for t in range(parts):
        for c, cols in enumerate((q_ref, k_ref, v_ref)):
            at = slice(c * part_width, (c + 1) * part_width)
            total = total + dot_nt(cols[t], w_ref[t, 0, :, at])
    out_ref[...] = total.astype(out_ref.dtype)


def input_grad(grad_first, grad_q, grad_k, grad_v, weights):
    rows, width = grad_first.shape
    parts, _, part_width = grad_q.shape
    step = min(256, rows)
    row = pl.BlockSpec((step, width), lambda i: (i, 0))
    split = pl.BlockSpec((parts, step, part_width), lambda i: (0, i, 0))
    return pl.pallas_call(
        input_grad_kernel,
        grid=(rows // step,),
        in_specs=[
            row,
            split,
            split,
            split,
            pl.BlockSpec((parts, 1, width, 3 * part_width), lambda i: (0, 0, 0, 0)),
        ],
        out_specs=row,
        out_shape=jax.ShapeDtypeStruct((rows, width), BF16),
        compiler_params=params(),
        name="input_grad",
    )(grad_first, grad_q, grad_k, grad_v, weights)


LINE = 4
CHUNK = 64


class Place:
    def __init__(self):
        dp = lax.axis_index("dp")
        self.y = lax.axis_index("tensor")
        self.core = lax.rem(dp, 2)
        self.x = lax.rem(lax.div(dp, 2), 2)
        self.z = lax.div(dp, 4)

    @staticmethod
    def at(z, x, core, y):
        return ((z * 2 + x) * 2 + core, y)

    def corners(self, mixed, core=None):
        core = self.core if core is None else core
        side = 1 - (1 - core) * mixed
        first = (lax.rem(self.y + side, 2), lax.rem(self.x + 1 - side, 2))
        second = (lax.rem(self.y + 1 - side, 2), lax.rem(self.x + side, 2))
        return ((self.y, self.x), first, second, (1 - self.y, 1 - self.x))

    def chip(self, corner):
        return self.at(self.z, corner[1], self.core, corner[0])

    def along(self, o):
        return lax.rem(self.z + o, LINE)

    def back(self, o):
        return lax.rem(self.z + LINE - o, LINE)

    def line(self, o):
        return self.at(self.along(o), self.x, self.core, self.y)

    def partner(self):
        return self.at(self.z, self.x, 1 - self.core, self.y)

    def across_x(self):
        return self.at(self.z, 1 - self.x, self.core, self.y)

    def across_y(self):
        return self.at(self.z, self.x, self.core, 1 - self.y)

    def greet(self):
        barrier = pltpu.get_barrier_semaphore()
        others = [self.across_x(), self.across_y(), self.partner()]
        others += [self.line(o) for o in range(1, LINE)]
        for device in others:
            pl.semaphore_signal(
                barrier, inc=1, device_id=device, device_id_type=pl.DeviceIdType.MESH
            )
        pl.semaphore_wait(barrier, len(others))


def remote(src, dst, sends, recvs, slot, device):
    return pltpu.make_async_remote_copy(
        src_ref=src,
        dst_ref=dst,
        send_sem=sends.at[slot],
        recv_sem=recvs.at[slot],
        device_id=device,
        device_id_type=pl.DeviceIdType.MESH,
    )


PER_PIECE = 8


def gather_kernel(
    shard_ref,
    in_ref,
    bias_ref,
    code_ref,
    seg_ref,
    docs_ref,
    bars_ref,
    vec_ref,
    bup_ref,
    grad_ref,
    first_ref,
    rest_out,
    x_ref,
    g_ref,
    proj_ref,
    ctx_ref,
    lse_ref,
    normed_out,
    factor_out,
    act_out,
    slope_out,
    rest_ref,
    normed_buf,
    factor_buf,
    act_buf,
    slope_buf,
    sends,
    recvs,
    local_sem,
    rows_sem,
    turned,
    score_buf,
    expo_buf,
):
    place = Place()
    z, x, y, core = place.z, place.x, place.y, place.core
    chunks = shard_ref.shape[0]
    parts, rows, wide = proj_ref.shape
    last = chunks * LINE * PER_PIECE
    place.greet()

    def copy(k, o, n, src, dst, device):
        return remote(src, dst, sends, recvs, (k * LINE + o) * PER_PIECE + n, device)

    def slot(k, yy, zz, xx, cc):
        if isinstance(k, int) and k == 0:
            return first_ref.at[yy, zz, xx, cc]
        return rest_ref.at[yy, k - 1, zz, xx, cc]

    def where(k, cc=None):
        return place.corners(0, cc)

    def held(k, o, corner, cc=core):
        return slot(k, corner[0], place.back(o), corner[1], cc)

    def to_line(k, o):
        here = slot(k, y, z, x, core)
        return copy(k, o, 0, shard_ref.at[k], here, place.line(o))

    def from_line(k, o):
        here = held(k, o, (y, x))
        return copy(k, o, 0, here, here, place.line(o))

    def hop(k, o, n, corner, device):
        here = held(k, o, where(k)[corner])
        return copy(k, o, n, here, here, device)

    def to_first(k, o):
        return hop(k, o, 1, 0, place.chip(where(k)[1]))

    def from_first(k, o):
        return hop(k, o, 1, 1, place.chip(where(k)[1]))

    def to_second(k, o, n):
        return hop(k, o, 2 + n, n, place.chip(where(k)[2]))

    def from_second(k, o, n):
        return hop(k, o, 2 + n, 2 + n, place.chip(where(k)[2]))

    def to_partner(k, o, n):
        return hop(k, o, 4 + n, n, place.partner())

    def from_partner(k, o, n):
        here = held(k, o, where(k, 1 - core)[n], 1 - core)
        return copy(k, o, 4 + n, here, here, place.partner())

    final = chunks - 1

    def corner_of(n):
        return lax.rem(y + lax.rem(n, 2), 2), lax.rem(x + lax.div(n, 2), 2)

    def final_line(o, n):
        here = held(final, 0, corner_of(n))
        return copy(final, o, n, here, here, place.line(o))

    def final_from(o, n):
        here = held(final, o, corner_of(n))
        return copy(final, o, n, here, here, place.line(o))

    def final_partner(o, n):
        here = held(final, o, corner_of(n))
        return copy(final, o, 4 + n, here, here, place.partner())

    trade = remote(in_ref.at[1 - y], x_ref.at[y], sends, recvs, last, place.across_y())
    arrive = remote(in_ref.at[y], x_ref.at[1 - y], sends, recvs, last, place.across_y())
    trade_g = remote(grad_ref.at[1 - y], g_ref.at[y], sends, recvs, last + 1, place.across_y())
    arrive_g = remote(
        grad_ref.at[y], g_ref.at[1 - y], sends, recvs, last + 1, place.across_y()
    )
    keep_g = pltpu.make_async_copy(grad_ref.at[y], g_ref.at[y], local_sem.at[chunks + 1])
    keep_g.start()
    local = [pltpu.make_async_copy(in_ref.at[y], x_ref.at[y], local_sem.at[chunks])]
    for k in range(chunks):
        own = slot(k, y, z, x, core)
        local.append(pltpu.make_async_copy(shard_ref.at[k], own, local_sem.at[k]))
    for part in local:
        part.start()
    for k in range(final):
        for o in (2, 1, 3):
            to_line(k, o).start()
    for part in local:
        part.wait()

    def start_line(k, o):
        to_first(k, o).start()
        to_second(k, o, 0).start()
        to_partner(k, o, 0).start()

    def arrive_first(k, o):
        from_first(k, o).wait_recv()
        to_second(k, o, 1).start()
        to_partner(k, o, 1).start()

    def arrive_second(k, o):
        for n in range(2):
            from_second(k, o, n).wait_recv()
            to_partner(k, o, 2 + n).start()

    order = (0, 1, 3, 2)
    lead = 2
    for i in range(LINE + lead):
        k, o = i // LINE, order[i % LINE]
        if o > 0:
            from_line(k, o).wait_recv()
        start_line(k, o)
        if i == 0:
            start_line(final, 0)
            trade.start()
        if i == 2:
            arrive_first(final, 0)
        if i == 3:
            arrive_second(final, 0)
            for n in range(4):
                for oo in (2, 1, 3):
                    final_line(oo, n).start()
        if i >= 1:
            arrive_first((i - 1) // LINE, order[(i - 1) % LINE])
        if i >= 2:
            arrive_second((i - 2) // LINE, order[(i - 2) % LINE])
    arrive.wait_recv()
    for o in order:
        for n in range(4):
            from_partner(0, o, n).wait_recv()

    step = 256

    def project_slice(i):
        t = lax.div(i, rows // step)
        row = lax.rem(i, rows // step)
        half = lax.div(row * step, x_ref.shape[1])
        row0 = pl.multiple_of(lax.rem(row * step, x_ref.shape[1]), step)
        left = x_ref[half, pl.ds(row0, step), :]
        right = first_ref[t, :, :, :, :, :wide].reshape(-1, wide)
        value = dot_nn(left, right) + bias_ref[t]
        proj_ref[t, pl.ds(pl.multiple_of(row * step, step), step), :] = value.astype(BF16)

    lanes = 128
    groups = wide // 3 // lanes
    heads = lanes // HEAD_DIM
    tiles = rows // TILE
    masks = head_masks(lanes)

    def attend_slice(i):
        group = lax.div(i, tiles)
        qi = lax.rem(i, tiles)
        t = lax.div(group, groups)
        j = lax.rem(group, groups)

        def lane(c):
            return pl.ds(pl.multiple_of((c * groups + j) * lanes, lanes), lanes)

        def at(ki):
            return pl.ds(pl.multiple_of(ki * TILE, TILE), TILE)

        @pl.when(qi == 0)
        def _():
            for ki in range(tiles):
                turned[ki] = proj_ref[t, ki * TILE : (ki + 1) * TILE, lane(2)].T

        here = at(qi)
        queries = proj_ref[t, here, lane(0)] * BF16(0.125)
        own_docs = docs_ref[here, :]
        allowed = allowed_tile(code_ref, seg_ref, qi * TILE, qi * TILE)
        others = [lax.rem(qi + r, tiles) for r in range(tiles)]
        keys = [proj_ref[t, at(ki), lane(1)] for ki in others]
        values_t = jnp.concatenate([turned[ki] for ki in others], axis=1)
        for r in range(1, tiles):
            keys[r] = jnp.concatenate([keys[r], bars_ref[at(others[r]), :]], axis=1)
        most = []
        for h in range(heads):
            plain = queries * masks[h]
            marked = jnp.concatenate([plain, own_docs], axis=1)
            peak = None
            for r in range(tiles):
                if r == 0:
                    scores = jnp.where(allowed, dot_nt(keys[0], plain), -1e30)
                else:
                    scores = dot_nt(keys[r], marked)
                score_buf[h, r * TILE : (r + 1) * TILE, :] = scores
                part = jnp.max(scores.reshape(-1, 8, TILE), axis=0)
                peak = part if peak is None else jnp.maximum(peak, part)
            most.append(jnp.max(peak, axis=0, keepdims=True))
        done = []
        for h in range(heads):
            total = None
            for c in range(0, tiles * TILE, CHUNK):
                expo = jnp.exp(score_buf[h, c : c + CHUNK, :] - most[h])
                expo_buf[h, c : c + CHUNK, :] = expo.astype(BF16)
                part = jnp.sum(expo.reshape(-1, 8, TILE), axis=0)
                total = part if total is None else total + part
            total = jnp.sum(total, axis=0, keepdims=True)
            part = dot_nn(values_t[h * HEAD_DIM : (h + 1) * HEAD_DIM], expo_buf[h])
            done.append(part / total)
            lse_ref[group, h : h + 1, here] = most[h] + jnp.log(total)
        ctx_ref[t, here, lane(0)] = jnp.concatenate(done, axis=0).astype(BF16).T

    def rows_copies(i):
        at = pl.ds(pl.multiple_of(i * step, step), step)
        pairs = (
            (normed_buf.at[at, :], normed_out.at[at, :]),
            (factor_buf.at[at, :], factor_out.at[at, :]),
            (act_buf.at[:, at, :], act_out.at[:, at, :]),
            (slope_buf.at[:, at, :], slope_out.at[:, at, :]),
        )
        return [
            pltpu.make_async_copy(src, dst, rows_sem.at[i * 4 + n])
            for n, (src, dst) in enumerate(pairs)
        ]

    def rows_slice(i):
        at = pl.ds(pl.multiple_of(i * step, step), step)
        half = lax.div(i * step, x_ref.shape[1])
        row0 = pl.multiple_of(lax.rem(i * step, x_ref.shape[1]), step)
        forward_block(
            x_ref[half, pl.ds(row0, step), :],
            lambda t: ctx_ref[t, at, :],
            lambda t: first_ref[t, :, :, :, :, wide:].reshape(-1, wide // 3),
            lambda t, cols: rest_ref[t, 0, :, :, :, :, cols].reshape(-1, UNIT_STEP),
            vec_ref,
            bup_ref,
            at,
            (normed_buf, factor_buf, act_buf, slope_buf),
        )
        for part in rows_copies(i):
            part.start()

    keep_rest = [
        pltpu.make_async_copy(
            rest_ref.at[t, k], rest_out.at[t, k], local_sem.at[chunks + 2 + parts * k + t]
        )
        for k in range(chunks - 1)
        for t in range(parts)
    ]
    count = (chunks - 1) * LINE
    heavy = 1
    calm = 2
    project_share = parts * (rows // step) // heavy
    attend_share = parts * groups * tiles // calm
    row_slices = rows // step
    rows_from = count - row_slices

    late = 2 * (LINE - 1)

    def split(r):
        return jnp.where(r < 2, r, 5 - r)

    def pass_final(q):
        n, r = lax.div(q, LINE - 1), lax.rem(q, LINE - 1)
        o = jnp.where(r == 0, 2, jnp.where(r == 1, 1, 3))
        final_from(o, n).wait_recv()
        final_partner(o, n).start()

    @pl.loop(0, count)
    def _(p):
        @pl.when(p + lead < LINE)
        def _():
            o = split(p + lead)

            @pl.when(o > 0)
            def _():
                from_line(1, o).wait_recv()

            start_line(1, o)

        @pl.when(p + lead - 1 < LINE)
        def _():
            arrive_first(1, split(p + lead - 1))

        @pl.when(p + lead - 2 < LINE)
        def _():
            arrive_second(1, split(p + lead - 2))

        @pl.when(p >= count - late)
        def _():
            for e in range(2):
                pass_final(2 * (p - count + late) + e)

        @pl.when(p == heavy + calm)
        def _():
            trade_g.start()

        @pl.when(p < heavy)
        def _():
            @pl.loop(0, project_share)
            def _(n):
                project_slice(p * project_share + n)

        @pl.when((p >= heavy) & (p < heavy + calm))
        def _():
            @pl.loop(0, attend_share)
            def _(n):
                attend_slice((p - heavy) * attend_share + n)

        @pl.when(p == rows_from)
        def _():
            for o in order:
                for n in range(4):
                    from_partner(1, o, n).wait_recv()
            for part in keep_rest[:parts]:
                part.start()

        @pl.when(p >= rows_from)
        def _():
            rows_slice(p - rows_from)

    for o in order:
        for n in range(4):
            from_partner(2, o, n).wait_recv()
    for part in keep_rest[parts:]:
        part.start()

    for k in range(final):
        for o in order:
            if o > 0:
                to_line(k, o).wait_send()
            to_first(k, o).wait_send()
            for n in range(2):
                to_second(k, o, n).wait_send()
            for n in range(4):
                to_partner(k, o, n).wait_send()
    to_first(final, 0).wait_send()
    for n in range(2):
        to_second(final, 0, n).wait_send()
    for n in range(4):
        to_partner(final, 0, n).wait_send()
        for o in range(1, LINE):
            final_line(o, n).wait_send()
            final_partner(o, n).wait_send()
    trade.wait_send()
    trade_g.wait_send()
    arrive_g.wait_recv()
    keep_g.wait()
    for part in keep_rest:
        part.wait()
    for i in range(row_slices):
        for part in rows_copies(i):
            part.wait()


def gather_all(shard, halves, bias, codes, seg_row, docs, bars, vectors, bias_up, grad_halves):
    chunks, own_rows, units = shard.shape
    parts, rows, width = halves.shape
    wide = bias.shape[-1]
    length = parts * rows
    groups = wide // 3 // 128
    anywhere = pl.BlockSpec(memory_space=pl.ANY)
    local = pl.BlockSpec(memory_space=pltpu.VMEM)
    copies = chunks * LINE * PER_PIECE + 2
    places = (LINE, 2, 2, own_rows, units)
    forward = forward_shapes(parts, length, width, units)
    first, rest, x, grads, projected, context, lse, *state = pl.pallas_call(
        gather_kernel,
        in_specs=[local] * 9 + [anywhere],
        out_specs=[local, anywhere, local, anywhere, local, local, local] + [anywhere] * 4,
        out_shape=[
            jax.ShapeDtypeStruct((parts,) + places, BF16),
            jax.ShapeDtypeStruct((parts, chunks - 1) + places, BF16),
            jax.ShapeDtypeStruct((parts, rows, width), BF16),
            jax.ShapeDtypeStruct((parts, rows, width), BF16),
            jax.ShapeDtypeStruct((parts, length, wide), BF16),
            jax.ShapeDtypeStruct((parts, length, wide // 3), BF16),
            jax.ShapeDtypeStruct((parts * groups, 2, length), F32),
        ]
        + forward,
        scratch_shapes=[
            pltpu.VMEM((parts, chunks - 1) + places, BF16),
        ]
        + [pltpu.VMEM(s.shape, s.dtype) for s in forward]
        + [
            pltpu.SemaphoreType.DMA((copies,)),
            pltpu.SemaphoreType.DMA((copies,)),
            pltpu.SemaphoreType.DMA((chunks + 2 + parts * (chunks - 1),)),
            pltpu.SemaphoreType.DMA((length // 256 * 4,)),
            pltpu.VMEM((length // TILE, 128, TILE), BF16),
            pltpu.VMEM((2, length, TILE), F32),
            pltpu.VMEM((2, length, TILE), BF16),
        ],
        compiler_params=params(collective_id=0, has_side_effects=True),
        name="gather_all",
    )(shard, halves, bias, codes, seg_row, docs, bars, vectors, bias_up, grad_halves)
    first = first.reshape(parts, 1, -1, units)
    rest = rest.reshape(parts, chunks - 1, -1, units)
    x, grads = x.reshape(length, width), grads.reshape(length, width)
    return first, rest, x, grads, projected, context, lse, state


def back_kernel(
    b_ref,
    c_ref,
    x_ref,
    first_ref,
    base_ref,
    proj_ref,
    ctx_ref,
    g_ref,
    lse_ref,
    code_ref,
    seg_ref,
    docs_ref,
    bars_ref,
    w_ref,
    small_ref,
    res_ref,
    out_ref,
    xr_ref,
    rr_ref,
    total_ref,
    a_buf,
    dp_buf,
    xg_buf,
    p_buf,
    s_buf,
    f_buf,
    z_buf,
    t_buf,
    turned,
    score_buf,
    gprob_buf,
    prob_buf,
    gscore_buf,
    dk_acc,
    dv_acc,
    sends,
    recvs,
    t_send,
    t_recv,
    local_sem,
):
    place = Place()
    z, x, y, core = place.z, place.x, place.y, place.core
    chunks = out_ref.shape[0]
    own_rows = out_ref.shape[1]
    parts, rows, wide = proj_ref.shape
    part_width = wide // 3
    width = x_ref.shape[1]
    place.greet()

    def where(k):
        return place.corners(int(k == 0) if isinstance(k, int) else 0)

    def copy(k, o, n, src, dst, device):
        return remote(src, dst, sends, recvs, (k * LINE + o) * PER_PIECE + n, device)

    def a_rows(zz, xx, cc):
        start = pl.multiple_of(((zz * 2 + xx) * 2 + cc) * own_rows, own_rows)
        return pl.ds(start, own_rows)

    def to_partner_a(o, n):
        yy, xx = n // 2, n % 2
        src = a_buf.at[yy, a_rows(place.along(o), xx, 1 - core)]
        slot = (0, 5, 6, 7)[n]
        return copy(0, o, slot, src, p_buf.at[0, o, yy, xx], place.partner())

    def to_partner(source, k, o):
        src = source.at[:, place.along(o), :, 1 - core]
        return copy(k, o, 0, src, p_buf.at[k, o], place.partner())

    def to_second(k, o, n):
        yy, xx = where(k)[2 + n]
        device = place.chip(where(k)[2])
        return copy(k, o, 1 + n, p_buf.at[k, o, yy, xx], s_buf.at[k, o, n], device)

    def to_first(k, o):
        device = place.chip(where(k)[1])
        return copy(k, o, 3, s_buf.at[k, o, 1], f_buf.at[k, o], device)

    def to_line(k, o):
        return copy(k, o, 4, f_buf.at[k, o], z_buf.at[k, o - 1], place.line(o))

    def small_copy(n, src, dst, device):
        return remote(src, dst, t_send, t_recv, n, device)

    hops = (
        small_copy(0, t_buf.at[9], t_buf.at[0], place.partner()),
        small_copy(1, t_buf.at[1], t_buf.at[2], place.across_x()),
        small_copy(2, t_buf.at[3], t_buf.at[4], place.across_y()),
    )

    def small_line(o):
        return small_copy(2 + o, t_buf.at[5 + z], t_buf.at[5 + z], place.line(o))

    def small_from(o):
        here = t_buf.at[5 + place.back(o)]
        return small_copy(2 + o, here, here, place.line(o))

    def small_step(step):
        if step == 0:
            hops[0].start()
        elif step == 1:
            hops[0].wait_recv()
            t_buf[1] = t_buf[9] + t_buf[0]
            hops[1].start()
        elif step == 2:
            hops[1].wait_recv()
            t_buf[3] = t_buf[1] + t_buf[2]
            hops[2].start()
        elif step == 3:
            hops[2].wait_recv()
            t_buf[5 + z] = t_buf[3] + t_buf[4]
            for o in range(1, LINE):
                small_line(o).start()
        elif step == 4:
            for o in range(1, LINE):
                small_from(o).wait_recv()
            total_ref[...] = (t_buf[5] + t_buf[6]) + (t_buf[7] + t_buf[8])

    trade = small_copy(2 + LINE, xg_buf.at[1 - y], xr_ref.at[y], place.across_y())
    arrive = small_copy(2 + LINE, xg_buf.at[1 - y], xr_ref.at[1 - y], place.across_y())
    keep = pltpu.make_async_copy(xg_buf.at[y], xr_ref.at[y], local_sem.at[0])
    trade_r = small_copy(3 + LINE, res_ref.at[1 - y], rr_ref.at[y], place.across_y())
    arrive_r = small_copy(3 + LINE, res_ref.at[1 - y], rr_ref.at[1 - y], place.across_y())
    keep_r = pltpu.make_async_copy(res_ref.at[y], rr_ref.at[y], local_sem.at[1])

    def add_partner(k, o, own):
        for n in (3, 2, 1, 0):
            yy, xx = where(k)[n]
            p_buf[k, o, yy, xx] = p_buf[k, o, yy, xx] + own(yy, xx)
            if n >= 2:
                to_second(k, o, n - 2).start()

    def stage_partner(source, k, o):
        to_partner(source, k, o).wait_recv()
        zz = place.along(o)
        add_partner(k, o, lambda yy, xx: source[yy, zz, xx, core])

    def stage_second(k, o):
        for n in (1, 0):
            yy, xx = where(k)[n]
            to_second(k, o, n).wait_recv()
            s_buf[k, o, n] = s_buf[k, o, n] + p_buf[k, o, yy, xx]
            if n == 1:
                to_first(k, o).start()

    def stage_first(k, o):
        to_first(k, o).wait_recv()
        f_buf[k, o] = f_buf[k, o] + s_buf[k, o, 0]

    def finish(k):
        total = f_buf[k, 0].astype(F32)
        for o in range(1, LINE):
            to_line(k, o).wait_recv()
            total = total + z_buf[k, o - 1].astype(F32)
        out_ref[k] = total

    lanes = 128
    groups = part_width // lanes
    heads = lanes // HEAD_DIM
    tiles = rows // TILE
    masks = head_masks(lanes)
    q_row = small_ref.shape[0] - (2 * parts * groups + parts * w_ref.shape[3] // lanes)

    def lane(c, j):
        return pl.ds(pl.multiple_of((c * groups + j) * lanes, lanes), lanes)

    def at(ki):
        return pl.ds(pl.multiple_of(ki * TILE, TILE), TILE)

    def attend_slice(i):
        group = lax.div(i, tiles)
        qi = lax.rem(i, tiles)
        t = lax.div(group, groups)
        j = lax.rem(group, groups)

        @pl.when(qi == 0)
        def _():
            dk_acc[...] = jnp.zeros_like(dk_acc)
            dv_acc[...] = jnp.zeros_like(dv_acc)
            for ki in range(tiles):
                turned[ki] = proj_ref[t, ki * TILE : (ki + 1) * TILE, lane(1, j)].T

        here = at(qi)
        queries = proj_ref[t, here, lane(0, j)] * BF16(0.125)
        grads = g_ref[t, here, lane(0, j)]
        own_docs = docs_ref[here, :]
        prod_t = (grads.astype(F32) * ctx_ref[t, here, lane(0, j)].astype(F32)).T
        plain = [queries * masks[h] for h in range(heads)]
        g_each = [grads * masks[h] for h in range(heads)]
        marked = [jnp.concatenate([plain[h], own_docs], axis=1) for h in range(heads)]
        q_tall = jnp.concatenate(plain, axis=0)
        g_tall = jnp.concatenate(g_each, axis=0)
        inner = [
            jnp.sum(prod_t[h * HEAD_DIM : (h + 1) * HEAD_DIM], axis=0, keepdims=True)
            for h in range(heads)
        ]
        lse = [lse_ref[group, h : h + 1, here] for h in range(heads)]
        allowed = allowed_tile(code_ref, seg_ref, qi * TILE, qi * TILE)
        dq = [None] * heads

        for r in range(tiles):
            there = at(lax.rem(qi + r, tiles))
            keys = proj_ref[t, there, lane(1, j)]
            values = proj_ref[t, there, lane(2, j)]
            if r > 0:
                keys = jnp.concatenate([keys, bars_ref[there, :]], axis=1)
            for h in range(heads):
                scores = dot_nt(keys, marked[h] if r > 0 else plain[h])
                if r == 0:
                    scores = jnp.where(allowed, scores, -1e30)
                score_buf[r % 2, h] = scores
                gprob_buf[r % 2, h] = dot_nt(values, g_each[h])
            for h in range(heads):
                cols = slice(h * TILE, (h + 1) * TILE)
                for c in range(0, TILE, CHUNK):
                    rows_c = slice(c, c + CHUNK)
                    probs = jnp.exp(score_buf[r % 2, h, rows_c, :] - lse[h])
                    gscores = probs * (gprob_buf[r % 2, h, rows_c, :] - inner[h])
                    prob_buf[r, rows_c, cols] = probs.astype(BF16)
                    gscore_buf[r, rows_c, cols] = gscores.astype(BF16)
            dv_acc[there, :] += dot_nn(prob_buf[r], g_tall)
            dk_acc[there, :] += dot_nn(gscore_buf[r], q_tall)
        keys_t = jnp.concatenate([turned[lax.rem(qi + r, tiles)] for r in range(tiles)], axis=1)
        dq = []
        for h in range(heads):
            tall = gscore_buf[:, :, h * TILE : (h + 1) * TILE].reshape(tiles * TILE, TILE)
            dq.append(dot_nn(keys_t[h * HEAD_DIM : (h + 1) * HEAD_DIM], tall))
        both = jnp.concatenate(dq, axis=0) * 0.125
        dp_buf[t, here, lane(0, j)] = both.astype(BF16).T

        @pl.when(qi == tiles - 1)
        def _():
            low_k = dk_acc[...].astype(BF16)
            low_v = dv_acc[...].astype(BF16)
            low_q = dp_buf[t, :, lane(0, j)]
            dp_buf[t, :, lane(1, j)] = low_k
            dp_buf[t, :, lane(2, j)] = low_v
            t_buf[9, pl.ds(q_row + group, 1), :] = col_sum(low_q.astype(F32))
            v_row = q_row + parts * groups + group
            t_buf[9, pl.ds(v_row, 1), :] = col_sum(low_v.astype(F32))

    order = (2, 1, 3, 0)

    def split(p):
        r = lax.rem(p, LINE)
        o = jnp.where(r == 0, 2, jnp.where(r == 1, 1, jnp.where(r == 2, 3, 0)))
        return 1 + lax.div(p, LINE), o

    for source, k in ((b_ref, 1), (c_ref, 2)):
        for o in order:
            to_partner(source, k, o).start()
    trade_r.start()
    keep_r.start()
    t_buf[9] = small_ref[...]
    count = (chunks - 1) * LINE
    calm = count - 2
    share = parts * groups * tiles // calm

    def pass_second(p):
        stage_second(*split(p))

    def pass_first(p):
        k, o = split(p)
        stage_first(k, o)

        @pl.when(o > 0)
        def _():
            to_line(k, o).start()

    step = 256
    half_rows = rows // parts

    def input_slice(i):
        at_rows = pl.ds(pl.multiple_of(i * step, step), step)
        value = base_ref[at_rows, :]
        for t in range(parts):
            value = value + dot_nt(dp_buf[t, at_rows, :], w_ref[t, 0, :, :wide])
        half = lax.div(i * step, half_rows)
        row0 = pl.multiple_of(lax.rem(i * step, half_rows), step)
        xg_buf[half, pl.ds(row0, step), :] = value.astype(BF16)

    @pl.loop(0, count)
    def _(p):
        k, o = split(p)

        @pl.when(p < LINE)
        def _():
            stage_partner(b_ref, k, o)

        @pl.when(p >= LINE)
        def _():
            stage_partner(c_ref, k, o)

        @pl.when(p >= 1)
        def _():
            pass_second(p - 1)

        @pl.when(p >= 2)
        def _():
            pass_first(p - 2)

        @pl.when(p < calm)
        def _():
            @pl.loop(0, share)
            def _(n):
                attend_slice(p * share + n)

        @pl.when(p == calm)
        def _():
            @pl.loop(0, rows // step)
            def _(n):
                input_slice(n)

            trade.start()
            keep.start()
            small_step(0)

    for t in range(parts):
        for m in range(0, width, GRAD_STEP):
            at = slice(m, m + GRAD_STEP)
            left = x_ref[:, at]
            part = dot_tn(left, dp_buf[t])
            a_buf[t, at, :wide] = part.astype(BF16)
            part = dot_tn(first_ref[:, at], ctx_ref[t])
            a_buf[t, at, wide:] = part.astype(BF16)
        for o in order:
            for n in (2 * t, 2 * t + 1):
                to_partner_a(o, n).start()
        small_step(1 + t)
        if t == 0:
            pass_second(count - 1)
            pass_first(count - 2)
        else:
            pass_first(count - 1)
    small_step(3)

    for i in range(LINE + 2):
        if i < LINE:
            o = order[i]
            for n in range(4):
                to_partner_a(o, n).wait_recv()
            zz = place.along(o)
            add_partner(0, o, lambda yy, xx: a_buf[yy, a_rows(zz, xx, core), :])
        if 0 <= i - 1 < LINE:
            stage_second(0, order[i - 1])
        if 0 <= i - 2 < LINE:
            stage_first(0, order[i - 2])
            if order[i - 2] > 0:
                to_line(0, order[i - 2]).start()
        if i == 2:
            small_step(4)
    for k in (1, 2, 0):
        finish(k)

    for part in (keep, keep_r):
        part.wait()
    for part in (trade, trade_r):
        part.wait_send()
    for part in (arrive, arrive_r):
        part.wait_recv()
    for part in hops:
        part.wait_send()
    for o in range(1, LINE):
        small_line(o).wait_send()
    for k in range(chunks):
        for o in order:
            if k == 0:
                for n in range(4):
                    to_partner_a(o, n).wait_send()
            else:
                to_partner((b_ref, c_ref)[k - 1], k, o).wait_send()
            for n in range(2):
                to_second(k, o, n).wait_send()
            to_first(k, o).wait_send()
            if o > 0:
                to_line(k, o).wait_send()


def back_all(
    grads_b,
    grads_c,
    x,
    first_low,
    grad_first,
    projected,
    context,
    grad_context,
    lse,
    codes,
    seg_row,
    docs,
    bars,
    first,
    small,
    result,
):
    parts, width, units = grads_b.shape
    rows, model = x.shape
    wide = projected.shape[2]
    own_rows = width // (4 * LINE)
    chunks = 3
    folded = [g.reshape(parts, LINE, 2, 2, own_rows, units) for g in (grads_b, grads_c)]
    small_rows = small.shape[0] // 128
    local = pl.BlockSpec(memory_space=pltpu.VMEM)
    anywhere = pl.BlockSpec(memory_space=pl.ANY)
    piece = (own_rows, units)
    copies = chunks * LINE * PER_PIECE
    own, x_rows, out_rows, total = pl.pallas_call(
        back_kernel,
        in_specs=[local] * 15 + [anywhere],
        out_specs=[local, anywhere, anywhere, local],
        out_shape=[
            jax.ShapeDtypeStruct((chunks, own_rows, units), F32),
            jax.ShapeDtypeStruct((parts, rows // parts, model), BF16),
            jax.ShapeDtypeStruct((parts, rows // parts, model), BF16),
            jax.ShapeDtypeStruct((small_rows, 128), F32),
        ],
        scratch_shapes=[
            pltpu.VMEM((parts, width, units), BF16),
            pltpu.VMEM((parts, rows, wide), BF16),
            pltpu.VMEM((parts, rows // parts, model), BF16),
            pltpu.VMEM((chunks, LINE, 2, 2) + piece, BF16),
            pltpu.VMEM((chunks, LINE, 2) + piece, BF16),
            pltpu.VMEM((chunks, LINE) + piece, BF16),
            pltpu.VMEM((chunks, LINE - 1) + piece, BF16),
            pltpu.VMEM((6 + LINE, small_rows, 128), F32),
            pltpu.VMEM((rows // TILE, 128, TILE), BF16),
            pltpu.VMEM((2, 2, TILE, TILE), F32),
            pltpu.VMEM((2, 2, TILE, TILE), F32),
            pltpu.VMEM((rows // TILE, TILE, 2 * TILE), BF16),
            pltpu.VMEM((rows // TILE, TILE, 2 * TILE), BF16),
            pltpu.VMEM((rows, 128), F32),
            pltpu.VMEM((rows, 128), F32),
            pltpu.SemaphoreType.DMA((copies,)),
            pltpu.SemaphoreType.DMA((copies,)),
            pltpu.SemaphoreType.DMA((4 + LINE,)),
            pltpu.SemaphoreType.DMA((4 + LINE,)),
            pltpu.SemaphoreType.DMA((2,)),
        ],
        compiler_params=params(collective_id=1, has_side_effects=True),
        name="back_all",
    )(
        *folded,
        x,
        first_low,
        grad_first,
        projected,
        context,
        grad_context,
        lse,
        codes,
        seg_row,
        docs,
        bars,
        first,
        small.reshape(small_rows, 128),
        result.reshape(parts, rows // parts, model),
    )
    return own, x_rows, out_rows, total.reshape(-1)


def trade_in(halves):
    return lax.all_to_all(halves, "tensor", split_axis=0, concat_axis=1, tiled=True)[0]


def trade_out(whole):
    return lax.all_to_all(whole[None], "tensor", split_axis=1, concat_axis=0, tiled=True)


def gather_weights(shard):
    full = lax.all_gather(shard, "dp", axis=1, tiled=True)
    return lax.all_gather(full, "tensor", axis=0, tiled=False)


def scatter_grads(partial):
    own = lax.psum_scatter(partial, "tensor", scatter_dimension=0, tiled=False)
    return lax.psum_scatter(own, "dp", scatter_dimension=0, tiled=True)


def shards(
    inputs,
    seg_ids,
    keep_mask,
    w_qkv,
    b_qv,
    w_o,
    b_o,
    gain_one,
    shift_one,
    w_up,
    b_up,
    w_down,
    b_down,
    gain_two,
    shift_two,
    out_grad,
):
    parts = lax.axis_size("tensor")
    assert inputs.shape[0] == parts
    own_rows = w_qkv.shape[1]
    part_width = w_qkv.shape[2]
    units = w_up.shape[1]
    rank = lax.axis_index("tensor")

    shard_a = jnp.concatenate([w_qkv[0], w_qkv[1], w_qkv[2], w_o.T], axis=1)
    shard = jnp.stack([shard_a, w_up, w_down.T])
    seg = lax.dynamic_index_in_dim(seg_ids[:, 0], rank, 0, keepdims=False)
    keep = lax.dynamic_index_in_dim(keep_mask[:, 0], rank, 0, keepdims=False)
    length = seg.shape[0]
    firsts, lasts = seg[::TILE], seg[TILE - 1 :: TILE]
    low = (jnp.sum(seg[None, :] < firsts[:, None], axis=1) // TILE).astype(jnp.int32)
    past = jnp.sum(seg[None, :] <= lasts[:, None], axis=1)
    high = ((past + TILE - 1) // TILE).astype(jnp.int32)
    codes = jnp.broadcast_to(jnp.where(keep == 1, seg, -1)[:, None], (length, 128))
    seg_row = seg[None, :]

    b_q = b_qv[0].reshape(parts, part_width)
    b_v = b_qv[1].reshape(parts, part_width)
    bias = jnp.concatenate([b_q, jnp.zeros_like(b_q), b_v], axis=1)[:, None, :]
    zero = jnp.zeros_like(b_o)
    vectors = jnp.stack([b_o, gain_one, shift_one, b_down, gain_two, shift_two, zero, zero])
    bias_up = b_up.reshape(parts, 1, units)
    linked = lax.axis_size("dp") == LINE * 4 and parts == 2
    if linked:
        number = lax.broadcasted_iota(jnp.int32, (1, 128), 1)
        docs = (seg[:, None] == number).astype(BF16)
        bars = jnp.where(codes == number, 0.0, -1e30).astype(BF16)
        first, rest, x, grads, projected, context, lse, state = gather_all(
            shard,
            inputs[:, 0],
            bias,
            codes,
            seg_row,
            docs,
            bars,
            vectors,
            bias_up,
            out_grad[:, 0],
        )
    else:
        weights = gather_weights(shard)
        first, rest = weights[:, :1], weights[:, 1:]
        x = trade_in(inputs[:, 0])
        grads = trade_in(out_grad[:, 0])
        projected = project(x, first, bias)
        context, lse = attend(projected, low, high, codes, seg_row)
        state = rows_forward(x, context, first, rest, vectors, bias_up)
    normed, factor, active, slope = state
    out, hidden_low, second_low, first_low, grad_first, grad_up, grad_context, sums, upsum = (
        rows_pass(normed, factor, active, slope, grads, first, rest, vectors)
    )
    partial_up = outer(hidden_low, grad_up)
    partial_down = outer(second_low, active)
    if linked:
        zeros = jnp.zeros((4 * part_width,), F32)
        small = jnp.concatenate([sums[:6].reshape(-1), zeros, upsum.reshape(-1)])
        own, x_rows, out_rows, small = back_all(
            partial_up,
            partial_down,
            x,
            first_low,
            grad_first,
            projected,
            context,
            grad_context,
            lse,
            codes,
            seg_row,
            docs,
            bars,
            first,
            small,
            out,
        )
    else:
        grad_q, grad_k, grad_v, qsum, vsum = attend_back(
            projected, context, grad_context, lse, low, high, codes, seg_row
        )
        partial_a = outer_four(x, first_low, grad_q, grad_k, grad_v, context)
        own = jnp.stack(
            [scatter_grads(g).astype(F32) for g in (partial_a, partial_up, partial_down)]
        )
        x_rows = trade_out(input_grad(grad_first, grad_q, grad_k, grad_v, first))
        out_rows = trade_out(out)
        small = jnp.concatenate(
            [sums[:6].reshape(-1), qsum.reshape(-1), vsum.reshape(-1), upsum.reshape(-1)]
        )
        small = lax.psum(small, ("dp", "tensor"))
    width = sums.shape[1]
    vec = small[: 6 * width].reshape(6, width)
    flat = parts * part_width
    start = 6 * width
    q_all = lax.dynamic_slice(small, (start + rank * part_width,), (part_width,))
    v_all = lax.dynamic_slice(small, (start + flat + rank * part_width,), (part_width,))
    up_all = lax.dynamic_slice(small, (start + 2 * flat + rank * units,), (units,))

    own_a = own[0]
    qkv_grad = jnp.stack([own_a[:, c * part_width : (c + 1) * part_width] for c in range(3)])
    return (
        out_rows[:, None],
        x_rows.astype(F32)[:, None],
        qkv_grad,
        jnp.stack([q_all, v_all]),
        own_a[:, 3 * part_width :].T,
        vec[0],
        vec[1],
        vec[2],
        own[1],
        up_all,
        own[2].T,
        vec[3],
        vec[4],
        vec[5],
    )


def solution(mesh):
    placed = (
        P(None, "dp", "tensor", None),
        P(None, "dp", None),
        P(None, "dp", None),
        P(None, "dp", "tensor"),
        P(),
        P("tensor", "dp"),
        P(),
        P(),
        P(),
        P("dp", "tensor"),
        P(),
        P("tensor", "dp"),
        P(),
        P(),
        P(),
        P(None, "dp", "tensor", None),
    )
    return jax.shard_map(
        shards,
        mesh=mesh,
        in_specs=placed,
        out_specs=(
            P(None, "dp", "tensor", None),
            P(None, "dp", "tensor", None),
            P(None, "dp", "tensor"),
            P(None, "tensor"),
            P("tensor", "dp"),
            P(),
            P(),
            P(),
            P("dp", "tensor"),
            P("tensor"),
            P("tensor", "dp"),
            P(),
            P(),
            P(),
        ),
        check_vma=False,
    )
```
